32 devices in a mesh: row: 4 (over z), col: 8 (over y, x, core).
Axes of the slice: x: 2, y: 2, z: 4, core: 2. Of those that a mesh axis runs over, the one named last changes fastest.
Arguments:
- tokens: bfloat16 [2048, 2048], P(('row', 'col')), may hold values from -6 to 6
- timestep: int32 [1], replicated, may hold values from 0 to 999
- mod_weight: float32 [256, 2048], replicated, may hold values from -0.375 to 0.375
- qkv_weight: bfloat16 [3, 2048, 2048], P(None, None, 'col'), may hold values from -0.125 to 0.125
- attn_scale: float32 [16], P('col'), may hold values from 4 to 40
- out_weight: bfloat16 [2048, 2048], P('col'), may hold values from -0.5 to 0.5
- grad_update: bfloat16 [2048, 2048], P(('row', 'col')), may hold values from -6 to 6
Outputs:
- update: bfloat16 [2048, 2048], P(('row', 'col'))
- grad_tokens: bfloat16 [2048, 2048], P(('row', 'col'))
- grad_qkv: float32 [3, 2048, 2048], P(None, 'row', 'col')
- grad_out: float32 [2048, 2048], P('col', 'row')
The draws below stay inside these ranges and needn't reach their ends.
All inputs are finite; a program needn't handle non-finite values.
Results may differ from the reference program's by a relative error of at most 0.018.
Values may be sent and summed in bfloat16 or wider, within the bound.
A program may use at most 128 MiB of HBM per device.

```python
import math
import jax
import jax.numpy as jnp
from jax import lax

D = 2048
HEADS = 16
FREQS = 128
HDIM = 128
TOKENS = 2048


def block_levels(key, shape, pieces, least, high):
    def one(position, parts):
        draws = jax.random.uniform(jax.random.fold_in(jax.random.fold_in(key, 6), position), (parts,), jnp.float32, least / len(pieces), high / len(pieces))
        return jnp.repeat(jnp.exp(draws), shape[position] // parts).reshape((-1,) + (1,) * (len(shape) - position - 1))

    loudness = one(*pieces[0])
    for cut in pieces[1:]:
        loudness = loudness * one(*cut)
    return loudness


def centred(stream_key, shape, scale, bound, split=(), held_as=jnp.bfloat16):
    entries = jax.random.normal(stream_key, shape, jnp.float32) * scale
    if len(split) > 0:
        entries = block_levels(stream_key, shape, split, -0.22, 0.18) * entries
    return jnp.clip(entries, min=-bound, max=bound).astype(held_as)


def setup_inputs(seed: int = 0) -> dict:
    streams_of = jax.random.split(jax.random.key(seed), 8)
    tokens = centred(streams_of[0], (TOKENS, D), 1.0, 6.0, ((0, 32),))
    timestep = jax.random.randint(streams_of[1], (1,), 0, 1000).astype(jnp.int32)
    mod_weight = centred(streams_of[2], (2 * FREQS, D), (2 * FREQS) ** -0.5, 0.375, (), jnp.float32)
    qkv_weight = centred(streams_of[3], (3, D, D), D ** -0.5, 0.125, ((2, 8),))
    attn_scale = jnp.clip(jnp.exp(math.log(40.0) - 2.3025851 * jax.random.uniform(streams_of[4], (HEADS,), jnp.float32) ** block_levels(streams_of[4], (HEADS,), ((0, 8),), -0.2, 0.2)), 4.0, 40.0)
    out_weight = centred(streams_of[5], (D, D), HDIM ** -0.5, 0.5, ((0, 8),))
    grad_update = centred(streams_of[6], (TOKENS, D), 1.0, 6.0, ((0, 32),))
    return dict(tokens=tokens, timestep=timestep, mod_weight=mod_weight, qkv_weight=qkv_weight, attn_scale=attn_scale, out_weight=out_weight, grad_update=grad_update)


epsilon = 1e-06

def embed(timestep, count):
    index = jnp.arange(count, dtype=jnp.float32)
    freqs = jnp.exp(-math.log(10000.0) * index / count)
    angles = timestep.astype(jnp.float32)[0] * freqs
    return jnp.concatenate([jnp.cos(angles), jnp.sin(angles)])

def unit_rows(values):
    factor = lax.rsqrt(lax.optimization_barrier(jnp.mean(values * values, -1, keepdims=True)) + epsilon)
    return (values * factor, factor)

def unit_grad(grad_unit, unit, factor):
    return factor * (grad_unit - unit * lax.optimization_barrier(jnp.mean(grad_unit * unit, -1, keepdims=True)))

def forward_head(packed):
    query, key_rows, value_rows, scale = packed
    head_dim = query.shape[1]
    coeff = scale / head_dim
    size = math.gcd(query.shape[0], 512)
    blocks = query.reshape(query.shape[0] // size, size, head_dim)

    def one_block(query_block):
        scores = jnp.dot(query_block, key_rows.T, preferred_element_type=jnp.float32) * coeff
        weights = jnp.exp(scores - scale)
        totals = lax.optimization_barrier(jnp.sum(weights, -1))
        mixed = jnp.dot(weights.astype(jnp.bfloat16), value_rows, preferred_element_type=jnp.float32)
        return (totals, mixed)
    totals, mixed = lax.map(one_block, blocks)
    return (totals.reshape(-1), mixed.reshape(-1, head_dim))

def backward_head(packed):
    query, key_rows, value_rows, grad_rows, delta_rows, inverse_rows, scale = packed
    head_dim = query.shape[1]
    coeff = scale / head_dim
    length = query.shape[0]
    size = math.gcd(length, 512)
    blocks = (query.reshape(length // size, size, head_dim), grad_rows.reshape(length // size, size, head_dim), delta_rows.reshape(length // size, size), inverse_rows.reshape(length // size, size))

    def step(state, block):
        query_block, grad_block, delta_block, inverse_block = block
        scores = jnp.dot(query_block, key_rows.T, preferred_element_type=jnp.float32) * coeff
        probs = jnp.exp(scores - scale) * inverse_block[:, None]
        dprobs = jnp.dot(grad_block, value_rows.T, preferred_element_type=jnp.float32)
        dscores = (probs * (dprobs - delta_block[:, None]) * coeff).astype(jnp.bfloat16)
        grad_query = jnp.dot(dscores, key_rows, preferred_element_type=jnp.float32)
        grad_key = state[0] + jnp.dot(dscores.T, query_block, preferred_element_type=jnp.float32)
        grad_value = state[1] + jnp.dot(probs.astype(jnp.bfloat16).T, grad_block, preferred_element_type=jnp.float32)
        return ((grad_key, grad_value), grad_query)
    empty = jnp.zeros((length, head_dim), jnp.float32)
    (grad_key, grad_value), grad_query = lax.scan(step, (empty, empty), blocks)
    return (grad_query.reshape(length, head_dim), grad_key, grad_value)

def reference(tokens, timestep, mod_weight, qkv_weight, attn_scale, out_weight, grad_update):
    length, width = tokens.shape
    heads = attn_scale.shape[0]
    head_dim = width // heads
    embedded = embed(timestep, mod_weight.shape[0] // 2)
    gain = 1.0 + lax.optimization_barrier(jnp.sum(embedded[:, None] * mod_weight, 0))
    tok_float = tokens.astype(jnp.float32)
    rstd = lax.rsqrt(lax.optimization_barrier(jnp.mean(tok_float * tok_float, -1, keepdims=True)) + epsilon)
    normed = tok_float * rstd
    hidden = (normed * gain).astype(jnp.bfloat16)
    raw = jnp.stack([jnp.dot(hidden, qkv_weight[k], preferred_element_type=jnp.float32) for k in range(3)])
    query_unit, query_factor = unit_rows(raw[0].reshape(length, heads, head_dim))
    key_unit, key_factor = unit_rows(raw[1].reshape(length, heads, head_dim))
    query_heads = jnp.transpose(query_unit.astype(jnp.bfloat16), (1, 0, 2))
    key_heads = jnp.transpose(key_unit.astype(jnp.bfloat16), (1, 0, 2))
    value_heads = jnp.transpose(raw[2].astype(jnp.bfloat16).reshape(length, heads, head_dim), (1, 0, 2))
    totals, mixed = lax.map(forward_head, (query_heads, key_heads, value_heads, attn_scale))
    attended_heads = (mixed / totals[:, :, None]).astype(jnp.bfloat16)
    attended = jnp.transpose(attended_heads, (1, 0, 2)).reshape(length, width)
    update = jnp.dot(attended, out_weight, preferred_element_type=jnp.float32).astype(jnp.bfloat16)
    grad_out = jnp.dot(attended.T, grad_update, preferred_element_type=jnp.float32)
    grad_attended = jnp.dot(grad_update, out_weight.T, preferred_element_type=jnp.float32).astype(jnp.bfloat16)
    grad_heads = jnp.transpose(grad_attended.reshape(length, heads, head_dim), (1, 0, 2))
    delta = lax.optimization_barrier(jnp.sum(grad_heads.astype(jnp.float32) * attended_heads.astype(jnp.float32), -1))
    inverse = 1.0 / totals
    grad_query, grad_key, grad_value = lax.map(backward_head, (query_heads, key_heads, value_heads, grad_heads, delta, inverse, attn_scale))
    grad_query = jnp.transpose(grad_query, (1, 0, 2))
    grad_key = jnp.transpose(grad_key, (1, 0, 2))
    grad_value = jnp.transpose(grad_value, (1, 0, 2))
    grad_q = unit_grad(grad_query, query_unit, query_factor).astype(jnp.bfloat16).reshape(length, width)
    grad_k = unit_grad(grad_key, key_unit, key_factor).astype(jnp.bfloat16).reshape(length, width)
    grad_v = grad_value.astype(jnp.bfloat16).reshape(length, width)
    grad_raw = [grad_q, grad_k, grad_v]
    grad_qkv = jnp.stack([jnp.dot(hidden.T, grad_raw[k], preferred_element_type=jnp.float32) for k in range(3)])
    grad_hidden = jnp.dot(grad_raw[0], qkv_weight[0].T, preferred_element_type=jnp.float32)
    grad_hidden = grad_hidden + jnp.dot(grad_raw[1], qkv_weight[1].T, preferred_element_type=jnp.float32)
    grad_hidden = grad_hidden + jnp.dot(grad_raw[2], qkv_weight[2].T, preferred_element_type=jnp.float32)
    grad_normed = grad_hidden * gain
    grad_tokens = (rstd * (grad_normed - normed * lax.optimization_barrier(jnp.mean(grad_normed * normed, -1, keepdims=True)))).astype(jnp.bfloat16)
    return (update, grad_tokens, grad_qkv, grad_out)
```

```python
import functools
import math

import jax
import jax.numpy as jnp
from jax import lax
from jax.experimental import pallas as pl
from jax.experimental.pallas import tpu as pltpu
from jax.sharding import PartitionSpec as P

epsilon = 1e-06
MESH = pl.DeviceIdType.MESH
RELAYED = 4


def embed(timestep, count):
    index = jnp.arange(count, dtype=jnp.float32)
    freqs = jnp.exp(-math.log(10000.0) * index / count)
    angles = timestep.astype(jnp.float32)[0] * freqs
    return jnp.concatenate([jnp.cos(angles), jnp.sin(angles)])


def by_head(array, head_dim):
    return [array[:, at : at + head_dim] for at in range(0, array.shape[1], head_dim)]


def unit_rows(values):
    factor = lax.rsqrt(jnp.mean(values * values, -1, keepdims=True) + epsilon)
    return (values * factor, factor)


def unit_grad(grad_unit, unit, factor):
    return factor * (grad_unit - unit * jnp.mean(grad_unit * unit, -1, keepdims=True))


def piece(ref, dim, size, index):
    start = index * size
    if isinstance(start, int):
        pass
    elif dim == len(ref.shape) - 1:
        start = pl.multiple_of(start, 128)
    elif dim == len(ref.shape) - 2:
        start = pl.multiple_of(start, 16)
    return ref.at[(slice(None),) * dim + (pl.ds(start, size),)]


def half(ref, side):
    dim = len(ref.shape) - 2
    size = ref.shape[dim] // 2
    return ref.at[(slice(None),) * dim + (pl.ds(side * size, size),)]


def exchange_kernel(plan, *refs):
    count = len(plan)
    sources, targets = refs[:count], refs[count : 2 * count]
    own_sem, send_sem, recv_sem = refs[2 * count : 2 * count + 3]
    relays = refs[2 * count + 3 :]
    sizes = {axis: n for axis, n, dim, size in plan}
    barrier = pltpu.get_barrier_semaphore()
    for axis, n in sizes.items():
        me = lax.axis_index(axis)
        for step in range(1, n):
            pl.semaphore_signal(
                barrier, inc=1, device_id={axis: lax.rem(me + step, n)}, device_id_type=MESH
            )
    pl.semaphore_wait(barrier, sum(n - 1 for n in sizes.values()))
    def send(job, slot, source, target, peer):
        copy = pltpu.make_async_remote_copy(
            src_ref=source,
            dst_ref=target,
            send_sem=send_sem.at[job, slot],
            recv_sem=recv_sem.at[job, slot],
            device_id={plan[job][0]: peer},
            device_id_type=MESH,
        )
        copy.start()
        return copy

    copies, hops = [], {}
    chained = [job for job in range(count) if plan[job][1] == RELAYED and plan[job][2] is not None]
    relayed = [job for job in range(count) if plan[job][1] == RELAYED and job not in chained]
    for step in range(1, max(sizes.values())):
        for job, (axis, n, dim, size) in enumerate(plan):
            if step >= n or job in chained or (n == RELAYED and step == 2):
                continue
            me = lax.axis_index(axis)
            peer = lax.rem(me + step, n)
            source = sources[job]
            source = source if dim is None else piece(source, dim, size, peer)
            copy = send(job, step, source, targets[job].at[me], peer)
            if n == RELAYED and dim is None:
                hops.setdefault(job, []).append(copy)
            else:
                copies.append(copy)
    for job, (axis, n, dim, size) in enumerate(plan):
        if job in chained:
            continue
        me = lax.axis_index(axis)
        source = sources[job]
        copy = pltpu.make_async_copy(
            source if dim is None else piece(source, dim, size, me),
            targets[job].at[me],
            own_sem.at[job],
        )
        copy.start()
        copies.append(copy)
    for side in range(2):
        for job in relayed:
            axis, n, dim, size = plan[job]
            me = lax.axis_index(axis)
            right, left = lax.rem(me + 1, n), lax.rem(me + 3, n)
            onward, origin = (right, left) if side == 0 else (left, right)
            hops[job][side].wait_recv()
            landing = half(targets[job].at[origin], side)
            copies.append(send(job, 6 + side, landing, landing, onward))
    def link(job, way, owner, source):
        axis = plan[job][0]
        me = lax.axis_index(axis)
        slot = owner - 1 if way == 0 else owner
        return pltpu.make_async_remote_copy(
            src_ref=relays[job].at[way, slot] if source is None else source,
            dst_ref=relays[job].at[way, slot],
            send_sem=send_sem.at[job, 3 * way + slot],
            recv_sem=recv_sem.at[job, 3 * way + slot],
            device_id={axis: lax.rem(me + (1 if way == 0 else RELAYED - 1), RELAYED)},
            device_id_type=MESH,
        )

    def forward(job, way, owner, place):
        axis, n, dim, size = plan[job]
        mine = piece(sources[job], dim, size, owner)

        @pl.when(lax.axis_index(axis) == place)
        def _():
            if place == (0 if way == 0 else n - 1):
                link(job, way, owner, mine).start()
            else:
                copy = link(job, way, owner, None)
                copy.wait_recv()
                inbox = relays[job].at[way, owner - 1 if way == 0 else owner]
                total = inbox[...].astype(jnp.float32) + mine[...].astype(jnp.float32)
                inbox[...] = total.astype(inbox.dtype)
                copy.start()

    order = [(0, 3, 0), (1, 0, 3), (0, 2, 0), (1, 1, 3), (0, 1, 0), (1, 2, 3)]
    order += [(0, 3, 1), (1, 0, 2), (0, 2, 1), (1, 1, 2), (0, 3, 2), (1, 0, 1)]
    for way, owner, place in order:
        for job in chained:
            forward(job, way, owner, place)
    for job in chained:
        axis, n, dim, size = plan[job]
        for owner in range(n):

            @pl.when(lax.axis_index(axis) == owner)
            def _():
                total = piece(sources[job], dim, size, owner)[...].astype(jnp.float32)
                if owner > 0:
                    link(job, 0, owner, None).wait_recv()
                    total = total + relays[job][0, owner - 1].astype(jnp.float32)
                if owner < n - 1:
                    link(job, 1, owner, None).wait_recv()
                    total = total + relays[job][1, owner].astype(jnp.float32)
                targets[job][0] = total
                for other in range(n):
                    if other > owner:
                        link(job, 0, other, None).wait_send()
                    if other < owner:
                        link(job, 1, other, None).wait_send()

    for job in relayed:
        for copy in hops[job]:
            copy.wait_send()
    for copy in copies:
        copy.wait()


def exchange(jobs, collective_id):
    plan, shapes, relays = [], [], []
    for array, axis, dim in jobs:
        n = lax.axis_size(axis)
        block = list(array.shape)
        size = None
        if dim is not None:
            size = block[dim] = block[dim] // n
        plan.append((axis, n, dim, size))
        if n == RELAYED and dim is not None:
            shapes.append(jax.ShapeDtypeStruct((1,) + tuple(block), jnp.float32))
            relays.append(pltpu.VMEM((2, n - 1) + tuple(block), array.dtype))
        else:
            shapes.append(jax.ShapeDtypeStruct((n,) + tuple(block), array.dtype))
            relays.append(pltpu.VMEM((16, 128), array.dtype))
    most = max(2 * RELAYED, max(n for axis, n, dim, size in plan))
    count = len(jobs)
    in_vmem = pl.BlockSpec(memory_space=pltpu.VMEM)
    return pl.pallas_call(
        functools.partial(exchange_kernel, tuple(plan)),
        out_shape=shapes,
        in_specs=[in_vmem] * count,
        out_specs=[in_vmem] * count,
        scratch_shapes=[
            pltpu.SemaphoreType.DMA((count,)),
            pltpu.SemaphoreType.DMA((count, most)),
            pltpu.SemaphoreType.DMA((count, most)),
            *relays,
        ],
        compiler_params=pltpu.CompilerParams(
            collective_id=collective_id, has_side_effects=True, vmem_limit_bytes=48 * 2**20
        ),
        name=f"exchange_{collective_id}",
    )(*[array for array, axis, dim in jobs])


def dot_rows(left, right):
    return lax.dot_general(
        left, right, (((1,), (1,)), ((), ())), preferred_element_type=jnp.float32
    )


def dot_columns(left, right):
    return lax.dot_general(
        left, right, (((0,), (0,)), ((), ())), preferred_element_type=jnp.float32
    )


def attention_kernel(
    scale_ref, q_ref, k_ref, v_ref, g_ref, o_ref, dq_ref, dk_ref, dv_ref, dk_sum, dv_sum
):
    block = pl.program_id(1)
    scale = scale_ref[pl.program_id(0)]
    coeff = scale * (1.0 / q_ref.shape[1])
    query, keys, values, grad = q_ref[...], k_ref[...], v_ref[...], g_ref[...]
    weights = jnp.exp(dot_rows(query, keys) * coeff - scale)
    inverse = 1.0 / jnp.sum(weights, -1, keepdims=True)
    mixed = jnp.dot(weights.astype(jnp.bfloat16), values, preferred_element_type=jnp.float32)
    attended = (mixed * inverse).astype(jnp.bfloat16)
    o_ref[...] = attended
    delta = jnp.sum(
        grad.astype(jnp.float32) * attended.astype(jnp.float32), -1, keepdims=True
    )
    probs = weights * inverse
    dscores = (probs * (dot_rows(grad, values) - delta) * coeff).astype(jnp.bfloat16)
    dq_ref[...] = jnp.dot(dscores, keys, preferred_element_type=jnp.float32)
    dk_part = dot_columns(dscores, query)
    dv_part = dot_columns(probs.astype(jnp.bfloat16), grad)

    @pl.when(block == 0)
    def _():
        dk_sum[...] = dk_part
        dv_sum[...] = dv_part

    @pl.when(block > 0)
    def _():
        dk_sum[...] += dk_part
        dv_sum[...] += dv_part

    @pl.when(block == pl.num_programs(1) - 1)
    def _():
        dk_ref[...] = dk_sum[...].astype(dk_ref.dtype)
        dv_ref[...] = dv_sum[...].astype(dv_ref.dtype)


def attention(attn_scale, queries, keys_values, grads, sums=jnp.bfloat16):
    heads = attn_scale.shape[0]
    span, inner = queries.shape
    length = keys_values.shape[0]
    head_dim = inner // heads
    size = math.gcd(span, 256)
    while size * length > 2**19 and size % 32 == 0:
        size //= 2
    mine = pl.BlockSpec((size, head_dim), lambda h, i: (i, h))
    keys = pl.BlockSpec((length, head_dim), lambda h, i: (0, h))
    values = pl.BlockSpec((length, head_dim), lambda h, i: (0, heads + h))
    return pl.pallas_call(
        attention_kernel,
        grid=(heads, span // size),
        out_shape=[
            jax.ShapeDtypeStruct((span, inner), jnp.bfloat16),
            jax.ShapeDtypeStruct((span, inner), jnp.float32),
            jax.ShapeDtypeStruct((length, inner), sums),
            jax.ShapeDtypeStruct((length, inner), sums),
        ],
        in_specs=[pl.BlockSpec(memory_space=pltpu.SMEM), mine, keys, values, mine],
        out_specs=[mine, mine, keys, keys],
        scratch_shapes=[pltpu.VMEM((length, head_dim), jnp.float32)] * 2,
        compiler_params=pltpu.CompilerParams(
            dimension_semantics=("arbitrary", "arbitrary"), vmem_limit_bytes=56 * 2**20
        ),
        name="attention",
    )(attn_scale, queries, keys_values, keys_values, grads)


def add_up(slots):
    return jnp.sum(slots.astype(jnp.float32), 0)


def per_device(tokens, timestep, mod_weight, qkv_weight, attn_scale, out_weight, grad_update):
    tok_dev, width = tokens.shape
    heads_here = attn_scale.shape[0]
    inner = qkv_weight.shape[2]
    head_dim = inner // heads_here
    span = tok_dev * lax.axis_size("col")
    embedded = embed(timestep, mod_weight.shape[0] // 2)
    gain = 1.0 + jnp.sum(embedded[:, None] * mod_weight, 0)
    tok_float = tokens.astype(jnp.float32)
    rstd = lax.rsqrt(jnp.mean(tok_float * tok_float, -1, keepdims=True) + epsilon)
    normed = tok_float * rstd
    hidden = (normed * gain).astype(jnp.bfloat16)
    (group,) = exchange([(hidden, "col", None)], 0)
    group = group.reshape(span, width)
    raw = [jnp.dot(group, qkv_weight[k], preferred_element_type=jnp.float32) for k in range(3)]
    query_unit, query_factor = zip(*[unit_rows(part) for part in by_head(raw[0], head_dim)])
    key_unit, key_factor = zip(*[unit_rows(part) for part in by_head(raw[1], head_dim)])
    queries = jnp.concatenate(query_unit, 1).astype(jnp.bfloat16)
    keys_values = jnp.concatenate(key_unit + (raw[2],), 1).astype(jnp.bfloat16)
    all_keys_values, grad_group = exchange(
        [(keys_values, "row", None), (grad_update, "col", None)], 1
    )
    all_keys_values = all_keys_values.reshape(-1, 2 * inner)
    grad_group = grad_group.reshape(span, width)
    grad_attended = dot_rows(grad_group, out_weight).astype(jnp.bfloat16)
    attended, grad_query, key_part, value_part = attention(
        attn_scale, queries, all_keys_values, grad_attended
    )
    update_part = jnp.dot(attended, out_weight, preferred_element_type=jnp.float32).astype(
        jnp.bfloat16
    )
    out_part = dot_columns(attended, grad_group).astype(jnp.bfloat16)
    key_slots, value_slots, update_slots = exchange(
        [(key_part, "row", 0), (value_part, "row", 0), (update_part, "col", 0)], 2
    )
    update = add_up(update_slots).astype(jnp.bfloat16)

    def raw_grads(grad_unit, unit, factor):
        parts = zip(by_head(grad_unit, head_dim), unit, factor)
        return jnp.concatenate([unit_grad(*part) for part in parts], 1).astype(jnp.bfloat16)

    grad_raw = [
        raw_grads(grad_query, query_unit, query_factor),
        raw_grads(add_up(key_slots), key_unit, key_factor),
        add_up(value_slots).astype(jnp.bfloat16),
    ]
    qkv_part = jnp.stack([dot_columns(group, part).astype(jnp.bfloat16) for part in grad_raw])
    hidden_part = (
        sum(dot_rows(part, qkv_weight[k]) for k, part in enumerate(grad_raw))
    ).astype(jnp.bfloat16)
    qkv_slots, hidden_slots, out_slots = exchange(
        [(qkv_part, "row", 1), (hidden_part, "col", 0), (out_part, "row", 1)], 3
    )
    grad_qkv = add_up(qkv_slots)
    grad_out = add_up(out_slots)
    grad_normed = add_up(hidden_slots) * gain
    grad_tokens = (
        rstd * (grad_normed - normed * jnp.mean(grad_normed * normed, -1, keepdims=True))
    ).astype(jnp.bfloat16)
    return (update, grad_tokens, grad_qkv, grad_out)


def flip(index, bit):
    return index + bit - 2 * bit * ((index // bit) % 2)


class Place:
    def __init__(self):
        self.row = lax.axis_index("row")
        self.col = lax.axis_index("col")
        self.partner = flip(self.col, 1)
        self.beside = flip(self.col, 2)
        self.across = flip(self.col, 4)
        self.corner = flip(self.beside, 4)
        self.inner = ((self.row + 1) // 2) % 2 == 1
        self.mate = flip(self.row, 1)
        self.facing = 3 - self.row
        low = 1 - self.row // 2
        self.ranks = [self.row, self.mate, 1 + low, 3 * low]

    def greet(self):
        barrier = pltpu.get_barrier_semaphore()
        for peer in (self.partner, self.beside, self.across):
            pl.semaphore_signal(barrier, inc=1, device_id={"col": peer}, device_id_type=MESH)
        pl.semaphore_signal(barrier, inc=1, device_id={"row": self.mate}, device_id_type=MESH)

        @pl.when(self.inner)
        def _():
            pl.semaphore_signal(
                barrier, inc=1, device_id={"row": self.facing}, device_id_type=MESH
            )

        pl.semaphore_wait(barrier, 4 + ((self.row + 1) // 2) % 2)


KINDS = 9
LINE, BESIDE, ACROSS, TOP, BOTTOM, MATE = 0, 1, 2, 3, 4, 5
SENDS = 12


class Gather:
    def __init__(self, place, job, tile, whole, send_sem, recv_sem):
        self.place, self.job, self.tile, self.whole = place, job, tile, whole
        self.send_sem, self.recv_sem = send_sem, recv_sem

    def slot(self, rank, col):
        return self.whole.at[self.place.ranks[rank], col]

    def link(self, rank, kind, send, source, landing, peer):
        return pltpu.make_async_remote_copy(
            src_ref=source,
            dst_ref=landing,
            send_sem=self.send_sem.at[self.job, send[0], send[1]],
            recv_sem=self.recv_sem.at[self.job, rank, kind],
            device_id=peer,
            device_id_type=MESH,
        )

    def arrived(self, rank, kind, landing):
        self.link(rank, kind, (0, 0), landing, landing, {"col": self.place.partner}).wait_recv()

    def held(self, rank):
        return self.tile if rank == 0 else self.slot(rank, self.place.col)

    def line_sends(self, rank):
        p = self.place
        mine = self.slot(rank, p.col)
        held = self.held(rank)
        if rank == 0:
            outward = self.link(1, LINE, (0, 0), held, mine, {"row": p.mate})
            inward = self.link(2, LINE, (0, 1), held, mine, {"row": p.facing})
            return [(outward, False), (inward, True)]
        if rank == 1:
            return [(self.link(3, LINE, (1, 0), held, mine, {"row": p.facing}), True)]
        return [(self.link(rank, LINE, (rank, 0), held, mine, {"row": p.mate}), True)]

    def plane_sends(self, rank):
        p = self.place
        mine, held = self.slot(rank, p.col), self.held(rank)
        return [
            self.link(rank, BESIDE, (rank, 2), held, mine, {"col": p.beside}),
            self.link(rank, ACROSS, (rank, 3), held, mine, {"col": p.across}),
            self.link(rank, MATE, (rank, 4), held, mine, {"col": p.partner}),
        ]

    def relays(self, rank):
        p = self.place
        side, over = self.slot(rank, p.beside), self.slot(rank, p.across)
        return [
            self.link(rank, TOP, (rank, 5), half(side, 0), half(side, 0), {"col": p.across}),
            self.link(rank, MATE + 1, (rank, 6), side, side, {"col": p.partner}),
            self.link(rank, BOTTOM, (rank, 7), half(over, 1), half(over, 1), {"col": p.beside}),
            self.link(rank, MATE + 2, (rank, 8), over, over, {"col": p.partner}),
        ]

    def last(self, rank):
        p = self.place
        far = self.slot(rank, p.corner)
        return self.link(rank, MATE + 3, (rank, 9), far, far, {"col": p.partner})

    def each(self, copies, act):
        for copy, inner in copies:
            if inner:
                pl.when(self.place.inner)(functools.partial(act, copy))
            else:
                act(copy)

    def open(self, rank):
        p = self.place
        if rank == 0:
            self.whole[p.row, p.col] = self.tile[...]
        else:
            self.arrived(rank, LINE, self.slot(rank, p.col))
            self.each(self.line_sends(rank), lambda copy: copy.start())
        for copy in self.plane_sends(rank):
            copy.start()

    def relay(self, rank):
        p = self.place
        top, side, bottom, over = self.relays(rank)
        self.arrived(rank, BESIDE, self.slot(rank, p.beside))
        top.start()
        side.start()
        self.arrived(rank, ACROSS, self.slot(rank, p.across))
        bottom.start()
        over.start()

    def close(self, rank):
        p = self.place
        far = self.slot(rank, p.corner)
        self.arrived(rank, TOP, half(far, 0))
        self.arrived(rank, BOTTOM, half(far, 1))
        self.last(rank).start()

    def whole_rank(self, rank):
        p = self.place
        for kind, col in enumerate((p.col, p.beside, p.across, p.corner)):
            self.arrived(rank, MATE + kind, self.slot(rank, flip(col, 1)))

    def drain(self):
        for rank in range(4):
            self.each(self.line_sends(rank), lambda copy: copy.wait_send())
            for copy in self.plane_sends(rank) + self.relays(rank) + [self.last(rank)]:
                copy.wait_send()


def gather_kernel(count, *refs):
    tiles, wholes = refs[:count], refs[count : 2 * count]
    send_sem, recv_sem = refs[2 * count :]
    place = Place()
    place.greet()
    jobs = [
        Gather(place, job, tiles[job], wholes[job], send_sem, recv_sem) for job in range(count)
    ]
    for job in jobs:
        job.each(job.line_sends(0), lambda copy: copy.start())
    steps = [(job, rank) for job in jobs for rank in range(4)]
    for at in range(len(steps) + 3):
        if at < len(steps):
            steps[at][0].open(steps[at][1])
        if 0 <= at - 1 < len(steps):
            steps[at - 1][0].relay(steps[at - 1][1])
        if 0 <= at - 2 < len(steps):
            steps[at - 2][0].close(steps[at - 2][1])
        if 0 <= at - 3 < len(steps):
            steps[at - 3][0].whole_rank(steps[at - 3][1])
    for job in jobs:
        job.drain()


def gather_all(tiles, collective_id):
    count = len(tiles)
    rows, cols = lax.axis_size("row"), lax.axis_size("col")
    in_vmem = pl.BlockSpec(memory_space=pltpu.VMEM)
    return pl.pallas_call(
        functools.partial(gather_kernel, count),
        out_shape=[jax.ShapeDtypeStruct((rows, cols) + t.shape, t.dtype) for t in tiles],
        in_specs=[in_vmem] * count,
        out_specs=[in_vmem] * count,
        scratch_shapes=[
            pltpu.SemaphoreType.DMA((count, 4, SENDS)),
            pltpu.SemaphoreType.DMA((count, 4, KINDS)),
        ],
        compiler_params=pltpu.CompilerParams(
            collective_id=collective_id, has_side_effects=True, vmem_limit_bytes=48 * 2**20
        ),
        name="gather_all",
    )(*tiles)


class Scatter:
    def __init__(self, place, job, part, crossed, staged, landed, send_sem, recv_sem):
        self.place, self.job, self.part = place, job, part
        self.crossed, self.staged, self.landed = crossed, staged, landed
        self.send_sem, self.recv_sem = send_sem, recv_sem
        self.size = part.shape[0] // 8

    def targets(self):
        p = self.place
        return (p.corner, p.beside, p.across, p.col)

    def rows(self, col):
        return pl.ds(pl.multiple_of(col * self.size, 16), self.size)

    def core_send(self, at):
        p = self.place
        return pltpu.make_async_remote_copy(
            src_ref=self.part.at[self.rows(flip(self.targets()[at], 1))],
            dst_ref=self.crossed.at[self.job, at],
            send_sem=self.send_sem.at[self.job, at],
            recv_sem=self.recv_sem.at[self.job, at],
            device_id={"col": p.partner},
            device_id_type=MESH,
        )

    def chip_send(self, at):
        return pltpu.make_async_remote_copy(
            src_ref=self.staged.at[self.job, at],
            dst_ref=self.landed.at[self.job, at],
            send_sem=self.send_sem.at[self.job, 4 + at],
            recv_sem=self.recv_sem.at[self.job, 4 + at],
            device_id={"col": self.targets()[at]},
            device_id_type=MESH,
        )

    def chip_sum(self, at):
        mine = self.part[self.rows(self.targets()[at]), :].astype(jnp.float32)
        return mine + self.crossed[self.job, at].astype(jnp.float32)

    def first(self):
        for at in range(4):
            self.core_send(at).start()

    def second(self):
        for at in range(3):
            self.core_send(at).wait_recv()
            self.staged[self.job, at] = self.chip_sum(at).astype(self.staged.dtype)
            self.chip_send(at).start()

    def third(self):
        self.core_send(3).wait_recv()
        total = self.chip_sum(3)
        for at in (1, 2, 0):
            self.chip_send(at).wait_recv()
            total = total + self.landed[self.job, at].astype(jnp.float32)
        for at in range(4):
            self.core_send(at).wait_send()
        for at in range(3):
            self.chip_send(at).wait_send()
        return total


def greet_plane(place):
    barrier = pltpu.get_barrier_semaphore()
    peers = (place.partner, place.beside, place.across, place.corner)
    for peer in peers:
        pl.semaphore_signal(barrier, inc=1, device_id={"col": peer}, device_id_type=MESH)
    pl.semaphore_wait(barrier, len(peers))


def scatter_kernel(count, *refs):
    parts, totals = refs[:count], refs[count : 2 * count]
    crossed, staged, landed, send_sem, recv_sem = refs[2 * count :]
    place = Place()
    greet_plane(place)
    jobs = [
        Scatter(place, job, parts[job], crossed, staged, landed, send_sem, recv_sem)
        for job in range(count)
    ]
    for job in jobs:
        job.first()
    for job in jobs:
        job.second()
    for job, total in zip(jobs, totals):
        total[...] = job.third()


def scatter(parts, collective_id):
    count = len(parts)
    rows, width = parts[0].shape
    size = rows // lax.axis_size("col")
    in_vmem = pl.BlockSpec(memory_space=pltpu.VMEM)
    return pl.pallas_call(
        functools.partial(scatter_kernel, count),
        out_shape=[jax.ShapeDtypeStruct((size, width), jnp.float32)] * count,
        in_specs=[in_vmem] * count,
        out_specs=[in_vmem] * count,
        scratch_shapes=[
            pltpu.VMEM((count, 4, size, width), jnp.bfloat16),
            pltpu.VMEM((count, 3, size, width), jnp.bfloat16),
            pltpu.VMEM((count, 3, size, width), jnp.bfloat16),
            pltpu.SemaphoreType.DMA((count, 8)),
            pltpu.SemaphoreType.DMA((count, 8)),
        ],
        compiler_params=pltpu.CompilerParams(
            collective_id=collective_id, has_side_effects=True, vmem_limit_bytes=48 * 2**20
        ),
        name=f"scatter_{collective_id}",
    )(*parts)


def gathered(tokens, timestep, mod_weight, qkv_weight, attn_scale, out_weight, grad_update):
    tok_dev, width = tokens.shape
    heads_here = attn_scale.shape[0]
    inner = qkv_weight.shape[2]
    head_dim = inner // heads_here
    rows = lax.axis_size("row")
    span = tok_dev * lax.axis_size("col")
    row = lax.axis_index("row")
    embedded = embed(timestep, mod_weight.shape[0] // 2)
    gain = 1.0 + jnp.sum(embedded[:, None] * mod_weight, 0)
    tok_float = tokens.astype(jnp.float32)
    rstd = lax.rsqrt(jnp.mean(tok_float * tok_float, -1, keepdims=True) + epsilon)
    normed = tok_float * rstd
    hidden = (normed * gain).astype(jnp.bfloat16)
    all_hidden, all_grads = gather_all([hidden, grad_update], 4)
    all_hidden = all_hidden.reshape(-1, width)
    all_grads = all_grads.reshape(-1, width)
    raw = [
        jnp.dot(all_hidden, qkv_weight[k], preferred_element_type=jnp.float32) for k in range(3)
    ]
    query_unit, query_factor = zip(*[unit_rows(part) for part in by_head(raw[0], head_dim)])
    key_unit, key_factor = zip(*[unit_rows(part) for part in by_head(raw[1], head_dim)])
    queries = jnp.concatenate(query_unit, 1).astype(jnp.bfloat16)
    keys_values = jnp.concatenate(key_unit + (raw[2],), 1).astype(jnp.bfloat16)
    grad_attended = dot_rows(all_grads, out_weight).astype(jnp.bfloat16)
    attended, grad_query, grad_key, grad_value = attention(
        attn_scale, queries, keys_values, grad_attended, jnp.float32
    )

    def of_row(array, dim):
        size = array.shape[dim] // rows
        return lax.dynamic_slice_in_dim(array, row * size, size, dim)

    update_part = jnp.dot(
        of_row(attended, 0), out_weight, preferred_element_type=jnp.float32
    ).astype(jnp.bfloat16)
    grad_out = dot_columns(attended, of_row(all_grads, 1))

    def raw_grads(grad_unit, unit, factor):
        parts = zip(by_head(grad_unit, head_dim), unit, factor)
        return jnp.concatenate([unit_grad(*part) for part in parts], 1).astype(jnp.bfloat16)

    grad_raw = [
        raw_grads(grad_query, query_unit, query_factor),
        raw_grads(grad_key, key_unit, key_factor),
        grad_value.astype(jnp.bfloat16),
    ]
    grad_qkv = jnp.stack([dot_columns(of_row(all_hidden, 1), part) for part in grad_raw])
    hidden_part = (
        sum(dot_rows(of_row(part, 0), qkv_weight[k]) for k, part in enumerate(grad_raw))
    ).astype(jnp.bfloat16)
    update, grad_hidden = scatter([update_part, hidden_part], 5)
    grad_normed = grad_hidden * gain
    grad_tokens = (
        rstd * (grad_normed - normed * jnp.mean(grad_normed * normed, -1, keepdims=True))
    ).astype(jnp.bfloat16)
    return (update.astype(jnp.bfloat16), grad_tokens, grad_qkv, grad_out)


def solution(mesh):
    placed = (
        P(("row", "col"), None),
        P(),
        P(),
        P(None, None, "col"),
        P("col"),
        P("col", None),
        P(("row", "col"), None),
    )
    plane = mesh.shape["row"] == 4 and mesh.shape["col"] == 8
    return jax.shard_map(
        gathered if plane else per_device,
        mesh=mesh,
        in_specs=placed,
        out_specs=(
            P(("row", "col"), None),
            P(("row", "col"), None),
            P(None, "row", "col"),
            P("col", "row"),
        ),
        check_vma=False,
    )
```

```python
import functools
import math

import jax
import jax.numpy as jnp
from jax import lax
from jax.experimental import pallas as pl
from jax.experimental.pallas import tpu as pltpu
from jax.sharding import PartitionSpec as P

epsilon = 1e-06
MESH = pl.DeviceIdType.MESH
RELAYED = 4


def embed(timestep, count):
    index = jnp.arange(count, dtype=jnp.float32)
    freqs = jnp.exp(-math.log(10000.0) * index / count)
    angles = timestep.astype(jnp.float32)[0] * freqs
    return jnp.concatenate([jnp.cos(angles), jnp.sin(angles)])


def by_head(array, head_dim):
    return [array[:, at : at + head_dim] for at in range(0, array.shape[1], head_dim)]


def unit_rows(values):
    factor = lax.rsqrt(jnp.mean(values * values, -1, keepdims=True) + epsilon)
    return (values * factor, factor)


def unit_grad(grad_unit, unit, factor):
    return factor * (grad_unit - unit * jnp.mean(grad_unit * unit, -1, keepdims=True))


def piece(ref, dim, size, index):
    start = index * size
    if isinstance(start, int):
        pass
    elif dim == len(ref.shape) - 1:
        start = pl.multiple_of(start, 128)
    elif dim == len(ref.shape) - 2:
        start = pl.multiple_of(start, 16)
    return ref.at[(slice(None),) * dim + (pl.ds(start, size),)]


def half(ref, side):
    dim = len(ref.shape) - 2
    size = ref.shape[dim] // 2
    return ref.at[(slice(None),) * dim + (pl.ds(side * size, size),)]


def exchange_kernel(plan, *refs):
    count = len(plan)
    sources, targets = refs[:count], refs[count : 2 * count]
    own_sem, send_sem, recv_sem = refs[2 * count : 2 * count + 3]
    relays = refs[2 * count + 3 :]
    sizes = {axis: n for axis, n, dim, size in plan}
    barrier = pltpu.get_barrier_semaphore()
    for axis, n in sizes.items():
        me = lax.axis_index(axis)
        for step in range(1, n):
            pl.semaphore_signal(
                barrier, inc=1, device_id={axis: lax.rem(me + step, n)}, device_id_type=MESH
            )
    pl.semaphore_wait(barrier, sum(n - 1 for n in sizes.values()))
    def send(job, slot, source, target, peer):
        copy = pltpu.make_async_remote_copy(
            src_ref=source,
            dst_ref=target,
            send_sem=send_sem.at[job, slot],
            recv_sem=recv_sem.at[job, slot],
            device_id={plan[job][0]: peer},
            device_id_type=MESH,
        )
        copy.start()
        return copy

    copies, hops = [], {}
    chained = [job for job in range(count) if plan[job][1] == RELAYED and plan[job][2] is not None]
    relayed = [job for job in range(count) if plan[job][1] == RELAYED and job not in chained]
    for step in range(1, max(sizes.values())):
        for job, (axis, n, dim, size) in enumerate(plan):
            if step >= n or job in chained or (n == RELAYED and step == 2):
                continue
            me = lax.axis_index(axis)
            peer = lax.rem(me + step, n)
            source = sources[job]
            source = source if dim is None else piece(source, dim, size, peer)
            copy = send(job, step, source, targets[job].at[me], peer)
            if n == RELAYED and dim is None:
                hops.setdefault(job, []).append(copy)
            else:
                copies.append(copy)
    for job, (axis, n, dim, size) in enumerate(plan):
        if job in chained:
            continue
        me = lax.axis_index(axis)
        source = sources[job]
        copy = pltpu.make_async_copy(
            source if dim is None else piece(source, dim, size, me),
            targets[job].at[me],
            own_sem.at[job],
        )
        copy.start()
        copies.append(copy)
    for side in range(2):
        for job in relayed:
            axis, n, dim, size = plan[job]
            me = lax.axis_index(axis)
            right, left = lax.rem(me + 1, n), lax.rem(me + 3, n)
            onward, origin = (right, left) if side == 0 else (left, right)
            hops[job][side].wait_recv()
            landing = half(targets[job].at[origin], side)
            copies.append(send(job, 6 + side, landing, landing, onward))
    def link(job, way, owner, source):
        axis = plan[job][0]
        me = lax.axis_index(axis)
        slot = owner - 1 if way == 0 else owner
        return pltpu.make_async_remote_copy(
            src_ref=relays[job].at[way, slot] if source is None else source,
            dst_ref=relays[job].at[way, slot],
            send_sem=send_sem.at[job, 3 * way + slot],
            recv_sem=recv_sem.at[job, 3 * way + slot],
            device_id={axis: lax.rem(me + (1 if way == 0 else RELAYED - 1), RELAYED)},
            device_id_type=MESH,
        )

    def forward(job, way, owner, place):
        axis, n, dim, size = plan[job]
        mine = piece(sources[job], dim, size, owner)

        @pl.when(lax.axis_index(axis) == place)
        def _():
            if place == (0 if way == 0 else n - 1):
                link(job, way, owner, mine).start()
            else:
                copy = link(job, way, owner, None)
                copy.wait_recv()
                inbox = relays[job].at[way, owner - 1 if way == 0 else owner]
                total = inbox[...].astype(jnp.float32) + mine[...].astype(jnp.float32)
                inbox[...] = total.astype(inbox.dtype)
                copy.start()

    order = [(0, 3, 0), (1, 0, 3), (0, 2, 0), (1, 1, 3), (0, 1, 0), (1, 2, 3)]
    order += [(0, 3, 1), (1, 0, 2), (0, 2, 1), (1, 1, 2), (0, 3, 2), (1, 0, 1)]
    for way, owner, place in order:
        for job in chained:
            forward(job, way, owner, place)
    for job in chained:
        axis, n, dim, size = plan[job]
        for owner in range(n):

            @pl.when(lax.axis_index(axis) == owner)
            def _():
                total = piece(sources[job], dim, size, owner)[...].astype(jnp.float32)
                if owner > 0:
                    link(job, 0, owner, None).wait_recv()
                    total = total + relays[job][0, owner - 1].astype(jnp.float32)
                if owner < n - 1:
                    link(job, 1, owner, None).wait_recv()
                    total = total + relays[job][1, owner].astype(jnp.float32)
                targets[job][0] = total
                for other in range(n):
                    if other > owner:
                        link(job, 0, other, None).wait_send()
                    if other < owner:
                        link(job, 1, other, None).wait_send()

    for job in relayed:
        for copy in hops[job]:
            copy.wait_send()
    for copy in copies:
        copy.wait()


def exchange(jobs, collective_id):
    plan, shapes, relays = [], [], []
    for array, axis, dim in jobs:
        n = lax.axis_size(axis)
        block = list(array.shape)
        size = None
        if dim is not None:
            size = block[dim] = block[dim] // n
        plan.append((axis, n, dim, size))
        if n == RELAYED and dim is not None:
            shapes.append(jax.ShapeDtypeStruct((1,) + tuple(block), jnp.float32))
            relays.append(pltpu.VMEM((2, n - 1) + tuple(block), array.dtype))
        else:
            shapes.append(jax.ShapeDtypeStruct((n,) + tuple(block), array.dtype))
            relays.append(pltpu.VMEM((16, 128), array.dtype))
    most = max(2 * RELAYED, max(n for axis, n, dim, size in plan))
    count = len(jobs)
    in_vmem = pl.BlockSpec(memory_space=pltpu.VMEM)
    return pl.pallas_call(
        functools.partial(exchange_kernel, tuple(plan)),
        out_shape=shapes,
        in_specs=[in_vmem] * count,
        out_specs=[in_vmem] * count,
        scratch_shapes=[
            pltpu.SemaphoreType.DMA((count,)),
            pltpu.SemaphoreType.DMA((count, most)),
            pltpu.SemaphoreType.DMA((count, most)),
            *relays,
        ],
        compiler_params=pltpu.CompilerParams(
            collective_id=collective_id, has_side_effects=True, vmem_limit_bytes=48 * 2**20
        ),
        name=f"exchange_{collective_id}",
    )(*[array for array, axis, dim in jobs])


def dot_rows(left, right):
    return lax.dot_general(
        left, right, (((1,), (1,)), ((), ())), preferred_element_type=jnp.float32
    )


def dot_columns(left, right):
    return lax.dot_general(
        left, right, (((0,), (0,)), ((), ())), preferred_element_type=jnp.float32
    )


def attention_kernel(
    scale_ref, q_ref, k_ref, v_ref, g_ref, o_ref, dq_ref, dk_ref, dv_ref, dk_sum, dv_sum
):
    block = pl.program_id(1)
    scale = scale_ref[pl.program_id(0)]
    coeff = scale * (1.0 / q_ref.shape[1])
    query, keys, values, grad = q_ref[...], k_ref[...], v_ref[...], g_ref[...]
    weights = jnp.exp(dot_rows(query, keys) * coeff - scale)
    inverse = 1.0 / jnp.sum(weights, -1, keepdims=True)
    mixed = jnp.dot(weights.astype(jnp.bfloat16), values, preferred_element_type=jnp.float32)
    attended = (mixed * inverse).astype(jnp.bfloat16)
    o_ref[...] = attended
    delta = jnp.sum(
        grad.astype(jnp.float32) * attended.astype(jnp.float32), -1, keepdims=True
    )
    probs = weights * inverse
    dscores = (probs * (dot_rows(grad, values) - delta) * coeff).astype(jnp.bfloat16)
    dq_ref[...] = jnp.dot(dscores, keys, preferred_element_type=jnp.float32)
    dk_part = dot_columns(dscores, query)
    dv_part = dot_columns(probs.astype(jnp.bfloat16), grad)

    @pl.when(block == 0)
    def _():
        dk_sum[...] = dk_part
        dv_sum[...] = dv_part

    @pl.when(block > 0)
    def _():
        dk_sum[...] += dk_part
        dv_sum[...] += dv_part

    @pl.when(block == pl.num_programs(1) - 1)
    def _():
        dk_ref[...] = dk_sum[...].astype(dk_ref.dtype)
        dv_ref[...] = dv_sum[...].astype(dv_ref.dtype)


def attention(attn_scale, queries, keys_values, grads):
    heads = attn_scale.shape[0]
    span, inner = queries.shape
    length = keys_values.shape[0]
    head_dim = inner // heads
    size = math.gcd(span, 256)
    while size * length > 2**19 and size % 32 == 0:
        size //= 2
    mine = pl.BlockSpec((size, head_dim), lambda h, i: (i, h))
    keys = pl.BlockSpec((length, head_dim), lambda h, i: (0, h))
    values = pl.BlockSpec((length, head_dim), lambda h, i: (0, heads + h))
    return pl.pallas_call(
        attention_kernel,
        grid=(heads, span // size),
        out_shape=[
            jax.ShapeDtypeStruct((span, inner), jnp.bfloat16),
            jax.ShapeDtypeStruct((span, inner), jnp.float32),
            jax.ShapeDtypeStruct((length, inner), jnp.bfloat16),
            jax.ShapeDtypeStruct((length, inner), jnp.bfloat16),
        ],
        in_specs=[pl.BlockSpec(memory_space=pltpu.SMEM), mine, keys, values, mine],
        out_specs=[mine, mine, keys, keys],
        scratch_shapes=[pltpu.VMEM((length, head_dim), jnp.float32)] * 2,
        compiler_params=pltpu.CompilerParams(
            dimension_semantics=("arbitrary", "arbitrary"), vmem_limit_bytes=56 * 2**20
        ),
        name="attention",
    )(attn_scale, queries, keys_values, keys_values, grads)


def add_up(slots):
    return jnp.sum(slots.astype(jnp.float32), 0)


def per_device(tokens, timestep, mod_weight, qkv_weight, attn_scale, out_weight, grad_update):
    tok_dev, width = tokens.shape
    heads_here = attn_scale.shape[0]
    inner = qkv_weight.shape[2]
    head_dim = inner // heads_here
    span = tok_dev * lax.axis_size("col")
    embedded = embed(timestep, mod_weight.shape[0] // 2)
    gain = 1.0 + jnp.sum(embedded[:, None] * mod_weight, 0)
    tok_float = tokens.astype(jnp.float32)
    rstd = lax.rsqrt(jnp.mean(tok_float * tok_float, -1, keepdims=True) + epsilon)
    normed = tok_float * rstd
    hidden = (normed * gain).astype(jnp.bfloat16)
    (group,) = exchange([(hidden, "col", None)], 0)
    group = group.reshape(span, width)
    raw = [jnp.dot(group, qkv_weight[k], preferred_element_type=jnp.float32) for k in range(3)]
    query_unit, query_factor = zip(*[unit_rows(part) for part in by_head(raw[0], head_dim)])
    key_unit, key_factor = zip(*[unit_rows(part) for part in by_head(raw[1], head_dim)])
    queries = jnp.concatenate(query_unit, 1).astype(jnp.bfloat16)
    keys_values = jnp.concatenate(key_unit + (raw[2],), 1).astype(jnp.bfloat16)
    all_keys_values, grad_group = exchange(
        [(keys_values, "row", None), (grad_update, "col", None)], 1
    )
    all_keys_values = all_keys_values.reshape(-1, 2 * inner)
    grad_group = grad_group.reshape(span, width)
    grad_attended = dot_rows(grad_group, out_weight).astype(jnp.bfloat16)
    attended, grad_query, key_part, value_part = attention(
        attn_scale, queries, all_keys_values, grad_attended
    )
    update_part = jnp.dot(attended, out_weight, preferred_element_type=jnp.float32).astype(
        jnp.bfloat16
    )
    out_part = dot_columns(attended, grad_group).astype(jnp.bfloat16)
    key_slots, value_slots, update_slots = exchange(
        [(key_part, "row", 0), (value_part, "row", 0), (update_part, "col", 0)], 2
    )
    update = add_up(update_slots).astype(jnp.bfloat16)

    def raw_grads(grad_unit, unit, factor):
        parts = zip(by_head(grad_unit, head_dim), unit, factor)
        return jnp.concatenate([unit_grad(*part) for part in parts], 1).astype(jnp.bfloat16)

    grad_raw = [
        raw_grads(grad_query, query_unit, query_factor),
        raw_grads(add_up(key_slots), key_unit, key_factor),
        add_up(value_slots).astype(jnp.bfloat16),
    ]
    qkv_part = jnp.stack([dot_columns(group, part).astype(jnp.bfloat16) for part in grad_raw])
    hidden_part = (
        sum(dot_rows(part, qkv_weight[k]) for k, part in enumerate(grad_raw))
    ).astype(jnp.bfloat16)
    qkv_slots, hidden_slots, out_slots = exchange(
        [(qkv_part, "row", 1), (hidden_part, "col", 0), (out_part, "row", 1)], 3
    )
    grad_qkv = add_up(qkv_slots)
    grad_out = add_up(out_slots)
    grad_normed = add_up(hidden_slots) * gain
    grad_tokens = (
        rstd * (grad_normed - normed * jnp.mean(grad_normed * normed, -1, keepdims=True))
    ).astype(jnp.bfloat16)
    return (update, grad_tokens, grad_qkv, grad_out)


def flip(index, bit):
    return index + bit - 2 * bit * ((index // bit) % 2)


class Place:
    def __init__(self):
        self.row = lax.axis_index("row")
        self.col = lax.axis_index("col")
        self.partner = flip(self.col, 1)
        self.beside = flip(self.col, 2)
        self.across = flip(self.col, 4)
        self.corner = flip(self.beside, 4)
        self.inner = ((self.row + 1) // 2) % 2 == 1
        self.mate = flip(self.row, 1)
        self.facing = 3 - self.row
        low = 1 - self.row // 2
        self.ranks = [self.row, self.mate, 1 + low, 3 * low]

    def greet(self):
        barrier = pltpu.get_barrier_semaphore()
        for peer in (self.partner, self.beside, self.across, self.corner):
            pl.semaphore_signal(barrier, inc=1, device_id={"col": peer}, device_id_type=MESH)
        pl.semaphore_signal(barrier, inc=1, device_id={"row": self.mate}, device_id_type=MESH)

        @pl.when(self.inner)
        def _():
            pl.semaphore_signal(
                barrier, inc=1, device_id={"row": self.facing}, device_id_type=MESH
            )

        pl.semaphore_wait(barrier, 5 + ((self.row + 1) // 2) % 2)


KINDS = 9
LINE, BESIDE, ACROSS, TOP, BOTTOM, MATE = 0, 1, 2, 3, 4, 5
SENDS = 12


class Gather:
    def __init__(self, place, job, tile, whole, send_sem, recv_sem):
        self.place, self.job, self.tile, self.whole = place, job, tile, whole
        self.send_sem, self.recv_sem = send_sem, recv_sem

    def slot(self, rank, col):
        return self.whole.at[self.place.ranks[rank], col]

    def link(self, rank, kind, send, source, landing, peer):
        return pltpu.make_async_remote_copy(
            src_ref=source,
            dst_ref=landing,
            send_sem=self.send_sem.at[self.job, send[0], send[1]],
            recv_sem=self.recv_sem.at[self.job, rank, kind],
            device_id=peer,
            device_id_type=MESH,
        )

    def arrived(self, rank, kind, landing):
        self.link(rank, kind, (0, 0), landing, landing, {"col": self.place.partner}).wait_recv()

    def held(self, rank):
        return self.tile if rank == 0 else self.slot(rank, self.place.col)

    def line_sends(self, rank):
        p = self.place
        mine = self.slot(rank, p.col)
        held = self.held(rank)
        if rank == 0:
            outward = self.link(1, LINE, (0, 0), held, mine, {"row": p.mate})
            inward = self.link(2, LINE, (0, 1), held, mine, {"row": p.facing})
            return [(outward, False), (inward, True)]
        if rank == 1:
            return [(self.link(3, LINE, (1, 0), held, mine, {"row": p.facing}), True)]
        return [(self.link(rank, LINE, (rank, 0), held, mine, {"row": p.mate}), True)]

    def plane_sends(self, rank):
        p = self.place
        mine, held = self.slot(rank, p.col), self.held(rank)
        return [
            self.link(rank, BESIDE, (rank, 2), held, mine, {"col": p.beside}),
            self.link(rank, ACROSS, (rank, 3), held, mine, {"col": p.across}),
            self.link(rank, MATE, (rank, 4), held, mine, {"col": p.partner}),
        ]

    def relays(self, rank):
        p = self.place
        side, over = self.slot(rank, p.beside), self.slot(rank, p.across)
        return [
            self.link(rank, TOP, (rank, 5), half(side, 0), half(side, 0), {"col": p.across}),
            self.link(rank, MATE + 1, (rank, 6), side, side, {"col": p.partner}),
            self.link(rank, BOTTOM, (rank, 7), half(over, 1), half(over, 1), {"col": p.beside}),
            self.link(rank, MATE + 2, (rank, 8), over, over, {"col": p.partner}),
        ]

    def last(self, rank):
        p = self.place
        far = self.slot(rank, p.corner)
        return self.link(rank, MATE + 3, (rank, 9), far, far, {"col": p.partner})

    def each(self, copies, act):
        for copy, inner in copies:
            if inner:
                pl.when(self.place.inner)(functools.partial(act, copy))
            else:
                act(copy)

    def open(self, rank):
        p = self.place
        if rank == 0:
            self.whole[p.row, p.col] = self.tile[...]
        else:
            self.arrived(rank, LINE, self.slot(rank, p.col))
            self.each(self.line_sends(rank), lambda copy: copy.start())
        for copy in self.plane_sends(rank):
            copy.start()

    def relay(self, rank):
        p = self.place
        top, side, bottom, over = self.relays(rank)
        self.arrived(rank, BESIDE, self.slot(rank, p.beside))
        top.start()
        side.start()
        self.arrived(rank, ACROSS, self.slot(rank, p.across))
        bottom.start()
        over.start()

    def close(self, rank):
        p = self.place
        far = self.slot(rank, p.corner)
        self.arrived(rank, TOP, half(far, 0))
        self.arrived(rank, BOTTOM, half(far, 1))
        self.last(rank).start()

    def whole_rank(self, rank):
        p = self.place
        for kind, col in enumerate((p.col, p.beside, p.across, p.corner)):
            self.arrived(rank, MATE + kind, self.slot(rank, flip(col, 1)))

    def drain(self):
        for rank in range(4):
            self.each(self.line_sends(rank), lambda copy: copy.wait_send())
            for copy in self.plane_sends(rank) + self.relays(rank) + [self.last(rank)]:
                copy.wait_send()


class Scatter:
    def __init__(self, place, job, part, crossed, staged, landed, send_sem, recv_sem):
        self.place, self.job, self.part = place, job, part
        self.crossed, self.staged, self.landed = crossed, staged, landed
        self.send_sem, self.recv_sem = send_sem, recv_sem
        self.size = part.shape[0] // 8

    def targets(self):
        p = self.place
        return (p.corner, p.beside, p.across, p.col)

    def rows(self, col):
        return pl.ds(pl.multiple_of(col * self.size, 16), self.size)

    def core_send(self, at):
        p = self.place
        return pltpu.make_async_remote_copy(
            src_ref=self.part.at[self.rows(flip(self.targets()[at], 1))],
            dst_ref=self.crossed.at[self.job, at],
            send_sem=self.send_sem.at[self.job, at],
            recv_sem=self.recv_sem.at[self.job, at],
            device_id={"col": p.partner},
            device_id_type=MESH,
        )

    def chip_send(self, at):
        return pltpu.make_async_remote_copy(
            src_ref=self.staged.at[self.job, at],
            dst_ref=self.landed.at[self.job, at],
            send_sem=self.send_sem.at[self.job, 4 + at],
            recv_sem=self.recv_sem.at[self.job, 4 + at],
            device_id={"col": self.targets()[at]},
            device_id_type=MESH,
        )

    def chip_sum(self, at):
        mine = self.part[self.rows(self.targets()[at]), :].astype(jnp.float32)
        return mine + self.crossed[self.job, at].astype(jnp.float32)

    def first(self):
        for at in range(4):
            self.core_send(at).start()

    def second(self):
        for at in range(3):
            self.core_send(at).wait_recv()
            self.staged[self.job, at] = self.chip_sum(at).astype(self.staged.dtype)
            self.chip_send(at).start()

    def third(self):
        self.core_send(3).wait_recv()
        total = self.chip_sum(3)
        for at in (1, 2, 0):
            self.chip_send(at).wait_recv()
            total = total + self.landed[self.job, at].astype(jnp.float32)
        for at in range(4):
            self.core_send(at).wait_send()
        for at in range(3):
            self.chip_send(at).wait_send()
        return total


LOG2E = 1.4426950408889634


def dot(left, right):
    return jnp.dot(left, right, preferred_element_type=jnp.float32)


def fused_kernel(
    scale_ref, hidden_ref, grad_ref, qkv_ref, out_ref,
    update_ref, down_ref, grad_qkv_ref, grad_out_ref,
    hid_all, grad_all, raw_ref, q_ref, k_ref, kt_ref, v_ref, vt_ref, do_ref, w_ref,
    att_ref, dkt_ref, dvt_ref, gr_ref,
    part_ref, crossed, staged, landed, send_sem, recv_sem, send_sum, recv_sum,
):
    bf = jnp.bfloat16
    place = Place()
    rows, cols, tok_dev, width = hid_all.shape
    heads, length, hdim = q_ref.shape
    span = cols * tok_dev
    size = w_ref.shape[0]
    per_rank = span // size
    narrow = width // rows
    place.greet()
    hid = Gather(place, 0, hidden_ref, hid_all, send_sem, recv_sem)
    grd = Gather(place, 1, grad_ref, grad_all, send_sem, recv_sem)
    scatters = [
        Scatter(place, job, part_ref.at[job], crossed, staged, landed, send_sum, recv_sum)
        for job in range(2)
    ]

    def start_all(copies):
        hid.each(copies, lambda copy: copy.start())

    def tokens_at(rank, chunk):
        return pl.multiple_of(place.ranks[rank] * span + chunk * size, size)

    def chunk_of(whole, rank, chunk):
        step = size // tok_dev
        picked = whole[place.ranks[rank], pl.ds(chunk * step, step)]
        return picked.reshape(size, width)

    def project(rank):
        def body(chunk, carry):
            at = pl.ds(tokens_at(rank, chunk), size)
            here = chunk_of(hid_all, rank, chunk)
            for k in range(3):
                raw = dot(here, qkv_ref[k])
                for head, part in enumerate(by_head(raw, hdim)):
                    if k < 2:
                        raw_ref[k, head, at, :] = part
                        part = unit_rows(part)[0]
                    part = part.astype(bf)
                    if k == 0:
                        q_ref[head, at, :] = part
                    elif k == 1:
                        k_ref[head, at, :] = part
                        kt_ref[head, :, at] = part.T
                    else:
                        v_ref[head, at, pl.ds(0, hdim)] = part
                        vt_ref[head, pl.ds(0, hdim), at] = part.T
            return carry

        lax.fori_loop(0, per_rank, body, 0)

    def cotangent(rank):
        def body(chunk, carry):
            value = dot_rows(chunk_of(grad_all, rank, chunk), out_ref[...]).astype(bf)
            for head, part in enumerate(by_head(value, hdim)):
                do_ref[head, pl.ds(pl.multiple_of(chunk * size, size), size), :] = part
            return carry

        lax.fori_loop(0, per_rank, body, 0)

    wide = min(512, length)
    lane = lax.broadcasted_iota(jnp.int32, (size, hdim), 1)

    def attend(rank):
        def body(step, carry):
            head = step // per_rank
            chunk = step % per_rank
            at = pl.ds(tokens_at(rank, chunk), size)
            scale = scale_ref[head]
            coeff = scale * (1.0 / hdim)
            query = q_ref[head, at, :]
            grad = do_ref[head, pl.ds(pl.multiple_of(chunk * size, size), size), :]
            mixed = None
            for start in range(0, length, wide):
                scores = dot(query, kt_ref[head, :, pl.ds(start, wide)])
                weights = jnp.exp2(scores * (coeff * LOG2E)).astype(bf)
                w_ref[:, pl.ds(start, wide)] = weights
                more = dot(weights, v_ref[head, pl.ds(start, wide), :])
                mixed = more if mixed is None else mixed + more
            inverse = 1.0 / mixed[:, hdim : hdim + 1]
            attended = (mixed[:, :hdim] * inverse).astype(bf)
            att_ref[head, at, :] = attended
            grad_float = grad.astype(jnp.float32)
            delta = jnp.sum(grad_float * attended.astype(jnp.float32), -1, keepdims=True)
            high = delta.astype(bf).astype(jnp.float32)
            spare = jnp.where(lane == 0, -high, jnp.where(lane == 1, high - delta, 0.0))
            grad_more = jnp.concatenate([grad, spare.astype(bf)], 1)
            grad_turned = (grad_float * inverse).T.astype(bf)
            query_turned = (query.astype(jnp.float32) * (inverse * coeff)).T.astype(bf)
            grad_query = None
            for start in range(0, length, wide):
                here = pl.ds(start, wide)
                weights = w_ref[:, here]
                dprobs = dot(grad_more, vt_ref[head, :, here])
                dscores = weights * dprobs.astype(bf)
                more = dot(dscores, k_ref[head, here, :])
                grad_query = more if grad_query is None else grad_query + more
                dkt_ref[head, :, here] += dot(query_turned, dscores)
                dvt_ref[head, :, here] += dot(grad_turned, weights)
            unit, factor = unit_rows(raw_ref[0, head, at, :])
            gr_ref[0, head, at, :] = unit_grad(
                grad_query * (inverse * coeff), unit, factor
            ).astype(bf)
            return carry

        lax.fori_loop(0, heads * per_rank, body, 0)

    def finish_keys(rank):
        def body(step, carry):
            head = step // per_rank
            at = pl.ds(tokens_at(rank, step % per_rank), size)
            unit, factor = unit_rows(raw_ref[1, head, at, :])
            gr_ref[1, head, at, :] = unit_grad(dkt_ref[head, :, at].T, unit, factor).astype(bf)
            gr_ref[2, head, at, :] = dvt_ref[head, :, at].T.astype(bf)
            return carry

        lax.fori_loop(0, heads * per_rank, body, 0)

    own = pl.multiple_of(place.row * span, span)

    def project_out():
        def body(chunk, carry):
            at = pl.ds(pl.multiple_of(own + chunk * size, size), size)
            mine = jnp.concatenate([att_ref[head, at, :] for head in range(heads)], 1)
            part_ref[0, pl.ds(pl.multiple_of(chunk * size, size), size), :] = dot(
                mine, out_ref[...]
            ).astype(bf)
            return carry

        lax.fori_loop(0, per_rank, body, 0)

    def project_down():
        def body(chunk, carry):
            at = pl.ds(pl.multiple_of(own + chunk * size, size), size)
            total = None
            for k in range(3):
                mine = jnp.concatenate([gr_ref[k, head, at, :] for head in range(heads)], 1)
                more = dot_rows(mine, qkv_ref[k])
                total = more if total is None else total + more
            part_ref[1, pl.ds(pl.multiple_of(chunk * size, size), size), :] = total.astype(bf)
            return carry

        lax.fori_loop(0, per_rank, body, 0)

    def columns(whole, start, count):
        at = pl.multiple_of(place.row * narrow + start, 128)
        return whole[:, :, :, pl.ds(at, count)].reshape(length, count)

    def weight_grads():
        few = 128

        def body(step, carry):
            start = pl.multiple_of(step * few, few)
            turned = columns(hid_all, start, few).T
            for k in range(3):
                for head in range(heads):
                    grad_qkv_ref[k, pl.ds(start, few), pl.ds(head * hdim, hdim)] = dot(
                        turned, gr_ref[k, head]
                    )
            return carry

        lax.fori_loop(0, narrow // few, body, 0)

    def out_grads():
        for head in range(heads):
            turned = att_ref[head].T
            grad_out_ref[pl.ds(head * hdim, hdim), :] = dot(turned, columns(grad_all, 0, narrow))

    start_all(hid.line_sends(0))
    hid.open(0)
    v_ref[:, :, pl.ds(hdim, hdim)] = jnp.ones((heads, length, hdim), bf)
    vt_ref[:, pl.ds(hdim, hdim), :] = jnp.ones((heads, hdim, length), bf)
    dkt_ref[...] = jnp.zeros_like(dkt_ref)
    dvt_ref[...] = jnp.zeros_like(dvt_ref)
    hid.open(1)
    hid.relay(0)
    hid.open(2)
    start_all(grd.line_sends(0))
    hid.relay(1)
    hid.close(0)
    hid.whole_rank(0)
    project(0)
    hid.open(3)
    hid.relay(2)
    hid.close(1)
    hid.whole_rank(1)
    grd.open(0)
    project(1)
    hid.relay(3)
    hid.close(2)
    hid.whole_rank(2)
    grd.open(1)
    project(2)
    hid.close(3)
    hid.whole_rank(3)
    grd.relay(0)
    project(3)
    grd.open(2)
    grd.relay(1)
    grd.close(0)
    grd.whole_rank(0)
    cotangent(0)
    attend(0)
    grd.open(3)
    grd.relay(2)
    grd.close(1)
    grd.whole_rank(1)
    project_out()
    scatters[0].first()
    cotangent(1)
    attend(1)
    grd.relay(3)
    grd.close(2)
    grd.whole_rank(2)
    scatters[0].second()
    cotangent(2)
    attend(2)
    grd.close(3)
    grd.whole_rank(3)
    cotangent(3)
    attend(3)
    finish_keys(0)
    project_down()
    scatters[1].first()
    for rank in range(1, 4):
        finish_keys(rank)
    scatters[1].second()
    weight_grads()
    out_grads()
    update_ref[...] = scatters[0].third()
    down_ref[...] = scatters[1].third()
    hid.drain()
    grd.drain()


def fused(scale, hidden, grad_update, qkv_weight, out_weight):
    bf, f32 = jnp.bfloat16, jnp.float32
    tok_dev, width = hidden.shape
    heads = scale.shape[0]
    inner = qkv_weight.shape[2]
    hdim = inner // heads
    rows, cols = lax.axis_size("row"), lax.axis_size("col")
    span = tok_dev * cols
    length = span * rows
    size = math.gcd(span, 256)
    narrow = width // rows
    in_vmem = pl.BlockSpec(memory_space=pltpu.VMEM)
    return pl.pallas_call(
        fused_kernel,
        out_shape=[
            jax.ShapeDtypeStruct((tok_dev, width), f32),
            jax.ShapeDtypeStruct((tok_dev, width), f32),
            jax.ShapeDtypeStruct((3, narrow, inner), f32),
            jax.ShapeDtypeStruct((inner, narrow), f32),
        ],
        in_specs=[pl.BlockSpec(memory_space=pltpu.SMEM)] + [in_vmem] * 4,
        out_specs=[in_vmem] * 4,
        scratch_shapes=[
            pltpu.VMEM((rows, cols, tok_dev, width), bf),
            pltpu.VMEM((rows, cols, tok_dev, width), bf),
            pltpu.VMEM((2, heads, length, hdim), f32),
            pltpu.VMEM((heads, length, hdim), bf),
            pltpu.VMEM((heads, length, hdim), bf),
            pltpu.VMEM((heads, hdim, length), bf),
            pltpu.VMEM((heads, length, 2 * hdim), bf),
            pltpu.VMEM((heads, 2 * hdim, length), bf),
            pltpu.VMEM((heads, span, hdim), bf),
            pltpu.VMEM((size, length), bf),
            pltpu.VMEM((heads, length, hdim), bf),
            pltpu.VMEM((heads, hdim, length), f32),
            pltpu.VMEM((heads, hdim, length), f32),
            pltpu.VMEM((3, heads, length, hdim), bf),
            pltpu.VMEM((2, span, width), bf),
            pltpu.VMEM((2, 4, tok_dev, width), bf),
            pltpu.VMEM((2, 3, tok_dev, width), bf),
            pltpu.VMEM((2, 3, tok_dev, width), bf),
            pltpu.SemaphoreType.DMA((2, 4, SENDS)),
            pltpu.SemaphoreType.DMA((2, 4, KINDS)),
            pltpu.SemaphoreType.DMA((2, 8)),
            pltpu.SemaphoreType.DMA((2, 8)),
        ],
        compiler_params=pltpu.CompilerParams(
            collective_id=4, has_side_effects=True, vmem_limit_bytes=60 * 2**20
        ),
        name="fused",
    )(scale, hidden, grad_update, qkv_weight, out_weight)


def gathered(tokens, timestep, mod_weight, qkv_weight, attn_scale, out_weight, grad_update):
    embedded = embed(timestep, mod_weight.shape[0] // 2)
    gain = 1.0 + jnp.sum(embedded[:, None] * mod_weight, 0)
    tok_float = tokens.astype(jnp.float32)
    rstd = lax.rsqrt(jnp.mean(tok_float * tok_float, -1, keepdims=True) + epsilon)
    normed = tok_float * rstd
    hidden = (normed * gain).astype(jnp.bfloat16)
    update, grad_hidden, grad_qkv, grad_out = fused(
        attn_scale, hidden, grad_update, qkv_weight, out_weight
    )
    grad_normed = grad_hidden * gain
    grad_tokens = (
        rstd * (grad_normed - normed * jnp.mean(grad_normed * normed, -1, keepdims=True))
    ).astype(jnp.bfloat16)
    return (update.astype(jnp.bfloat16), grad_tokens, grad_qkv, grad_out)


def solution(mesh):
    placed = (
        P(("row", "col"), None),
        P(),
        P(),
        P(None, None, "col"),
        P("col"),
        P("col", None),
        P(("row", "col"), None),
    )
    plane = mesh.shape["row"] == 4 and mesh.shape["col"] == 8
    return jax.shard_map(
        gathered if plane else per_device,
        mesh=mesh,
        in_specs=placed,
        out_specs=(
            P(("row", "col"), None),
            P(("row", "col"), None),
            P(None, "row", "col"),
            P("col", "row"),
        ),
        check_vma=False,
    )
```

```python
import functools
import math

import jax
import jax.numpy as jnp
from jax import lax
from jax.experimental import pallas as pl
from jax.experimental.pallas import tpu as pltpu
from jax.sharding import PartitionSpec as P

epsilon = 1e-06
MESH = pl.DeviceIdType.MESH
RELAYED = 4


def embed(timestep, count):
    index = jnp.arange(count, dtype=jnp.float32)
    freqs = jnp.exp(-math.log(10000.0) * index / count)
    angles = timestep.astype(jnp.float32)[0] * freqs
    return jnp.concatenate([jnp.cos(angles), jnp.sin(angles)])


def by_head(array, head_dim):
    return [array[:, at : at + head_dim] for at in range(0, array.shape[1], head_dim)]


def unit_rows(values):
    factor = lax.rsqrt(jnp.mean(values * values, -1, keepdims=True) + epsilon)
    return (values * factor, factor)


def unit_grad(grad_unit, unit, factor):
    return factor * (grad_unit - unit * jnp.mean(grad_unit * unit, -1, keepdims=True))


def piece(ref, dim, size, index):
    start = index * size
    if isinstance(start, int):
        pass
    elif dim == len(ref.shape) - 1:
        start = pl.multiple_of(start, 128)
    elif dim == len(ref.shape) - 2:
        start = pl.multiple_of(start, 16)
    return ref.at[(slice(None),) * dim + (pl.ds(start, size),)]


def half(ref, side):
    dim = len(ref.shape) - 2
    size = ref.shape[dim] // 2
    return ref.at[(slice(None),) * dim + (pl.ds(side * size, size),)]


def exchange_kernel(plan, *refs):
    count = len(plan)
    sources, targets = refs[:count], refs[count : 2 * count]
    own_sem, send_sem, recv_sem = refs[2 * count : 2 * count + 3]
    relays = refs[2 * count + 3 :]
    sizes = {axis: n for axis, n, dim, size in plan}
    barrier = pltpu.get_barrier_semaphore()
    for axis, n in sizes.items():
        me = lax.axis_index(axis)
        for step in range(1, n):
            pl.semaphore_signal(
                barrier, inc=1, device_id={axis: lax.rem(me + step, n)}, device_id_type=MESH
            )
    pl.semaphore_wait(barrier, sum(n - 1 for n in sizes.values()))
    def send(job, slot, source, target, peer):
        copy = pltpu.make_async_remote_copy(
            src_ref=source,
            dst_ref=target,
            send_sem=send_sem.at[job, slot],
            recv_sem=recv_sem.at[job, slot],
            device_id={plan[job][0]: peer},
            device_id_type=MESH,
        )
        copy.start()
        return copy

    copies, hops = [], {}
    chained = [job for job in range(count) if plan[job][1] == RELAYED and plan[job][2] is not None]
    relayed = [job for job in range(count) if plan[job][1] == RELAYED and job not in chained]
    for step in range(1, max(sizes.values())):
        for job, (axis, n, dim, size) in enumerate(plan):
            if step >= n or job in chained or (n == RELAYED and step == 2):
                continue
            me = lax.axis_index(axis)
            peer = lax.rem(me + step, n)
            source = sources[job]
            source = source if dim is None else piece(source, dim, size, peer)
            copy = send(job, step, source, targets[job].at[me], peer)
            if n == RELAYED and dim is None:
                hops.setdefault(job, []).append(copy)
            else:
                copies.append(copy)
    for job, (axis, n, dim, size) in enumerate(plan):
        if job in chained:
            continue
        me = lax.axis_index(axis)
        source = sources[job]
        copy = pltpu.make_async_copy(
            source if dim is None else piece(source, dim, size, me),
            targets[job].at[me],
            own_sem.at[job],
        )
        copy.start()
        copies.append(copy)
    for side in range(2):
        for job in relayed:
            axis, n, dim, size = plan[job]
            me = lax.axis_index(axis)
            right, left = lax.rem(me + 1, n), lax.rem(me + 3, n)
            onward, origin = (right, left) if side == 0 else (left, right)
            hops[job][side].wait_recv()
            landing = half(targets[job].at[origin], side)
            copies.append(send(job, 6 + side, landing, landing, onward))
    def link(job, way, owner, source):
        axis = plan[job][0]
        me = lax.axis_index(axis)
        slot = owner - 1 if way == 0 else owner
        return pltpu.make_async_remote_copy(
            src_ref=relays[job].at[way, slot] if source is None else source,
            dst_ref=relays[job].at[way, slot],
            send_sem=send_sem.at[job, 3 * way + slot],
            recv_sem=recv_sem.at[job, 3 * way + slot],
            device_id={axis: lax.rem(me + (1 if way == 0 else RELAYED - 1), RELAYED)},
            device_id_type=MESH,
        )

    def forward(job, way, owner, place):
        axis, n, dim, size = plan[job]
        mine = piece(sources[job], dim, size, owner)

        @pl.when(lax.axis_index(axis) == place)
        def _():
            if place == (0 if way == 0 else n - 1):
                link(job, way, owner, mine).start()
            else:
                copy = link(job, way, owner, None)
                copy.wait_recv()
                inbox = relays[job].at[way, owner - 1 if way == 0 else owner]
                total = inbox[...].astype(jnp.float32) + mine[...].astype(jnp.float32)
                inbox[...] = total.astype(inbox.dtype)
                copy.start()

    order = [(0, 3, 0), (1, 0, 3), (0, 2, 0), (1, 1, 3), (0, 1, 0), (1, 2, 3)]
    order += [(0, 3, 1), (1, 0, 2), (0, 2, 1), (1, 1, 2), (0, 3, 2), (1, 0, 1)]
    for way, owner, place in order:
        for job in chained:
            forward(job, way, owner, place)
    for job in chained:
        axis, n, dim, size = plan[job]
        for owner in range(n):

            @pl.when(lax.axis_index(axis) == owner)
            def _():
                total = piece(sources[job], dim, size, owner)[...].astype(jnp.float32)
                if owner > 0:
                    link(job, 0, owner, None).wait_recv()
                    total = total + relays[job][0, owner - 1].astype(jnp.float32)
                if owner < n - 1:
                    link(job, 1, owner, None).wait_recv()
                    total = total + relays[job][1, owner].astype(jnp.float32)
                targets[job][0] = total
                for other in range(n):
                    if other > owner:
                        link(job, 0, other, None).wait_send()
                    if other < owner:
                        link(job, 1, other, None).wait_send()

    for job in relayed:
        for copy in hops[job]:
            copy.wait_send()
    for copy in copies:
        copy.wait()


def exchange(jobs, collective_id):
    plan, shapes, relays = [], [], []
    for array, axis, dim in jobs:
        n = lax.axis_size(axis)
        block = list(array.shape)
        size = None
        if dim is not None:
            size = block[dim] = block[dim] // n
        plan.append((axis, n, dim, size))
        if n == RELAYED and dim is not None:
            shapes.append(jax.ShapeDtypeStruct((1,) + tuple(block), jnp.float32))
            relays.append(pltpu.VMEM((2, n - 1) + tuple(block), array.dtype))
        else:
            shapes.append(jax.ShapeDtypeStruct((n,) + tuple(block), array.dtype))
            relays.append(pltpu.VMEM((16, 128), array.dtype))
    most = max(2 * RELAYED, max(n for axis, n, dim, size in plan))
    count = len(jobs)
    in_vmem = pl.BlockSpec(memory_space=pltpu.VMEM)
    return pl.pallas_call(
        functools.partial(exchange_kernel, tuple(plan)),
        out_shape=shapes,
        in_specs=[in_vmem] * count,
        out_specs=[in_vmem] * count,
        scratch_shapes=[
            pltpu.SemaphoreType.DMA((count,)),
            pltpu.SemaphoreType.DMA((count, most)),
            pltpu.SemaphoreType.DMA((count, most)),
            *relays,
        ],
        compiler_params=pltpu.CompilerParams(
            collective_id=collective_id, has_side_effects=True, vmem_limit_bytes=48 * 2**20
        ),
        name=f"exchange_{collective_id}",
    )(*[array for array, axis, dim in jobs])


def dot_rows(left, right):
    return lax.dot_general(
        left, right, (((1,), (1,)), ((), ())), preferred_element_type=jnp.float32
    )


def dot_columns(left, right):
    return lax.dot_general(
        left, right, (((0,), (0,)), ((), ())), preferred_element_type=jnp.float32
    )


def attention_kernel(
    scale_ref, q_ref, k_ref, v_ref, g_ref, o_ref, dq_ref, dk_ref, dv_ref, dk_sum, dv_sum
):
    block = pl.program_id(1)
    scale = scale_ref[pl.program_id(0)]
    coeff = scale * (1.0 / q_ref.shape[1])
    query, keys, values, grad = q_ref[...], k_ref[...], v_ref[...], g_ref[...]
    weights = jnp.exp(dot_rows(query, keys) * coeff - scale)
    inverse = 1.0 / jnp.sum(weights, -1, keepdims=True)
    mixed = jnp.dot(weights.astype(jnp.bfloat16), values, preferred_element_type=jnp.float32)
    attended = (mixed * inverse).astype(jnp.bfloat16)
    o_ref[...] = attended
    delta = jnp.sum(
        grad.astype(jnp.float32) * attended.astype(jnp.float32), -1, keepdims=True
    )
    probs = weights * inverse
    dscores = (probs * (dot_rows(grad, values) - delta) * coeff).astype(jnp.bfloat16)
    dq_ref[...] = jnp.dot(dscores, keys, preferred_element_type=jnp.float32)
    dk_part = dot_columns(dscores, query)
    dv_part = dot_columns(probs.astype(jnp.bfloat16), grad)

    @pl.when(block == 0)
    def _():
        dk_sum[...] = dk_part
        dv_sum[...] = dv_part

    @pl.when(block > 0)
    def _():
        dk_sum[...] += dk_part
        dv_sum[...] += dv_part

    @pl.when(block == pl.num_programs(1) - 1)
    def _():
        dk_ref[...] = dk_sum[...].astype(dk_ref.dtype)
        dv_ref[...] = dv_sum[...].astype(dv_ref.dtype)


def attention(attn_scale, queries, keys_values, grads):
    heads = attn_scale.shape[0]
    span, inner = queries.shape
    length = keys_values.shape[0]
    head_dim = inner // heads
    size = math.gcd(span, 256)
    while size * length > 2**19 and size % 32 == 0:
        size //= 2
    mine = pl.BlockSpec((size, head_dim), lambda h, i: (i, h))
    keys = pl.BlockSpec((length, head_dim), lambda h, i: (0, h))
    values = pl.BlockSpec((length, head_dim), lambda h, i: (0, heads + h))
    return pl.pallas_call(
        attention_kernel,
        grid=(heads, span // size),
        out_shape=[
            jax.ShapeDtypeStruct((span, inner), jnp.bfloat16),
            jax.ShapeDtypeStruct((span, inner), jnp.float32),
            jax.ShapeDtypeStruct((length, inner), jnp.bfloat16),
            jax.ShapeDtypeStruct((length, inner), jnp.bfloat16),
        ],
        in_specs=[pl.BlockSpec(memory_space=pltpu.SMEM), mine, keys, values, mine],
        out_specs=[mine, mine, keys, keys],
        scratch_shapes=[pltpu.VMEM((length, head_dim), jnp.float32)] * 2,
        compiler_params=pltpu.CompilerParams(
            dimension_semantics=("arbitrary", "arbitrary"), vmem_limit_bytes=56 * 2**20
        ),
        name="attention",
    )(attn_scale, queries, keys_values, keys_values, grads)


def add_up(slots):
    return jnp.sum(slots.astype(jnp.float32), 0)


def per_device(tokens, timestep, mod_weight, qkv_weight, attn_scale, out_weight, grad_update):
    tok_dev, width = tokens.shape
    heads_here = attn_scale.shape[0]
    inner = qkv_weight.shape[2]
    head_dim = inner // heads_here
    span = tok_dev * lax.axis_size("col")
    embedded = embed(timestep, mod_weight.shape[0] // 2)
    gain = 1.0 + jnp.sum(embedded[:, None] * mod_weight, 0)
    tok_float = tokens.astype(jnp.float32)
    rstd = lax.rsqrt(jnp.mean(tok_float * tok_float, -1, keepdims=True) + epsilon)
    normed = tok_float * rstd
    hidden = (normed * gain).astype(jnp.bfloat16)
    (group,) = exchange([(hidden, "col", None)], 0)
    group = group.reshape(span, width)
    raw = [jnp.dot(group, qkv_weight[k], preferred_element_type=jnp.float32) for k in range(3)]
    query_unit, query_factor = zip(*[unit_rows(part) for part in by_head(raw[0], head_dim)])
    key_unit, key_factor = zip(*[unit_rows(part) for part in by_head(raw[1], head_dim)])
    queries = jnp.concatenate(query_unit, 1).astype(jnp.bfloat16)
    keys_values = jnp.concatenate(key_unit + (raw[2],), 1).astype(jnp.bfloat16)
    all_keys_values, grad_group = exchange(
        [(keys_values, "row", None), (grad_update, "col", None)], 1
    )
    all_keys_values = all_keys_values.reshape(-1, 2 * inner)
    grad_group = grad_group.reshape(span, width)
    grad_attended = dot_rows(grad_group, out_weight).astype(jnp.bfloat16)
    attended, grad_query, key_part, value_part = attention(
        attn_scale, queries, all_keys_values, grad_attended
    )
    update_part = jnp.dot(attended, out_weight, preferred_element_type=jnp.float32).astype(
        jnp.bfloat16
    )
    out_part = dot_columns(attended, grad_group).astype(jnp.bfloat16)
    key_slots, value_slots, update_slots = exchange(
        [(key_part, "row", 0), (value_part, "row", 0), (update_part, "col", 0)], 2
    )
    update = add_up(update_slots).astype(jnp.bfloat16)

    def raw_grads(grad_unit, unit, factor):
        parts = zip(by_head(grad_unit, head_dim), unit, factor)
        return jnp.concatenate([unit_grad(*part) for part in parts], 1).astype(jnp.bfloat16)

    grad_raw = [
        raw_grads(grad_query, query_unit, query_factor),
        raw_grads(add_up(key_slots), key_unit, key_factor),
        add_up(value_slots).astype(jnp.bfloat16),
    ]
    qkv_part = jnp.stack([dot_columns(group, part).astype(jnp.bfloat16) for part in grad_raw])
    hidden_part = (
        sum(dot_rows(part, qkv_weight[k]) for k, part in enumerate(grad_raw))
    ).astype(jnp.bfloat16)
    qkv_slots, hidden_slots, out_slots = exchange(
        [(qkv_part, "row", 1), (hidden_part, "col", 0), (out_part, "row", 1)], 3
    )
    grad_qkv = add_up(qkv_slots)
    grad_out = add_up(out_slots)
    grad_normed = add_up(hidden_slots) * gain
    grad_tokens = (
        rstd * (grad_normed - normed * jnp.mean(grad_normed * normed, -1, keepdims=True))
    ).astype(jnp.bfloat16)
    return (update, grad_tokens, grad_qkv, grad_out)


def flip(index, bit):
    return index + bit - 2 * bit * ((index // bit) % 2)


class Place:
    def __init__(self):
        self.row = lax.axis_index("row")
        self.col = lax.axis_index("col")
        self.partner = flip(self.col, 1)
        self.beside = flip(self.col, 2)
        self.across = flip(self.col, 4)
        self.corner = flip(self.beside, 4)
        self.inner = ((self.row + 1) // 2) % 2 == 1
        self.mate = flip(self.row, 1)
        self.facing = 3 - self.row
        low = 1 - self.row // 2
        self.ranks = [self.row, self.mate, 1 + low, 3 * low]

    def greet(self):
        barrier = pltpu.get_barrier_semaphore()
        for peer in (self.partner, self.beside, self.across, self.corner):
            pl.semaphore_signal(barrier, inc=1, device_id={"col": peer}, device_id_type=MESH)
        for peer in self.ranks[1:]:
            pl.semaphore_signal(barrier, inc=1, device_id={"row": peer}, device_id_type=MESH)

    def await_greetings(self):
        pl.semaphore_wait(pltpu.get_barrier_semaphore(), 7)


KINDS = 9
LINE, BESIDE, ACROSS, TOP, BOTTOM, MATE = 0, 1, 2, 3, 4, 5
SENDS = 12


class Gather:
    def __init__(self, place, job, tile, whole, send_sem, recv_sem):
        self.place, self.job, self.tile, self.whole = place, job, tile, whole
        self.send_sem, self.recv_sem = send_sem, recv_sem

    def slot(self, rank, col):
        return self.whole.at[self.place.ranks[rank], col]

    def link(self, rank, kind, send, source, landing, peer):
        return pltpu.make_async_remote_copy(
            src_ref=source,
            dst_ref=landing,
            send_sem=self.send_sem.at[self.job, send[0], send[1]],
            recv_sem=self.recv_sem.at[self.job, rank, kind],
            device_id=peer,
            device_id_type=MESH,
        )

    def arrived(self, rank, kind, landing):
        self.link(rank, kind, (0, 0), landing, landing, {"col": self.place.partner}).wait_recv()

    def held(self, rank):
        return self.tile if rank == 0 else self.slot(rank, self.place.col)

    def line_sends(self, rank):
        p = self.place
        mine = self.slot(rank, p.col)
        held = self.held(rank)
        if rank == 0:
            outward = self.link(1, LINE, (0, 0), held, mine, {"row": p.mate})
            inward = self.link(2, LINE, (0, 1), held, mine, {"row": p.facing})
            return [(outward, False), (inward, True)]
        if rank == 1:
            return [(self.link(3, LINE, (1, 0), held, mine, {"row": p.facing}), True)]
        return [(self.link(rank, LINE, (rank, 0), held, mine, {"row": p.mate}), True)]

    def plane_sends(self, rank):
        p = self.place
        mine, held = self.slot(rank, p.col), self.held(rank)
        return [
            self.link(rank, BESIDE, (rank, 2), held, mine, {"col": p.beside}),
            self.link(rank, ACROSS, (rank, 3), held, mine, {"col": p.across}),
            self.link(rank, MATE, (rank, 4), held, mine, {"col": p.partner}),
        ]

    def relays(self, rank):
        p = self.place
        side, over = self.slot(rank, p.beside), self.slot(rank, p.across)
        return [
            self.link(rank, TOP, (rank, 5), half(side, 0), half(side, 0), {"col": p.across}),
            self.link(rank, MATE + 1, (rank, 6), side, side, {"col": p.partner}),
            self.link(rank, BOTTOM, (rank, 7), half(over, 1), half(over, 1), {"col": p.beside}),
            self.link(rank, MATE + 2, (rank, 8), over, over, {"col": p.partner}),
        ]

    def last(self, rank):
        p = self.place
        far = self.slot(rank, p.corner)
        return self.link(rank, MATE + 3, (rank, 9), far, far, {"col": p.partner})

    def each(self, copies, act):
        for copy, inner in copies:
            if inner:
                pl.when(self.place.inner)(functools.partial(act, copy))
            else:
                act(copy)

    def pass_on(self, rank):
        self.arrived(rank, LINE, self.slot(rank, self.place.col))
        self.each(self.line_sends(rank), lambda copy: copy.start())

    def spread(self, rank):
        for copy in self.plane_sends(rank):
            copy.start()

    def relay(self, rank):
        p = self.place
        top, side, bottom, over = self.relays(rank)
        self.arrived(rank, BESIDE, self.slot(rank, p.beside))
        top.start()
        side.start()
        self.arrived(rank, ACROSS, self.slot(rank, p.across))
        bottom.start()
        over.start()

    def close(self, rank):
        p = self.place
        far = self.slot(rank, p.corner)
        self.arrived(rank, TOP, half(far, 0))
        self.arrived(rank, BOTTOM, half(far, 1))
        self.last(rank).start()

    def whole_rank(self, rank):
        p = self.place
        for kind, col in enumerate((p.col, p.beside, p.across, p.corner)):
            self.arrived(rank, MATE + kind, self.slot(rank, flip(col, 1)))

    def drain_line(self):
        for rank in range(4):
            self.each(self.line_sends(rank), lambda copy: copy.wait_send())

    def drain_plane(self, rank):
        for copy in self.plane_sends(rank) + self.relays(rank) + [self.last(rank)]:
            copy.wait_send()


class Level(Gather):
    def slot(self, rank, col):
        return self.whole.at[col]


class Line(Gather):
    def slot(self, rank, col):
        return self.whole.at[self.place.ranks[rank]]


class Slices(Gather):
    def cuts(self):
        p = self.place
        size = self.whole.shape[3]
        copies = []
        for at, peer in enumerate(p.ranks[1:]):
            mine = pl.ds(pl.multiple_of(peer * size, 128), size)
            copies.append(
                pltpu.make_async_remote_copy(
                    src_ref=self.tile.at[:, mine],
                    dst_ref=self.slot(0, p.col),
                    send_sem=self.send_sem.at[self.job, at, 0],
                    recv_sem=self.recv_sem.at[self.job, p.row, LINE],
                    device_id={"row": peer},
                    device_id_type=MESH,
                )
            )
        return copies

    def landed(self, rank):
        p = self.place
        slot = self.slot(rank, p.col)
        pltpu.make_async_remote_copy(
            src_ref=slot,
            dst_ref=slot,
            send_sem=self.send_sem.at[self.job, 0, 0],
            recv_sem=self.recv_sem.at[self.job, p.ranks[rank], LINE],
            device_id={"col": p.partner},
            device_id_type=MESH,
        ).wait_recv()

    def held(self, rank):
        return self.slot(rank, self.place.col)


class Scatter:
    def __init__(self, place, job, part, crossed, landed, send_sem, recv_sem):
        self.place, self.job, self.part = place, job, part
        self.crossed, self.landed = crossed, landed
        self.send_sem, self.recv_sem = send_sem, recv_sem
        self.size = part.shape[0] // 8

    def targets(self):
        p = self.place
        return (p.corner, p.beside, p.across, p.col)

    def rows(self, col):
        return pl.ds(pl.multiple_of(col * self.size, 16), self.size)

    def core_send(self, at):
        p = self.place
        return pltpu.make_async_remote_copy(
            src_ref=self.part.at[self.rows(flip(self.targets()[at], 1))],
            dst_ref=self.crossed.at[self.job, at],
            send_sem=self.send_sem.at[self.job, at],
            recv_sem=self.recv_sem.at[self.job, at],
            device_id={"col": p.partner},
            device_id_type=MESH,
        )

    def chip_send(self, at):
        return pltpu.make_async_remote_copy(
            src_ref=self.part.at[self.rows(self.targets()[at])],
            dst_ref=self.landed.at[self.job, at],
            send_sem=self.send_sem.at[self.job, 4 + at],
            recv_sem=self.recv_sem.at[self.job, 4 + at],
            device_id={"col": self.targets()[at]},
            device_id_type=MESH,
        )

    def chip_sum(self, at):
        mine = self.part[self.rows(self.targets()[at]), :].astype(jnp.float32)
        return mine + self.crossed[self.job, at].astype(jnp.float32)

    def first(self):
        for at in range(4):
            self.core_send(at).start()

    def second(self):
        for at in range(3):
            self.core_send(at).wait_recv()
            self.part[self.rows(self.targets()[at]), :] = self.chip_sum(at).astype(self.part.dtype)
            self.chip_send(at).start()

    def third(self):
        self.core_send(3).wait_recv()
        total = self.chip_sum(3)
        for at in (1, 2, 0):
            self.chip_send(at).wait_recv()
            total = total + self.landed[self.job, at].astype(jnp.float32)
        for at in range(4):
            self.core_send(at).wait_send()
        for at in range(3):
            self.chip_send(at).wait_send()
        return total


LOG2E = 1.4426950408889634


def dot(left, right):
    return jnp.dot(left, right, preferred_element_type=jnp.float32)


def fused_kernel(
    scale_ref, embed_ref, tok_ref, grad_ref, mod_hbm, qkv_hbm, out_hbm,
    update_ref, grad_tok_ref, grad_qkv_ref, grad_out_ref,
    hidden_ref, gain_ref, qkv_ref, out_ref, load_sem, hid_all, grad_level, grad_cut, do_all, raw_ref, q_ref, qt_ref, k_ref, kt_ref, v_ref, vt_ref,
    w_ref, inv_ref, own_ref, att_ref, dot_ref, dkt_ref, dvt_ref, gr_ref,
    part_ref, crossed, landed, send_sem, recv_sem, send_sum, recv_sum,
):
    bf = jnp.bfloat16
    place = Place()
    rows, cols, tok_dev, width = hid_all.shape
    heads, length, hdim = q_ref.shape
    span = cols * tok_dev
    size = math.gcd(span, 256)
    per_rank = span // size
    narrow = width // rows
    dog_ref = v_ref
    mod_loads = [
        pltpu.make_async_copy(
            mod_hbm.at[pl.ds(head * hdim, hdim)], dkt_ref.at[head], load_sem.at[2 + head]
        )
        for head in range(heads)
    ]
    loads = [
        pltpu.make_async_copy(qkv_hbm, qkv_ref, load_sem.at[0]),
        pltpu.make_async_copy(out_hbm, out_ref, load_sem.at[1]),
    ]
    for load in mod_loads + loads:
        load.start()
    place.greet()
    gain = 1.0
    for head, load in enumerate(mod_loads):
        load.wait()
        here = embed_ref[pl.ds(head * hdim, hdim), :] * dkt_ref[head]
        gain = gain + jnp.sum(here, 0, keepdims=True)
    gain_ref[...] = jnp.broadcast_to(gain, gain_ref.shape)

    def normed_rows():
        tok_float = tok_ref[...].astype(jnp.float32)
        rstd = lax.rsqrt(jnp.mean(tok_float * tok_float, -1, keepdims=True) + epsilon)
        return tok_float * rstd, rstd

    hidden_ref[...] = (normed_rows()[0] * gain_ref[0:1, :]).astype(bf)
    place.await_greetings()
    hid = Gather(place, 0, hidden_ref, hid_all, send_sem, recv_sem)
    grd = Level(place, 1, grad_ref, grad_level, send_sem, recv_sem)
    cut = Slices(place, 2, grad_ref, grad_cut, send_sem, recv_sem)
    dol = Line(place, 3, do_all.at[place.row], do_all, send_sem, recv_sem)
    scatters = [
        Scatter(place, job, part_ref, crossed, landed, send_sum, recv_sum) for job in range(2)
    ]

    def start_all(copies):
        hid.each(copies, lambda copy: copy.start())

    def tokens_at(rank, chunk):
        return pl.multiple_of(place.ranks[rank] * span + chunk * size, size)

    def within(chunk):
        return pl.ds(pl.multiple_of(chunk * size, size), size)

    def steps(count, body):
        def step(at, carry):
            body(at)
            return carry

        lax.fori_loop(0, count, step, 0)

    def blocks(body):
        steps(heads * per_rank, lambda at: body(at // per_rank, at % per_rank))

    few = size // tok_dev

    def project(rank):
        def body(chunk):
            at = pl.ds(tokens_at(rank, chunk), size)
            here = hid_all[place.ranks[rank], pl.ds(chunk * few, few)].reshape(size, width)
            for k in range(3):
                raw = dot(here, qkv_ref[k])
                for head, part in enumerate(by_head(raw, hdim)):
                    if k < 2:
                        raw_ref[k, head, at, :] = part.astype(bf)
                        part = unit_rows(part)[0]
                    part = part.astype(bf)
                    if k == 0:
                        q_ref[head, at, :] = part
                        qt_ref[head, :, at] = part.T
                    elif k == 1:
                        k_ref[head, at, :] = part
                        kt_ref[head, :, at] = part.T
                    else:
                        v_ref[head, at, pl.ds(0, hdim)] = part
                        vt_ref[head, pl.ds(0, hdim), at] = part.T

        steps(per_rank, body)

    def cotangent():
        def body(chunk):
            here = grad_level[pl.ds(chunk * few, few)].reshape(size, width)
            value = dot_rows(here, out_ref[...]).astype(bf)
            for head, part in enumerate(by_head(value, hdim)):
                do_all[place.row, head, within(chunk), :] = part

        steps(per_rank, body)

    wide = min(512, span)

    def forward(rank):
        def body(head, chunk):
            at = pl.ds(tokens_at(rank, chunk), size)
            coeff = scale_ref[head] * (LOG2E / hdim)
            query = q_ref[head, at, :]
            mixed = None
            for start in range(0, length, wide):
                here = pl.ds(start, wide)
                weights = jnp.exp2(dot(query, kt_ref[head, :, here]) * coeff).astype(bf)
                w_ref[head, at, here] = weights
                more = dot(weights, v_ref[head, here, :])
                mixed = more if mixed is None else mixed + more
            inverse = 1.0 / mixed[:, hdim:]
            attended = (mixed[:, :hdim] * inverse).astype(bf)
            if rank == 0:
                own_ref[head, within(chunk), :] = attended
            att_ref[head, :, at] = attended.T
            inv_ref[head, :, at] = inverse.T[:8]

        blocks(body)

    def prepare(rank):
        def body(head, chunk):
            at = pl.ds(tokens_at(rank, chunk), size)
            turned = do_all[place.ranks[rank], head, within(chunk), :].T.astype(jnp.float32)
            delta = jnp.sum(turned * att_ref[head, :, at].astype(jnp.float32), 0, keepdims=True)
            inverse = inv_ref[head, 0:1, at]
            turned = turned * inverse
            dot_ref[head, :, at] = turned.astype(bf)
            delta = jnp.broadcast_to(delta * inverse, (hdim, size))
            high = delta.astype(bf).astype(jnp.float32)
            line = lax.broadcasted_iota(jnp.int32, (hdim, size), 0)
            spare = jnp.where(line == 0, -high, jnp.where(line == 1, high - delta, 0.0))
            dog_ref[head, at, :] = jnp.concatenate([turned, spare], 0).astype(bf).T

        blocks(body)

    def backward(rank, fresh, stored=()):
        def body(head, chunk):
            at = pl.ds(tokens_at(rank, chunk), size)
            coeff = scale_ref[head] * (1.0 / hdim)
            whole = len(fresh) + len(stored) == rows
            grad_more = dog_ref[head, at, :]
            grad_turned = dot_ref[head, :, at]
            query_turned = qt_ref[head, :, at]
            grad_query = None
            for key_rank in stored + fresh:
                first = pl.multiple_of(place.ranks[key_rank] * span, span)
                for start in range(0, span, wide):
                    here = pl.ds(pl.multiple_of(first + start, wide), wide)
                    weights = w_ref[head, at, here]
                    if key_rank in fresh:
                        dprobs = dot(grad_more, vt_ref[head, :, here])
                        dscores = weights * dprobs.astype(bf)
                        dkt_ref[head, :, here] += dot(query_turned, dscores)
                        dvt_ref[head, :, here] += dot(grad_turned, weights)
                        if not whole:
                            w_ref[head, at, here] = dscores
                    else:
                        dscores = weights
                    if whole:
                        more = dot(dscores, k_ref[head, here, :])
                        grad_query = more if grad_query is None else grad_query + more
            if whole:
                unit, factor = unit_rows(raw_ref[0, head, at, :].astype(jnp.float32))
                gr_ref[0, head, at, :] = unit_grad(grad_query * coeff, unit, factor).astype(bf)

        blocks(body)

    def finish_keys(rank):
        def body(head, chunk):
            at = pl.ds(tokens_at(rank, chunk), size)
            coeff = scale_ref[head] * (1.0 / hdim)
            unit, factor = unit_rows(raw_ref[1, head, at, :].astype(jnp.float32))
            both = jnp.concatenate([dkt_ref[head, :, at], dvt_ref[head, :, at]], 0).astype(bf).T
            grad_key = both[:, :hdim].astype(jnp.float32) * coeff
            gr_ref[1, head, at, :] = unit_grad(grad_key, unit, factor).astype(bf)
            gr_ref[2, head, at, :] = both[:, hdim:]

        blocks(body)

    def project_out():
        def body(chunk):
            mine = jnp.concatenate([own_ref[h, within(chunk), :] for h in range(heads)], 1)
            part_ref[within(chunk), :] = dot(mine, out_ref[...]).astype(bf)

        steps(per_rank, body)

    def project_down():
        def body(chunk):
            at = pl.ds(tokens_at(0, chunk), size)
            total = None
            for k in range(3):
                mine = jnp.concatenate([gr_ref[k, head, at, :] for head in range(heads)], 1)
                more = dot_rows(mine, qkv_ref[k])
                total = more if total is None else total + more
            part_ref[within(chunk), :] = total.astype(bf)

        steps(per_rank, body)

    def weight_grads():
        part = min(256, narrow)

        def body(step):
            start = pl.multiple_of(step * part, part)
            at = pl.ds(pl.multiple_of(place.row * narrow + start, 128), part)
            turned = hid_all[:, :, :, at].reshape(length, part).T
            for k in range(3):
                here = jnp.concatenate([gr_ref[k, head] for head in range(heads)], 1)
                grad_qkv_ref[k, pl.ds(start, part), :] = dot(turned, here)

        steps(narrow // part, body)

    def out_grads():
        mine = pl.ds(pl.multiple_of(place.row * narrow, 128), narrow)
        for rank in range(rows):
            if rank == 0:
                here = grad_level[:, :, mine]
            else:
                here = grad_cut[place.ranks[rank]]
            here = here.reshape(span, narrow)
            at = pl.ds(tokens_at(rank, 0), span)
            for head in range(heads):
                more = dot(att_ref[head, :, at], here)
                to = pl.ds(head * hdim, hdim)
                if rank == 0:
                    grad_out_ref[to, :] = more
                else:
                    grad_out_ref[to, :] += more

    def tokens_grad(down):
        normed, rstd = normed_rows()
        grad_normed = down * gain_ref[0:1, :]
        pull = jnp.mean(grad_normed * normed, -1, keepdims=True)
        grad_tok_ref[...] = (rstd * (grad_normed - normed * pull)).astype(bf)

    start_all(hid.line_sends(0))
    hid.spread(0)
    hid_all[place.row, place.col] = hidden_ref[...]
    v_ref[:, :, pl.ds(hdim, hdim)] = jnp.ones((heads, length, hdim), bf)
    vt_ref[:, pl.ds(hdim, hdim), :] = jnp.ones((heads, hdim, length), bf)
    dkt_ref[...] = jnp.zeros_like(dkt_ref)
    dvt_ref[...] = jnp.zeros_like(dvt_ref)
    grad_level[place.col] = grad_ref[...]
    hid.pass_on(1)
    hid.spread(1)
    hid.relay(0)
    hid.pass_on(2)
    hid.spread(2)

    @pl.when(place.inner)
    def _():
        hid.pass_on(3)

    hid.relay(1)
    hid.close(0)
    hid.whole_rank(0)
    for load in loads:
        load.wait()
    project(0)

    @pl.when(jnp.logical_not(place.inner))
    def _():
        hid.arrived(3, LINE, hid.slot(3, place.col))

    hid.spread(3)
    for copy in cut.cuts():
        copy.start()
    hid.relay(2)
    hid.close(1)
    hid.whole_rank(1)
    project(1)
    hid.relay(3)
    grd.spread(0)
    hid.close(2)
    hid.whole_rank(2)
    project(2)
    hid.close(3)
    hid.whole_rank(3)
    project(3)
    grd.relay(0)
    forward(0)
    grd.close(0)
    project_out()
    scatters[0].first()
    grd.whole_rank(0)
    cotangent()
    start_all(dol.line_sends(0))
    scatters[0].second()
    for rank in range(1, 4):
        cut.landed(rank)
        cut.spread(rank)
    forward(1)
    forward(2)
    dol.pass_on(1)

    @pl.when(place.inner)
    def _():
        dol.pass_on(2)

    forward(3)
    prepare(0)

    @pl.when(place.inner)
    def _():
        dol.pass_on(3)

    backward(0, (0, 1, 2, 3))
    cut.relay(1)
    cut.relay(2)
    prepare(1)
    backward(1, (0, 1, 2, 3))
    cut.relay(3)
    cut.close(1)
    cut.close(2)

    @pl.when(jnp.logical_not(place.inner))
    def _():
        dol.arrived(2, LINE, dol.slot(2, place.col))

    prepare(2)
    backward(2, (0,))
    cut.close(3)

    @pl.when(jnp.logical_not(place.inner))
    def _():
        dol.arrived(3, LINE, dol.slot(3, place.col))

    prepare(3)
    backward(3, (0,))
    update_ref[...] = scatters[0].third().astype(update_ref.dtype)
    finish_keys(0)
    project_down()
    scatters[1].first()
    for rank in range(1, 4):
        cut.whole_rank(rank)
    out_grads()
    scatters[1].second()
    backward(2, (1, 2, 3), (0,))
    backward(3, (1, 2, 3), (0,))
    for rank in range(1, 4):
        finish_keys(rank)
    weight_grads()
    tokens_grad(scatters[1].third())
    hid.drain_line()
    dol.drain_line()
    grd.drain_plane(0)
    for copy in cut.cuts():
        copy.wait_send()
    for rank in range(4):
        hid.drain_plane(rank)
        if rank > 0:
            cut.drain_plane(rank)


def fused(scale, embedded, tokens, grad_update, mod_weight, qkv_weight, out_weight):
    bf, f32 = jnp.bfloat16, jnp.float32
    tok_dev, width = tokens.shape
    heads = scale.shape[0]
    inner = qkv_weight.shape[2]
    hdim = inner // heads
    rows, cols = lax.axis_size("row"), lax.axis_size("col")
    span = tok_dev * cols
    length = span * rows
    narrow = width // rows
    in_vmem = pl.BlockSpec(memory_space=pltpu.VMEM)
    return pl.pallas_call(
        fused_kernel,
        out_shape=[
            jax.ShapeDtypeStruct((tok_dev, width), bf),
            jax.ShapeDtypeStruct((tok_dev, width), bf),
            jax.ShapeDtypeStruct((3, narrow, inner), f32),
            jax.ShapeDtypeStruct((inner, narrow), f32),
        ],
        in_specs=[pl.BlockSpec(memory_space=pltpu.SMEM)]
        + [in_vmem] * 3
        + [pl.BlockSpec(memory_space=pl.ANY)] * 3,
        out_specs=[in_vmem] * 4,
        scratch_shapes=[
            pltpu.VMEM((tok_dev, width), bf),
            pltpu.VMEM((8, width), f32),
            pltpu.VMEM(qkv_weight.shape, bf),
            pltpu.VMEM(out_weight.shape, bf),
            pltpu.SemaphoreType.DMA((2 + heads,)),
            pltpu.VMEM((rows, cols, tok_dev, width), bf),
            pltpu.VMEM((cols, tok_dev, width), bf),
            pltpu.VMEM((rows, cols, tok_dev, narrow), bf),
            pltpu.VMEM((rows, heads, span, hdim), bf),
            pltpu.VMEM((2, heads, length, hdim), bf),
            pltpu.VMEM((heads, length, hdim), bf),
            pltpu.VMEM((heads, hdim, length), bf),
            pltpu.VMEM((heads, length, hdim), bf),
            pltpu.VMEM((heads, hdim, length), bf),
            pltpu.VMEM((heads, length, 2 * hdim), bf),
            pltpu.VMEM((heads, 2 * hdim, length), bf),
            pltpu.VMEM((heads, length, length), bf),
            pltpu.VMEM((heads, 8, length), f32),
            pltpu.VMEM((heads, span, hdim), bf),
            pltpu.VMEM((heads, hdim, length), bf),
            pltpu.VMEM((heads, hdim, length), bf),
            pltpu.VMEM((heads, hdim, length), f32),
            pltpu.VMEM((heads, hdim, length), f32),
            pltpu.VMEM((3, heads, length, hdim), bf),
            pltpu.VMEM((span, width), bf),
            pltpu.VMEM((2, 4, tok_dev, width), bf),
            pltpu.VMEM((2, 3, tok_dev, width), bf),
            pltpu.SemaphoreType.DMA((4, 4, SENDS)),
            pltpu.SemaphoreType.DMA((4, 4, KINDS)),
            pltpu.SemaphoreType.DMA((2, 8)),
            pltpu.SemaphoreType.DMA((2, 8)),
        ],
        compiler_params=pltpu.CompilerParams(
            collective_id=4, has_side_effects=True, vmem_limit_bytes=67043328
        ),
        name="fused",
    )(scale, embedded, tokens, grad_update, mod_weight, qkv_weight, out_weight)


def hand_over_kernel(*refs):
    count = (len(refs) - 2) // 3
    given, taken, held = refs[:count], refs[count : 2 * count], refs[2 * count : 3 * count]
    in_sem, out_sem = refs[3 * count :]
    ins = [pltpu.make_async_copy(given[n], held[n], in_sem.at[n]) for n in range(count)]
    outs = [pltpu.make_async_copy(held[n], taken[n], out_sem.at[n]) for n in range(count)]
    for copy in ins:
        copy.start()
    for first, then in zip(ins, outs):
        first.wait()
        then.start()
    for copy in outs:
        copy.wait()


def hand_over(arrays):
    count = len(arrays)
    anywhere = pl.BlockSpec(memory_space=pl.ANY)
    return pl.pallas_call(
        hand_over_kernel,
        out_shape=[jax.ShapeDtypeStruct(a.shape, a.dtype) for a in arrays],
        in_specs=[anywhere] * count,
        out_specs=[anywhere] * count,
        scratch_shapes=[pltpu.VMEM(a.shape, a.dtype) for a in arrays]
        + [pltpu.SemaphoreType.DMA((count,))] * 2,
        name="hand_over",
    )(*arrays)


def gathered(tokens, timestep, mod_weight, qkv_weight, attn_scale, out_weight, grad_update):
    length = tokens.shape[0] * lax.axis_size("row") * lax.axis_size("col")
    if mod_weight.shape != (qkv_weight.shape[2], length):
        return per_device(
            tokens, timestep, mod_weight, qkv_weight, attn_scale, out_weight, grad_update
        )
    embedded = embed(timestep, mod_weight.shape[0] // 2)[:, None]
    return tuple(
        hand_over(
            fused(attn_scale, embedded, tokens, grad_update, mod_weight, qkv_weight, out_weight)
        )
    )


def solution(mesh):
    placed = (
        P(("row", "col"), None),
        P(),
        P(),
        P(None, None, "col"),
        P("col"),
        P("col", None),
        P(("row", "col"), None),
    )
    plane = mesh.shape["row"] == 4 and mesh.shape["col"] == 8
    return jax.shard_map(
        gathered if plane else per_device,
        mesh=mesh,
        in_specs=placed,
        out_specs=(
            P(("row", "col"), None),
            P(("row", "col"), None),
            P(None, "row", "col"),
            P("col", "row"),
        ),
        check_vma=False,
    )
```

```python
import functools
import math

import jax
import jax.numpy as jnp
from jax import lax
from jax.experimental import pallas as pl
from jax.experimental.pallas import tpu as pltpu
from jax.sharding import PartitionSpec as P

epsilon = 1e-06
MESH = pl.DeviceIdType.MESH
RELAYED = 4


def embed(timestep, count):
    index = jnp.arange(count, dtype=jnp.float32)
    freqs = jnp.exp(-math.log(10000.0) * index / count)
    angles = timestep.astype(jnp.float32)[0] * freqs
    return jnp.concatenate([jnp.cos(angles), jnp.sin(angles)])


def by_head(array, head_dim):
    return [array[:, at : at + head_dim] for at in range(0, array.shape[1], head_dim)]


def unit_rows(values):
    factor = lax.rsqrt(jnp.mean(values * values, -1, keepdims=True) + epsilon)
    return (values * factor, factor)


def unit_grad(grad_unit, unit, factor):
    return factor * (grad_unit - unit * jnp.mean(grad_unit * unit, -1, keepdims=True))


def piece(ref, dim, size, index):
    start = index * size
    if isinstance(start, int):
        pass
    elif dim == len(ref.shape) - 1:
        start = pl.multiple_of(start, 128)
    elif dim == len(ref.shape) - 2:
        start = pl.multiple_of(start, 16)
    return ref.at[(slice(None),) * dim + (pl.ds(start, size),)]


def half(ref, side):
    dim = len(ref.shape) - 2
    size = ref.shape[dim] // 2
    return ref.at[(slice(None),) * dim + (pl.ds(side * size, size),)]


def exchange_kernel(plan, *refs):
    count = len(plan)
    sources, targets = refs[:count], refs[count : 2 * count]
    own_sem, send_sem, recv_sem = refs[2 * count : 2 * count + 3]
    relays = refs[2 * count + 3 :]
    sizes = {axis: n for axis, n, dim, size in plan}
    barrier = pltpu.get_barrier_semaphore()
    for axis, n in sizes.items():
        me = lax.axis_index(axis)
        for step in range(1, n):
            pl.semaphore_signal(
                barrier, inc=1, device_id={axis: lax.rem(me + step, n)}, device_id_type=MESH
            )
    pl.semaphore_wait(barrier, sum(n - 1 for n in sizes.values()))
    def send(job, slot, source, target, peer):
        copy = pltpu.make_async_remote_copy(
            src_ref=source,
            dst_ref=target,
            send_sem=send_sem.at[job, slot],
            recv_sem=recv_sem.at[job, slot],
            device_id={plan[job][0]: peer},
            device_id_type=MESH,
        )
        copy.start()
        return copy

    copies, hops = [], {}
    chained = [job for job in range(count) if plan[job][1] == RELAYED and plan[job][2] is not None]
    relayed = [job for job in range(count) if plan[job][1] == RELAYED and job not in chained]
    for step in range(1, max(sizes.values())):
        for job, (axis, n, dim, size) in enumerate(plan):
            if step >= n or job in chained or (n == RELAYED and step == 2):
                continue
            me = lax.axis_index(axis)
            peer = lax.rem(me + step, n)
            source = sources[job]
            source = source if dim is None else piece(source, dim, size, peer)
            copy = send(job, step, source, targets[job].at[me], peer)
            if n == RELAYED and dim is None:
                hops.setdefault(job, []).append(copy)
            else:
                copies.append(copy)
    for job, (axis, n, dim, size) in enumerate(plan):
        if job in chained:
            continue
        me = lax.axis_index(axis)
        source = sources[job]
        copy = pltpu.make_async_copy(
            source if dim is None else piece(source, dim, size, me),
            targets[job].at[me],
            own_sem.at[job],
        )
        copy.start()
        copies.append(copy)
    for side in range(2):
        for job in relayed:
            axis, n, dim, size = plan[job]
            me = lax.axis_index(axis)
            right, left = lax.rem(me + 1, n), lax.rem(me + 3, n)
            onward, origin = (right, left) if side == 0 else (left, right)
            hops[job][side].wait_recv()
            landing = half(targets[job].at[origin], side)
            copies.append(send(job, 6 + side, landing, landing, onward))
    def link(job, way, owner, source):
        axis = plan[job][0]
        me = lax.axis_index(axis)
        slot = owner - 1 if way == 0 else owner
        return pltpu.make_async_remote_copy(
            src_ref=relays[job].at[way, slot] if source is None else source,
            dst_ref=relays[job].at[way, slot],
            send_sem=send_sem.at[job, 3 * way + slot],
            recv_sem=recv_sem.at[job, 3 * way + slot],
            device_id={axis: lax.rem(me + (1 if way == 0 else RELAYED - 1), RELAYED)},
            device_id_type=MESH,
        )

    def forward(job, way, owner, place):
        axis, n, dim, size = plan[job]
        mine = piece(sources[job], dim, size, owner)

        @pl.when(lax.axis_index(axis) == place)
        def _():
            if place == (0 if way == 0 else n - 1):
                link(job, way, owner, mine).start()
            else:
                copy = link(job, way, owner, None)
                copy.wait_recv()
                inbox = relays[job].at[way, owner - 1 if way == 0 else owner]
                total = inbox[...].astype(jnp.float32) + mine[...].astype(jnp.float32)
                inbox[...] = total.astype(inbox.dtype)
                copy.start()

    order = [(0, 3, 0), (1, 0, 3), (0, 2, 0), (1, 1, 3), (0, 1, 0), (1, 2, 3)]
    order += [(0, 3, 1), (1, 0, 2), (0, 2, 1), (1, 1, 2), (0, 3, 2), (1, 0, 1)]
    for way, owner, place in order:
        for job in chained:
            forward(job, way, owner, place)
    for job in chained:
        axis, n, dim, size = plan[job]
        for owner in range(n):

            @pl.when(lax.axis_index(axis) == owner)
            def _():
                total = piece(sources[job], dim, size, owner)[...].astype(jnp.float32)
                if owner > 0:
                    link(job, 0, owner, None).wait_recv()
                    total = total + relays[job][0, owner - 1].astype(jnp.float32)
                if owner < n - 1:
                    link(job, 1, owner, None).wait_recv()
                    total = total + relays[job][1, owner].astype(jnp.float32)
                targets[job][0] = total
                for other in range(n):
                    if other > owner:
                        link(job, 0, other, None).wait_send()
                    if other < owner:
                        link(job, 1, other, None).wait_send()

    for job in relayed:
        for copy in hops[job]:
            copy.wait_send()
    for copy in copies:
        copy.wait()


def exchange(jobs, collective_id):
    plan, shapes, relays = [], [], []
    for array, axis, dim in jobs:
        n = lax.axis_size(axis)
        block = list(array.shape)
        size = None
        if dim is not None:
            size = block[dim] = block[dim] // n
        plan.append((axis, n, dim, size))
        if n == RELAYED and dim is not None:
            shapes.append(jax.ShapeDtypeStruct((1,) + tuple(block), jnp.float32))
            relays.append(pltpu.VMEM((2, n - 1) + tuple(block), array.dtype))
        else:
            shapes.append(jax.ShapeDtypeStruct((n,) + tuple(block), array.dtype))
            relays.append(pltpu.VMEM((16, 128), array.dtype))
    most = max(2 * RELAYED, max(n for axis, n, dim, size in plan))
    count = len(jobs)
    in_vmem = pl.BlockSpec(memory_space=pltpu.VMEM)
    return pl.pallas_call(
        functools.partial(exchange_kernel, tuple(plan)),
        out_shape=shapes,
        in_specs=[in_vmem] * count,
        out_specs=[in_vmem] * count,
        scratch_shapes=[
            pltpu.SemaphoreType.DMA((count,)),
            pltpu.SemaphoreType.DMA((count, most)),
            pltpu.SemaphoreType.DMA((count, most)),
            *relays,
        ],
        compiler_params=pltpu.CompilerParams(
            collective_id=collective_id, has_side_effects=True, vmem_limit_bytes=48 * 2**20
        ),
        name=f"exchange_{collective_id}",
    )(*[array for array, axis, dim in jobs])


def dot_rows(left, right):
    return lax.dot_general(
        left, right, (((1,), (1,)), ((), ())), preferred_element_type=jnp.float32
    )


def dot_columns(left, right):
    return lax.dot_general(
        left, right, (((0,), (0,)), ((), ())), preferred_element_type=jnp.float32
    )


def attention_kernel(
    scale_ref, q_ref, k_ref, v_ref, g_ref, o_ref, dq_ref, dk_ref, dv_ref, dk_sum, dv_sum
):
    block = pl.program_id(1)
    scale = scale_ref[pl.program_id(0)]
    coeff = scale * (1.0 / q_ref.shape[1])
    query, keys, values, grad = q_ref[...], k_ref[...], v_ref[...], g_ref[...]
    weights = jnp.exp(dot_rows(query, keys) * coeff - scale)
    inverse = 1.0 / jnp.sum(weights, -1, keepdims=True)
    mixed = jnp.dot(weights.astype(jnp.bfloat16), values, preferred_element_type=jnp.float32)
    attended = (mixed * inverse).astype(jnp.bfloat16)
    o_ref[...] = attended
    delta = jnp.sum(
        grad.astype(jnp.float32) * attended.astype(jnp.float32), -1, keepdims=True
    )
    probs = weights * inverse
    dscores = (probs * (dot_rows(grad, values) - delta) * coeff).astype(jnp.bfloat16)
    dq_ref[...] = jnp.dot(dscores, keys, preferred_element_type=jnp.float32)
    dk_part = dot_columns(dscores, query)
    dv_part = dot_columns(probs.astype(jnp.bfloat16), grad)

    @pl.when(block == 0)
    def _():
        dk_sum[...] = dk_part
        dv_sum[...] = dv_part

    @pl.when(block > 0)
    def _():
        dk_sum[...] += dk_part
        dv_sum[...] += dv_part

    @pl.when(block == pl.num_programs(1) - 1)
    def _():
        dk_ref[...] = dk_sum[...].astype(dk_ref.dtype)
        dv_ref[...] = dv_sum[...].astype(dv_ref.dtype)


def attention(attn_scale, queries, keys_values, grads):
    heads = attn_scale.shape[0]
    span, inner = queries.shape
    length = keys_values.shape[0]
    head_dim = inner // heads
    size = math.gcd(span, 256)
    while size * length > 2**19 and size % 32 == 0:
        size //= 2
    mine = pl.BlockSpec((size, head_dim), lambda h, i: (i, h))
    keys = pl.BlockSpec((length, head_dim), lambda h, i: (0, h))
    values = pl.BlockSpec((length, head_dim), lambda h, i: (0, heads + h))
    return pl.pallas_call(
        attention_kernel,
        grid=(heads, span // size),
        out_shape=[
            jax.ShapeDtypeStruct((span, inner), jnp.bfloat16),
            jax.ShapeDtypeStruct((span, inner), jnp.float32),
            jax.ShapeDtypeStruct((length, inner), jnp.bfloat16),
            jax.ShapeDtypeStruct((length, inner), jnp.bfloat16),
        ],
        in_specs=[pl.BlockSpec(memory_space=pltpu.SMEM), mine, keys, values, mine],
        out_specs=[mine, mine, keys, keys],
        scratch_shapes=[pltpu.VMEM((length, head_dim), jnp.float32)] * 2,
        compiler_params=pltpu.CompilerParams(
            dimension_semantics=("arbitrary", "arbitrary"), vmem_limit_bytes=56 * 2**20
        ),
        name="attention",
    )(attn_scale, queries, keys_values, keys_values, grads)


def add_up(slots):
    return jnp.sum(slots.astype(jnp.float32), 0)


def per_device(tokens, timestep, mod_weight, qkv_weight, attn_scale, out_weight, grad_update):
    tok_dev, width = tokens.shape
    heads_here = attn_scale.shape[0]
    inner = qkv_weight.shape[2]
    head_dim = inner // heads_here
    span = tok_dev * lax.axis_size("col")
    embedded = embed(timestep, mod_weight.shape[0] // 2)
    gain = 1.0 + jnp.sum(embedded[:, None] * mod_weight, 0)
    tok_float = tokens.astype(jnp.float32)
    rstd = lax.rsqrt(jnp.mean(tok_float * tok_float, -1, keepdims=True) + epsilon)
    normed = tok_float * rstd
    hidden = (normed * gain).astype(jnp.bfloat16)
    (group,) = exchange([(hidden, "col", None)], 0)
    group = group.reshape(span, width)
    raw = [jnp.dot(group, qkv_weight[k], preferred_element_type=jnp.float32) for k in range(3)]
    query_unit, query_factor = zip(*[unit_rows(part) for part in by_head(raw[0], head_dim)])
    key_unit, key_factor = zip(*[unit_rows(part) for part in by_head(raw[1], head_dim)])
    queries = jnp.concatenate(query_unit, 1).astype(jnp.bfloat16)
    keys_values = jnp.concatenate(key_unit + (raw[2],), 1).astype(jnp.bfloat16)
    all_keys_values, grad_group = exchange(
        [(keys_values, "row", None), (grad_update, "col", None)], 1
    )
    all_keys_values = all_keys_values.reshape(-1, 2 * inner)
    grad_group = grad_group.reshape(span, width)
    grad_attended = dot_rows(grad_group, out_weight).astype(jnp.bfloat16)
    attended, grad_query, key_part, value_part = attention(
        attn_scale, queries, all_keys_values, grad_attended
    )
    update_part = jnp.dot(attended, out_weight, preferred_element_type=jnp.float32).astype(
        jnp.bfloat16
    )
    out_part = dot_columns(attended, grad_group).astype(jnp.bfloat16)
    key_slots, value_slots, update_slots = exchange(
        [(key_part, "row", 0), (value_part, "row", 0), (update_part, "col", 0)], 2
    )
    update = add_up(update_slots).astype(jnp.bfloat16)

    def raw_grads(grad_unit, unit, factor):
        parts = zip(by_head(grad_unit, head_dim), unit, factor)
        return jnp.concatenate([unit_grad(*part) for part in parts], 1).astype(jnp.bfloat16)

    grad_raw = [
        raw_grads(grad_query, query_unit, query_factor),
        raw_grads(add_up(key_slots), key_unit, key_factor),
        add_up(value_slots).astype(jnp.bfloat16),
    ]
    qkv_part = jnp.stack([dot_columns(group, part).astype(jnp.bfloat16) for part in grad_raw])
    hidden_part = (
        sum(dot_rows(part, qkv_weight[k]) for k, part in enumerate(grad_raw))
    ).astype(jnp.bfloat16)
    qkv_slots, hidden_slots, out_slots = exchange(
        [(qkv_part, "row", 1), (hidden_part, "col", 0), (out_part, "row", 1)], 3
    )
    grad_qkv = add_up(qkv_slots)
    grad_out = add_up(out_slots)
    grad_normed = add_up(hidden_slots) * gain
    grad_tokens = (
        rstd * (grad_normed - normed * jnp.mean(grad_normed * normed, -1, keepdims=True))
    ).astype(jnp.bfloat16)
    return (update, grad_tokens, grad_qkv, grad_out)


def flip(index, bit):
    return index + bit - 2 * bit * ((index // bit) % 2)


class Place:
    def __init__(self):
        self.row = lax.axis_index("row")
        self.col = lax.axis_index("col")
        self.partner = flip(self.col, 1)
        self.beside = flip(self.col, 2)
        self.across = flip(self.col, 4)
        self.corner = flip(self.beside, 4)
        self.inner = ((self.row + 1) // 2) % 2 == 1
        self.mate = flip(self.row, 1)
        self.facing = 3 - self.row
        low = 1 - self.row // 2
        self.ranks = [self.row, self.mate, 1 + low, 3 * low]

    def greet(self):
        barrier = pltpu.get_barrier_semaphore()
        for peer in (self.partner, self.beside, self.across, self.corner):
            pl.semaphore_signal(barrier, inc=1, device_id={"col": peer}, device_id_type=MESH)
        for peer in self.ranks[1:]:
            pl.semaphore_signal(barrier, inc=1, device_id={"row": peer}, device_id_type=MESH)

    def await_greetings(self):
        pl.semaphore_wait(pltpu.get_barrier_semaphore(), 7)


LINE, BESIDE, ACROSS, TOP, BOTTOM, MATE = 0, 1, 2, 3, 4, 5
WHOLE, LEVEL, SLICE, BLOCK, FAR = 0, 1, 2, 3, 4
LINES = (WHOLE, BLOCK, FAR)
PLANES = [(WHOLE, rank) for rank in range(4)] + [(LEVEL, 0)] + [(SLICE, r) for r in (1, 2, 3)]


def numbered(keys):
    return {key: at for at, key in enumerate(keys)}


SENDS = numbered(
    [(job, rank, 0) for job in LINES for rank in range(4)]
    + [(job, 0, 1) for job in LINES]
    + [(SLICE, at, 0) for at in range(3)]
    + [plane + (kind,) for plane in PLANES for kind in range(2, 10)]
)
ARRIVALS = numbered(
    [(SLICE, row, LINE) for row in range(4)]
    + [(job, rank, LINE) for job in LINES for rank in (1, 2, 3)]
    + [plane + (kind,) for plane in PLANES for kind in range(1, 9)]
)


class Gather:
    def __init__(self, place, job, tile, whole, send_sem, recv_sem, split=False):
        self.split = split
        self.place, self.job, self.tile, self.whole = place, job, tile, whole
        self.send_sem, self.recv_sem = send_sem, recv_sem

    def slot(self, rank, col):
        return self.whole.at[self.place.ranks[rank], col]

    def link(self, rank, kind, send, source, landing, peer):
        return pltpu.make_async_remote_copy(
            src_ref=source,
            dst_ref=landing,
            send_sem=self.send_sem.at[SENDS.get((self.job,) + send, 0)],
            recv_sem=self.recv_sem.at[ARRIVALS[self.job, rank, kind]],
            device_id=peer,
            device_id_type=MESH,
        )

    def arrived(self, rank, kind, landing):
        self.link(rank, kind, (0, 0), landing, landing, {"col": self.place.partner}).wait_recv()

    def held(self, rank):
        return self.tile if rank == 0 else self.slot(rank, self.place.col)

    def line_sends(self, rank):
        p = self.place
        mine = self.slot(rank, p.col)
        held = self.held(rank)
        if rank == 0:
            outward = self.link(1, LINE, (0, 0), held, mine, {"row": p.mate})
            inward = self.link(2, LINE, (0, 1), held, mine, {"row": p.facing})
            return [(outward, False), (inward, True)]
        if rank == 1:
            return [(self.link(3, LINE, (1, 0), held, mine, {"row": p.facing}), True)]
        return [(self.link(rank, LINE, (rank, 0), held, mine, {"row": p.mate}), True)]

    def plane_sends(self, rank):
        p = self.place
        mine, held = self.slot(rank, p.col), self.held(rank)
        return [
            self.link(rank, BESIDE, (rank, 2), held, mine, {"col": p.beside}),
            self.link(rank, ACROSS, (rank, 3), held, mine, {"col": p.across}),
            self.link(rank, MATE, (rank, 4), held, mine, {"col": p.partner}),
        ]

    def strip(self, ref, rank, side):
        if not self.split or rank == 0:
            return half(ref, side)
        size = ref.shape[0] // 4
        return ref.at[pl.ds(side * size, size)]

    def relays(self, rank):
        p = self.place
        side, over = self.slot(rank, p.beside), self.slot(rank, p.across)
        return [
            self.link(rank, TOP, (rank, 5), self.strip(side, rank, 0), self.strip(side, rank, 0), {"col": p.across}),
            self.link(rank, MATE + 1, (rank, 6), side, side, {"col": p.partner}),
            self.link(rank, BOTTOM, (rank, 7), self.strip(over, rank, 1), self.strip(over, rank, 1), {"col": p.beside}),
            self.link(rank, MATE + 2, (rank, 8), over, over, {"col": p.partner}),
        ]

    def last(self, rank):
        p = self.place
        far = self.slot(rank, p.corner)
        return self.link(rank, MATE + 3, (rank, 9), far, far, {"col": p.partner})

    def each(self, copies, act):
        for copy, inner in copies:
            if inner:
                pl.when(self.place.inner)(functools.partial(act, copy))
            else:
                act(copy)

    def pass_on(self, rank):
        self.arrived(rank, LINE, self.slot(rank, self.place.col))
        self.each(self.line_sends(rank), lambda copy: copy.start())

    def spread(self, rank):
        for copy in self.plane_sends(rank):
            copy.start()

    def relay(self, rank):
        p = self.place
        top, side, bottom, over = self.relays(rank)
        self.arrived(rank, BESIDE, self.slot(rank, p.beside))
        top.start()
        side.start()
        self.arrived(rank, ACROSS, self.slot(rank, p.across))
        bottom.start()
        over.start()

    def close(self, rank):
        p = self.place
        far = self.slot(rank, p.corner)
        self.arrived(rank, TOP, self.strip(far, rank, 0))
        self.arrived(rank, BOTTOM, self.strip(far, rank, 1))
        self.last(rank).start()

    def whole_rank(self, rank):
        p = self.place
        for kind, col in enumerate((p.col, p.beside, p.across, p.corner)):
            self.arrived(rank, MATE + kind, self.slot(rank, flip(col, 1)))

    def drain_line(self):
        for rank in range(4):
            self.each(self.line_sends(rank), lambda copy: copy.wait_send())

    def drain_plane(self, rank):
        for copy in self.plane_sends(rank) + self.relays(rank) + [self.last(rank)]:
            copy.wait_send()


class Level(Gather):
    def slot(self, rank, col):
        return self.whole.at[col]


class Line(Gather):
    def slot(self, rank, col):
        return self.whole.at[self.place.ranks[rank]]


class Corner(Gather):
    def slot(self, rank, col):
        return half(self.whole.at[self.place.ranks[rank], self.place.corner], 1)


class Slices(Gather):
    def cuts(self):
        p = self.place
        size = self.whole.shape[3]
        copies = []
        for at, peer in enumerate(p.ranks[1:]):
            mine = pl.ds(pl.multiple_of(peer * size, 128), size)
            copies.append(
                pltpu.make_async_remote_copy(
                    src_ref=self.tile.at[:, mine],
                    dst_ref=self.slot(0, p.col),
                    send_sem=self.send_sem.at[SENDS[self.job, at, 0]],
                    recv_sem=self.recv_sem.at[p.row],
                    device_id={"row": peer},
                    device_id_type=MESH,
                )
            )
        return copies

    def landed(self, rank):
        p = self.place
        slot = self.slot(rank, p.col)
        pltpu.make_async_remote_copy(
            src_ref=slot,
            dst_ref=slot,
            send_sem=self.send_sem.at[SENDS[self.job, 0, 0]],
            recv_sem=self.recv_sem.at[p.ranks[rank]],
            device_id={"col": p.partner},
            device_id_type=MESH,
        ).wait_recv()

    def held(self, rank):
        return self.slot(rank, self.place.col)


class Scatter:
    def __init__(self, place, job, part, crossed, landed, send_sem, recv_sem):
        self.place, self.job, self.part = place, job, part
        self.crossed, self.landed = crossed, landed
        self.send_sem, self.recv_sem = send_sem, recv_sem
        self.size = part.shape[0] // 8

    def targets(self):
        p = self.place
        return (p.corner, p.beside, p.across, p.col)

    def rows(self, col):
        return pl.ds(pl.multiple_of(col * self.size, 16), self.size)

    def core_send(self, at):
        p = self.place
        return pltpu.make_async_remote_copy(
            src_ref=self.part.at[self.rows(flip(self.targets()[at], 1))],
            dst_ref=self.crossed.at[self.job, at],
            send_sem=self.send_sem.at[self.job, at],
            recv_sem=self.recv_sem.at[self.job, at],
            device_id={"col": p.partner},
            device_id_type=MESH,
        )

    def chip_send(self, at):
        return pltpu.make_async_remote_copy(
            src_ref=self.part.at[self.rows(self.targets()[at])],
            dst_ref=self.landed.at[self.job, at],
            send_sem=self.send_sem.at[self.job, 4 + at],
            recv_sem=self.recv_sem.at[self.job, 4 + at],
            device_id={"col": self.targets()[at]},
            device_id_type=MESH,
        )

    def chip_sum(self, at):
        mine = self.part[self.rows(self.targets()[at]), :].astype(jnp.float32)
        return mine + self.crossed[self.job, at].astype(jnp.float32)

    def first(self):
        for at in range(4):
            self.core_send(at).start()

    def second(self):
        for at in range(3):
            self.core_send(at).wait_recv()
            self.part[self.rows(self.targets()[at]), :] = self.chip_sum(at).astype(self.part.dtype)
            self.chip_send(at).start()

    def third(self):
        self.core_send(3).wait_recv()
        total = self.chip_sum(3)
        for at in (1, 2, 0):
            self.chip_send(at).wait_recv()
            total = total + self.landed[self.job, at].astype(jnp.float32)
        for at in range(4):
            self.core_send(at).wait_send()
        for at in range(3):
            self.chip_send(at).wait_send()
        return total


LOG2E = 1.4426950408889634


def dot(left, right):
    return jnp.dot(left, right, preferred_element_type=jnp.float32)


def fused_kernel(
    scale_ref, embed_ref, tok_ref, grad_ref, mod_hbm, qkv_hbm, out_hbm,
    update_hbm, grad_tok_hbm, grad_qkv_hbm, grad_out_hbm,
    update_ref, grad_tok_ref, grad_qkv_ref, grad_out_ref, hidden_ref, gain_ref, qkv_ref, out_ref, load_sem, hid_all, grad_level, grad_cut, do_all, raw_ref, q_ref, qt_ref, k_ref, kt_ref, v_ref, vt_ref,
    w_ref, inv_ref, own_ref, att_ref, dot_ref, dkt_ref, dvt_ref, gr_ref,
    part_ref, crossed, landed, send_sem, recv_sem, send_sum, recv_sum,
):
    bf = jnp.bfloat16
    place = Place()
    rows, cols, tok_dev, width = hid_all.shape
    heads, length, hdim = q_ref.shape
    span = cols * tok_dev
    size = math.gcd(span, 256)
    per_rank = span // size
    narrow = width // rows
    dog_ref = v_ref
    mod_loads = [
        pltpu.make_async_copy(
            mod_hbm.at[pl.ds(head * hdim, hdim)], dkt_ref.at[head], load_sem.at[2 + head]
        )
        for head in range(heads)
    ]
    loads = [
        pltpu.make_async_copy(qkv_hbm, qkv_ref, load_sem.at[0]),
        pltpu.make_async_copy(out_hbm, out_ref, load_sem.at[1]),
    ]
    stores = [
        pltpu.make_async_copy(held, to, load_sem.at[2 + heads + at])
        for at, (held, to) in enumerate(
            (
                (update_ref, update_hbm),
                (grad_tok_ref, grad_tok_hbm),
                (grad_qkv_ref, grad_qkv_hbm),
                (grad_out_ref, grad_out_hbm),
            )
        )
    ]
    for load in mod_loads + loads:
        load.start()
    place.greet()
    gain = 1.0
    for head, load in enumerate(mod_loads):
        load.wait()
        here = embed_ref[pl.ds(head * hdim, hdim), :] * dkt_ref[head]
        gain = gain + jnp.sum(here, 0, keepdims=True)
    gain_ref[...] = jnp.broadcast_to(gain, gain_ref.shape)

    def normed_rows():
        tok_float = tok_ref[...].astype(jnp.float32)
        rstd = lax.rsqrt(jnp.mean(tok_float * tok_float, -1, keepdims=True) + epsilon)
        return tok_float * rstd, rstd

    hidden_ref[...] = (normed_rows()[0] * gain_ref[0:1, :]).astype(bf)
    place.await_greetings()
    hid = Gather(place, 0, hidden_ref, hid_all, send_sem, recv_sem, True)
    far = Corner(
        place, 4, half(hid_all.at[place.row, place.corner], 1), hid_all, send_sem, recv_sem
    )
    grd = Level(place, 1, grad_ref, grad_level, send_sem, recv_sem)
    cut = Slices(place, 2, grad_ref, grad_cut, send_sem, recv_sem)
    dol = Line(place, 3, do_all.at[place.row], do_all, send_sem, recv_sem)
    scatters = [
        Scatter(place, job, part_ref, crossed, landed, send_sum, recv_sum) for job in range(2)
    ]

    def start_all(copies):
        hid.each(copies, lambda copy: copy.start())

    def tokens_at(rank, chunk):
        return pl.multiple_of(place.ranks[rank] * span + chunk * size, size)

    def within(chunk):
        return pl.ds(pl.multiple_of(chunk * size, size), size)

    def steps(count, body):
        def step(at, carry):
            body(at)
            return carry

        lax.fori_loop(0, count, step, 0)

    def blocks(body):
        steps(heads * per_rank, lambda at: body(at // per_rank, at % per_rank))

    few = size // tok_dev

    def project(rank):
        def body(chunk):
            at = pl.ds(tokens_at(rank, chunk), size)
            here = hid_all[place.ranks[rank], pl.ds(chunk * few, few)].reshape(size, width)
            for k in range(3):
                raw = dot(here, qkv_ref[k])
                for head, part in enumerate(by_head(raw, hdim)):
                    if k < 2:
                        raw_ref[k, head, at, :] = part.astype(bf)
                        part = unit_rows(part)[0]
                    part = part.astype(bf)
                    if k == 0:
                        q_ref[head, at, :] = part
                        qt_ref[head, :, at] = part.T
                    elif k == 1:
                        k_ref[head, at, :] = part
                        kt_ref[head, :, at] = part.T
                    else:
                        v_ref[head, at, pl.ds(0, hdim)] = part
                        vt_ref[head, pl.ds(0, hdim), at] = part.T

        steps(per_rank, body)

    def cotangent():
        def body(chunk):
            here = grad_level[pl.ds(chunk * few, few)].reshape(size, width)
            value = dot_rows(here, out_ref[...]).astype(bf)
            for head, part in enumerate(by_head(value, hdim)):
                do_all[place.row, head, within(chunk), :] = part

        steps(per_rank, body)

    wide = min(512, span)

    def forward(rank):
        def body(head, chunk):
            at = pl.ds(tokens_at(rank, chunk), size)
            coeff = scale_ref[head] * (LOG2E / hdim)
            query = q_ref[head, at, :]
            mixed = None
            for start in range(0, length, wide):
                here = pl.ds(start, wide)
                weights = jnp.exp2(dot(query, kt_ref[head, :, here]) * coeff).astype(bf)
                w_ref[head, at, here] = weights
                more = dot(weights, v_ref[head, here, :])
                mixed = more if mixed is None else mixed + more
            inverse = 1.0 / mixed[:, hdim:]
            attended = (mixed[:, :hdim] * inverse).astype(bf)
            if rank == 0:
                own_ref[head, within(chunk), :] = attended
            att_ref[head, :, at] = attended.T
            inv_ref[head, :, at] = inverse.T[:8]

        blocks(body)

    def prepare(rank):
        def body(head, chunk):
            at = pl.ds(tokens_at(rank, chunk), size)
            turned = do_all[place.ranks[rank], head, within(chunk), :].T.astype(jnp.float32)
            delta = jnp.sum(turned * att_ref[head, :, at].astype(jnp.float32), 0, keepdims=True)
            inverse = inv_ref[head, 0:1, at]
            turned = turned * inverse
            dot_ref[head, :, at] = turned.astype(bf)
            delta = jnp.broadcast_to(delta * inverse, (hdim, size))
            high = delta.astype(bf).astype(jnp.float32)
            line = lax.broadcasted_iota(jnp.int32, (hdim, size), 0)
            spare = jnp.where(line == 0, -high, jnp.where(line == 1, high - delta, 0.0))
            dog_ref[head, at, :] = jnp.concatenate([turned, spare], 0).astype(bf).T

        blocks(body)

    def backward(rank, fresh, stored=()):
        def body(head, chunk):
            at = pl.ds(tokens_at(rank, chunk), size)
            coeff = scale_ref[head] * (1.0 / hdim)
            whole = len(fresh) + len(stored) == rows
            grad_more = dog_ref[head, at, :]
            grad_turned = dot_ref[head, :, at]
            query_turned = qt_ref[head, :, at]
            grad_query = None
            for key_rank in stored + fresh:
                first = pl.multiple_of(place.ranks[key_rank] * span, span)
                for start in range(0, span, wide):
                    here = pl.ds(pl.multiple_of(first + start, wide), wide)
                    weights = w_ref[head, at, here]
                    if key_rank in fresh:
                        dprobs = dot(grad_more, vt_ref[head, :, here])
                        dscores = weights * dprobs.astype(bf)
                        dkt_ref[head, :, here] += dot(query_turned, dscores)
                        dvt_ref[head, :, here] += dot(grad_turned, weights)
                        if not whole:
                            w_ref[head, at, here] = dscores
                    else:
                        dscores = weights
                    if whole:
                        more = dot(dscores, k_ref[head, here, :])
                        grad_query = more if grad_query is None else grad_query + more
            if whole:
                unit, factor = unit_rows(raw_ref[0, head, at, :].astype(jnp.float32))
                gr_ref[0, head, at, :] = unit_grad(grad_query * coeff, unit, factor).astype(bf)

        blocks(body)

    def finish_keys(rank):
        def body(head, chunk):
            at = pl.ds(tokens_at(rank, chunk), size)
            coeff = scale_ref[head] * (1.0 / hdim)
            unit, factor = unit_rows(raw_ref[1, head, at, :].astype(jnp.float32))
            both = jnp.concatenate([dkt_ref[head, :, at], dvt_ref[head, :, at]], 0).astype(bf).T
            grad_key = both[:, :hdim].astype(jnp.float32) * coeff
            gr_ref[1, head, at, :] = unit_grad(grad_key, unit, factor).astype(bf)
            gr_ref[2, head, at, :] = both[:, hdim:]

        blocks(body)

    def project_out():
        def body(chunk):
            mine = jnp.concatenate([own_ref[h, within(chunk), :] for h in range(heads)], 1)
            part_ref[within(chunk), :] = dot(mine, out_ref[...]).astype(bf)

        steps(per_rank, body)

    def project_down():
        def body(chunk):
            at = pl.ds(tokens_at(0, chunk), size)
            total = None
            for k in range(3):
                mine = jnp.concatenate([gr_ref[k, head, at, :] for head in range(heads)], 1)
                more = dot_rows(mine, qkv_ref[k])
                total = more if total is None else total + more
            part_ref[within(chunk), :] = total.astype(bf)

        steps(per_rank, body)

    def weight_grads():
        part = min(256, narrow)

        def body(step):
            start = pl.multiple_of(step * part, part)
            at = pl.ds(pl.multiple_of(place.row * narrow + start, 128), part)
            turned = hid_all[:, :, :, at].reshape(length, part).T
            for k in range(3):
                here = jnp.concatenate([gr_ref[k, head] for head in range(heads)], 1)
                grad_qkv_ref[k, pl.ds(start, part), :] = dot(turned, here)

        steps(narrow // part, body)

    def out_grads():
        mine = pl.ds(pl.multiple_of(place.row * narrow, 128), narrow)
        for rank in range(rows):
            if rank == 0:
                here = grad_level[:, :, mine]
            else:
                here = grad_cut[place.ranks[rank]]
            here = here.reshape(span, narrow)
            at = pl.ds(tokens_at(rank, 0), span)
            for head in range(heads):
                more = dot(att_ref[head, :, at], here)
                to = pl.ds(head * hdim, hdim)
                if rank == 0:
                    grad_out_ref[to, :] = more
                else:
                    grad_out_ref[to, :] += more

    def tokens_grad(down):
        normed, rstd = normed_rows()
        grad_normed = down * gain_ref[0:1, :]
        pull = jnp.mean(grad_normed * normed, -1, keepdims=True)
        grad_tok_ref[...] = (rstd * (grad_normed - normed * pull)).astype(bf)

    start_all(hid.line_sends(0))
    hid.spread(0)
    hid_all[place.row, place.col] = hidden_ref[...]
    v_ref[:, :, pl.ds(hdim, hdim)] = jnp.ones((heads, length, hdim), bf)
    vt_ref[:, pl.ds(hdim, hdim), :] = jnp.ones((heads, hdim, length), bf)
    dkt_ref[...] = jnp.zeros_like(dkt_ref)
    dvt_ref[...] = jnp.zeros_like(dvt_ref)
    grad_level[place.col] = grad_ref[...]
    hid.pass_on(1)
    hid.spread(1)
    hid.relay(0)
    hid.pass_on(2)
    hid.spread(2)

    @pl.when(place.inner)
    def _():
        hid.pass_on(3)

    hid.relay(1)
    hid.close(0)
    start_all(far.line_sends(0))
    hid.whole_rank(0)
    for load in loads:
        load.wait()
    project(0)

    @pl.when(jnp.logical_not(place.inner))
    def _():
        hid.arrived(3, LINE, hid.slot(3, place.col))

    hid.spread(3)
    for copy in cut.cuts():
        copy.start()
    far.pass_on(1)
    hid.relay(2)
    hid.close(1)

    @pl.when(place.inner)
    def _():
        far.pass_on(2)

    hid.whole_rank(1)
    project(1)

    @pl.when(place.inner)
    def _():
        far.pass_on(3)

    hid.relay(3)
    grd.spread(0)

    @pl.when(jnp.logical_not(place.inner))
    def _():
        far.arrived(2, LINE, far.slot(2, place.col))

    hid.close(2)
    hid.whole_rank(2)
    project(2)

    @pl.when(jnp.logical_not(place.inner))
    def _():
        far.arrived(3, LINE, far.slot(3, place.col))

    hid.close(3)
    hid.whole_rank(3)
    project(3)
    grd.relay(0)
    forward(0)
    grd.close(0)
    project_out()
    scatters[0].first()
    grd.whole_rank(0)
    cotangent()
    start_all(dol.line_sends(0))
    scatters[0].second()
    for rank in range(1, 4):
        cut.landed(rank)
        cut.spread(rank)
    forward(1)
    forward(2)
    dol.pass_on(1)

    @pl.when(place.inner)
    def _():
        dol.pass_on(2)

    forward(3)
    prepare(0)
    backward(0, (0, 1, 2, 3))

    @pl.when(place.inner)
    def _():
        dol.pass_on(3)

    cut.relay(1)
    cut.relay(2)
    prepare(1)
    backward(1, (0, 1, 2, 3))
    cut.relay(3)
    cut.close(1)
    cut.close(2)

    @pl.when(jnp.logical_not(place.inner))
    def _():
        dol.arrived(2, LINE, dol.slot(2, place.col))

    prepare(2)
    backward(2, (0,))
    cut.close(3)

    @pl.when(jnp.logical_not(place.inner))
    def _():
        dol.arrived(3, LINE, dol.slot(3, place.col))

    prepare(3)
    backward(3, (0,))
    update_ref[...] = scatters[0].third().astype(update_ref.dtype)
    stores[0].start()
    finish_keys(0)
    project_down()
    scatters[1].first()
    for rank in range(1, 4):
        cut.whole_rank(rank)
    out_grads()
    stores[3].start()
    scatters[1].second()
    backward(2, (1, 2, 3), (0,))
    backward(3, (1, 2, 3), (0,))
    for rank in range(1, 4):
        finish_keys(rank)
    weight_grads()
    stores[2].start()
    tokens_grad(scatters[1].third())
    stores[1].start()
    hid.drain_line()
    far.drain_line()
    dol.drain_line()
    grd.drain_plane(0)
    for copy in cut.cuts():
        copy.wait_send()
    for rank in range(4):
        hid.drain_plane(rank)
        if rank > 0:
            cut.drain_plane(rank)
    for store in stores:
        store.wait()


def fused(scale, embedded, tokens, grad_update, mod_weight, qkv_weight, out_weight):
    bf, f32 = jnp.bfloat16, jnp.float32
    tok_dev, width = tokens.shape
    heads = scale.shape[0]
    inner = qkv_weight.shape[2]
    hdim = inner // heads
    rows, cols = lax.axis_size("row"), lax.axis_size("col")
    span = tok_dev * cols
    length = span * rows
    narrow = width // rows
    in_vmem = pl.BlockSpec(memory_space=pltpu.VMEM)
    return pl.pallas_call(
        fused_kernel,
        out_shape=[
            jax.ShapeDtypeStruct((tok_dev, width), bf),
            jax.ShapeDtypeStruct((tok_dev, width), bf),
            jax.ShapeDtypeStruct((3, narrow, inner), f32),
            jax.ShapeDtypeStruct((inner, narrow), f32),
        ],
        in_specs=[pl.BlockSpec(memory_space=pltpu.SMEM)]
        + [in_vmem] * 3
        + [pl.BlockSpec(memory_space=pl.ANY)] * 3,
        out_specs=[pl.BlockSpec(memory_space=pl.ANY)] * 4,
        scratch_shapes=[
            pltpu.VMEM((tok_dev, width), bf),
            pltpu.VMEM((tok_dev, width), bf),
            pltpu.VMEM((3, narrow, inner), f32),
            pltpu.VMEM((inner, narrow), f32),
            pltpu.VMEM((tok_dev, width), bf),
            pltpu.VMEM((8, width), f32),
            pltpu.VMEM(qkv_weight.shape, bf),
            pltpu.VMEM(out_weight.shape, bf),
            pltpu.SemaphoreType.DMA((6 + heads,)),
            pltpu.VMEM((rows, cols, tok_dev, width), bf),
            pltpu.VMEM((cols, tok_dev, width), bf),
            pltpu.VMEM((rows, cols, tok_dev, narrow), bf),
            pltpu.VMEM((rows, heads, span, hdim), bf),
            pltpu.VMEM((2, heads, length, hdim), bf),
            pltpu.VMEM((heads, length, hdim), bf),
            pltpu.VMEM((heads, hdim, length), bf),
            pltpu.VMEM((heads, length, hdim), bf),
            pltpu.VMEM((heads, hdim, length), bf),
            pltpu.VMEM((heads, length, 2 * hdim), bf),
            pltpu.VMEM((heads, 2 * hdim, length), bf),
            pltpu.VMEM((heads, length, length), bf),
            pltpu.VMEM((heads, 8, length), f32),
            pltpu.VMEM((heads, span, hdim), bf),
            pltpu.VMEM((heads, hdim, length), bf),
            pltpu.VMEM((heads, hdim, length), bf),
            pltpu.VMEM((heads, hdim, length), f32),
            pltpu.VMEM((heads, hdim, length), f32),
            pltpu.VMEM((3, heads, length, hdim), bf),
            pltpu.VMEM((span, width), bf),
            pltpu.VMEM((2, 4, tok_dev, width), bf),
            pltpu.VMEM((2, 3, tok_dev, width), bf),
            pltpu.SemaphoreType.DMA((len(SENDS),)),
            pltpu.SemaphoreType.DMA((len(ARRIVALS),)),
            pltpu.SemaphoreType.DMA((2, 8)),
            pltpu.SemaphoreType.DMA((2, 8)),
        ],
        compiler_params=pltpu.CompilerParams(
            collective_id=4, has_side_effects=True, vmem_limit_bytes=67043328
        ),
        name="fused",
    )(scale, embedded, tokens, grad_update, mod_weight, qkv_weight, out_weight)


def hand_over_kernel(*refs):
    count = (len(refs) - 2) // 3
    given, taken, held = refs[:count], refs[count : 2 * count], refs[2 * count : 3 * count]
    in_sem, out_sem = refs[3 * count :]
    ins = [pltpu.make_async_copy(given[n], held[n], in_sem.at[n]) for n in range(count)]
    outs = [pltpu.make_async_copy(held[n], taken[n], out_sem.at[n]) for n in range(count)]
    for copy in ins:
        copy.start()
    for first, then in zip(ins, outs):
        first.wait()
        then.start()
    for copy in outs:
        copy.wait()


def hand_over(arrays):
    count = len(arrays)
    anywhere = pl.BlockSpec(memory_space=pl.ANY)
    return pl.pallas_call(
        hand_over_kernel,
        out_shape=[jax.ShapeDtypeStruct(a.shape, a.dtype) for a in arrays],
        in_specs=[anywhere] * count,
        out_specs=[anywhere] * count,
        scratch_shapes=[pltpu.VMEM(a.shape, a.dtype) for a in arrays]
        + [pltpu.SemaphoreType.DMA((count,))] * 2,
        name="hand_over",
    )(*arrays)


def gathered(tokens, timestep, mod_weight, qkv_weight, attn_scale, out_weight, grad_update):
    length = tokens.shape[0] * lax.axis_size("row") * lax.axis_size("col")
    if mod_weight.shape != (qkv_weight.shape[2], length):
        return per_device(
            tokens, timestep, mod_weight, qkv_weight, attn_scale, out_weight, grad_update
        )
    embedded = embed(timestep, mod_weight.shape[0] // 2)[:, None]
    return tuple(
        hand_over(
            fused(attn_scale, embedded, tokens, grad_update, mod_weight, qkv_weight, out_weight)
        )
    )


def solution(mesh):
    placed = (
        P(("row", "col"), None),
        P(),
        P(),
        P(None, None, "col"),
        P("col"),
        P("col", None),
        P(("row", "col"), None),
    )
    plane = mesh.shape["row"] == 4 and mesh.shape["col"] == 8
    return jax.shard_map(
        gathered if plane else per_device,
        mesh=mesh,
        in_specs=placed,
        out_specs=(
            P(("row", "col"), None),
            P(("row", "col"), None),
            P(None, "row", "col"),
            P("col", "row"),
        ),
        check_vma=False,
    )
```

```python
import functools
import math

import jax
import jax.numpy as jnp
from jax import lax
from jax.experimental import pallas as pl
from jax.experimental.pallas import tpu as pltpu
from jax.sharding import PartitionSpec as P

epsilon = 1e-06
MESH = pl.DeviceIdType.MESH
RELAYED = 4


def embed(timestep, count):
    index = jnp.arange(count, dtype=jnp.float32)
    freqs = jnp.exp(-math.log(10000.0) * index / count)
    angles = timestep.astype(jnp.float32)[0] * freqs
    return jnp.concatenate([jnp.cos(angles), jnp.sin(angles)])


def by_head(array, head_dim):
    return [array[:, at : at + head_dim] for at in range(0, array.shape[1], head_dim)]


def unit_rows(values):
    factor = lax.rsqrt(jnp.mean(values * values, -1, keepdims=True) + epsilon)
    return (values * factor, factor)


def unit_grad(grad_unit, unit, factor):
    return factor * (grad_unit - unit * jnp.mean(grad_unit * unit, -1, keepdims=True))


def piece(ref, dim, size, index):
    start = index * size
    if isinstance(start, int):
        pass
    elif dim == len(ref.shape) - 1:
        start = pl.multiple_of(start, 128)
    elif dim == len(ref.shape) - 2:
        start = pl.multiple_of(start, 16)
    return ref.at[(slice(None),) * dim + (pl.ds(start, size),)]


def half(ref, side):
    dim = len(ref.shape) - 2
    size = ref.shape[dim] // 2
    return ref.at[(slice(None),) * dim + (pl.ds(side * size, size),)]


def exchange_kernel(plan, *refs):
    count = len(plan)
    sources, targets = refs[:count], refs[count : 2 * count]
    own_sem, send_sem, recv_sem = refs[2 * count : 2 * count + 3]
    relays = refs[2 * count + 3 :]
    sizes = {axis: n for axis, n, dim, size in plan}
    barrier = pltpu.get_barrier_semaphore()
    for axis, n in sizes.items():
        me = lax.axis_index(axis)
        for step in range(1, n):
            pl.semaphore_signal(
                barrier, inc=1, device_id={axis: lax.rem(me + step, n)}, device_id_type=MESH
            )
    pl.semaphore_wait(barrier, sum(n - 1 for n in sizes.values()))
    def send(job, slot, source, target, peer):
        copy = pltpu.make_async_remote_copy(
            src_ref=source,
            dst_ref=target,
            send_sem=send_sem.at[job, slot],
            recv_sem=recv_sem.at[job, slot],
            device_id={plan[job][0]: peer},
            device_id_type=MESH,
        )
        copy.start()
        return copy

    copies, hops = [], {}
    chained = [job for job in range(count) if plan[job][1] == RELAYED and plan[job][2] is not None]
    relayed = [job for job in range(count) if plan[job][1] == RELAYED and job not in chained]
    for step in range(1, max(sizes.values())):
        for job, (axis, n, dim, size) in enumerate(plan):
            if step >= n or job in chained or (n == RELAYED and step == 2):
                continue
            me = lax.axis_index(axis)
            peer = lax.rem(me + step, n)
            source = sources[job]
            source = source if dim is None else piece(source, dim, size, peer)
            copy = send(job, step, source, targets[job].at[me], peer)
            if n == RELAYED and dim is None:
                hops.setdefault(job, []).append(copy)
            else:
                copies.append(copy)
    for job, (axis, n, dim, size) in enumerate(plan):
        if job in chained:
            continue
        me = lax.axis_index(axis)
        source = sources[job]
        copy = pltpu.make_async_copy(
            source if dim is None else piece(source, dim, size, me),
            targets[job].at[me],
            own_sem.at[job],
        )
        copy.start()
        copies.append(copy)
    for side in range(2):
        for job in relayed:
            axis, n, dim, size = plan[job]
            me = lax.axis_index(axis)
            right, left = lax.rem(me + 1, n), lax.rem(me + 3, n)
            onward, origin = (right, left) if side == 0 else (left, right)
            hops[job][side].wait_recv()
            landing = half(targets[job].at[origin], side)
            copies.append(send(job, 6 + side, landing, landing, onward))
    def link(job, way, owner, source):
        axis = plan[job][0]
        me = lax.axis_index(axis)
        slot = owner - 1 if way == 0 else owner
        return pltpu.make_async_remote_copy(
            src_ref=relays[job].at[way, slot] if source is None else source,
            dst_ref=relays[job].at[way, slot],
            send_sem=send_sem.at[job, 3 * way + slot],
            recv_sem=recv_sem.at[job, 3 * way + slot],
            device_id={axis: lax.rem(me + (1 if way == 0 else RELAYED - 1), RELAYED)},
            device_id_type=MESH,
        )

    def forward(job, way, owner, place):
        axis, n, dim, size = plan[job]
        mine = piece(sources[job], dim, size, owner)

        @pl.when(lax.axis_index(axis) == place)
        def _():
            if place == (0 if way == 0 else n - 1):
                link(job, way, owner, mine).start()
            else:
                copy = link(job, way, owner, None)
                copy.wait_recv()
                inbox = relays[job].at[way, owner - 1 if way == 0 else owner]
                total = inbox[...].astype(jnp.float32) + mine[...].astype(jnp.float32)
                inbox[...] = total.astype(inbox.dtype)
                copy.start()

    order = [(0, 3, 0), (1, 0, 3), (0, 2, 0), (1, 1, 3), (0, 1, 0), (1, 2, 3)]
    order += [(0, 3, 1), (1, 0, 2), (0, 2, 1), (1, 1, 2), (0, 3, 2), (1, 0, 1)]
    for way, owner, place in order:
        for job in chained:
            forward(job, way, owner, place)
    for job in chained:
        axis, n, dim, size = plan[job]
        for owner in range(n):

            @pl.when(lax.axis_index(axis) == owner)
            def _():
                total = piece(sources[job], dim, size, owner)[...].astype(jnp.float32)
                if owner > 0:
                    link(job, 0, owner, None).wait_recv()
                    total = total + relays[job][0, owner - 1].astype(jnp.float32)
                if owner < n - 1:
                    link(job, 1, owner, None).wait_recv()
                    total = total + relays[job][1, owner].astype(jnp.float32)
                targets[job][0] = total
                for other in range(n):
                    if other > owner:
                        link(job, 0, other, None).wait_send()
                    if other < owner:
                        link(job, 1, other, None).wait_send()

    for job in relayed:
        for copy in hops[job]:
            copy.wait_send()
    for copy in copies:
        copy.wait()


def exchange(jobs, collective_id):
    plan, shapes, relays = [], [], []
    for array, axis, dim in jobs:
        n = lax.axis_size(axis)
        block = list(array.shape)
        size = None
        if dim is not None:
            size = block[dim] = block[dim] // n
        plan.append((axis, n, dim, size))
        if n == RELAYED and dim is not None:
            shapes.append(jax.ShapeDtypeStruct((1,) + tuple(block), jnp.float32))
            relays.append(pltpu.VMEM((2, n - 1) + tuple(block), array.dtype))
        else:
            shapes.append(jax.ShapeDtypeStruct((n,) + tuple(block), array.dtype))
            relays.append(pltpu.VMEM((16, 128), array.dtype))
    most = max(2 * RELAYED, max(n for axis, n, dim, size in plan))
    count = len(jobs)
    in_vmem = pl.BlockSpec(memory_space=pltpu.VMEM)
    return pl.pallas_call(
        functools.partial(exchange_kernel, tuple(plan)),
        out_shape=shapes,
        in_specs=[in_vmem] * count,
        out_specs=[in_vmem] * count,
        scratch_shapes=[
            pltpu.SemaphoreType.DMA((count,)),
            pltpu.SemaphoreType.DMA((count, most)),
            pltpu.SemaphoreType.DMA((count, most)),
            *relays,
        ],
        compiler_params=pltpu.CompilerParams(
            collective_id=collective_id, has_side_effects=True, vmem_limit_bytes=48 * 2**20
        ),
        name=f"exchange_{collective_id}",
    )(*[array for array, axis, dim in jobs])


def dot_rows(left, right):
    return lax.dot_general(
        left, right, (((1,), (1,)), ((), ())), preferred_element_type=jnp.float32
    )


def dot_columns(left, right):
    return lax.dot_general(
        left, right, (((0,), (0,)), ((), ())), preferred_element_type=jnp.float32
    )


def attention_kernel(
    scale_ref, q_ref, k_ref, v_ref, g_ref, o_ref, dq_ref, dk_ref, dv_ref, dk_sum, dv_sum
):
    block = pl.program_id(1)
    scale = scale_ref[pl.program_id(0)]
    coeff = scale * (1.0 / q_ref.shape[1])
    query, keys, values, grad = q_ref[...], k_ref[...], v_ref[...], g_ref[...]
    weights = jnp.exp(dot_rows(query, keys) * coeff - scale)
    inverse = 1.0 / jnp.sum(weights, -1, keepdims=True)
    mixed = jnp.dot(weights.astype(jnp.bfloat16), values, preferred_element_type=jnp.float32)
    attended = (mixed * inverse).astype(jnp.bfloat16)
    o_ref[...] = attended
    delta = jnp.sum(
        grad.astype(jnp.float32) * attended.astype(jnp.float32), -1, keepdims=True
    )
    probs = weights * inverse
    dscores = (probs * (dot_rows(grad, values) - delta) * coeff).astype(jnp.bfloat16)
    dq_ref[...] = jnp.dot(dscores, keys, preferred_element_type=jnp.float32)
    dk_part = dot_columns(dscores, query)
    dv_part = dot_columns(probs.astype(jnp.bfloat16), grad)

    @pl.when(block == 0)
    def _():
        dk_sum[...] = dk_part
        dv_sum[...] = dv_part

    @pl.when(block > 0)
    def _():
        dk_sum[...] += dk_part
        dv_sum[...] += dv_part

    @pl.when(block == pl.num_programs(1) - 1)
    def _():
        dk_ref[...] = dk_sum[...].astype(dk_ref.dtype)
        dv_ref[...] = dv_sum[...].astype(dv_ref.dtype)


def attention(attn_scale, queries, keys_values, grads):
    heads = attn_scale.shape[0]
    span, inner = queries.shape
    length = keys_values.shape[0]
    head_dim = inner // heads
    size = math.gcd(span, 256)
    while size * length > 2**19 and size % 32 == 0:
        size //= 2
    mine = pl.BlockSpec((size, head_dim), lambda h, i: (i, h))
    keys = pl.BlockSpec((length, head_dim), lambda h, i: (0, h))
    values = pl.BlockSpec((length, head_dim), lambda h, i: (0, heads + h))
    return pl.pallas_call(
        attention_kernel,
        grid=(heads, span // size),
        out_shape=[
            jax.ShapeDtypeStruct((span, inner), jnp.bfloat16),
            jax.ShapeDtypeStruct((span, inner), jnp.float32),
            jax.ShapeDtypeStruct((length, inner), jnp.bfloat16),
            jax.ShapeDtypeStruct((length, inner), jnp.bfloat16),
        ],
        in_specs=[pl.BlockSpec(memory_space=pltpu.SMEM), mine, keys, values, mine],
        out_specs=[mine, mine, keys, keys],
        scratch_shapes=[pltpu.VMEM((length, head_dim), jnp.float32)] * 2,
        compiler_params=pltpu.CompilerParams(
            dimension_semantics=("arbitrary", "arbitrary"), vmem_limit_bytes=56 * 2**20
        ),
        name="attention",
    )(attn_scale, queries, keys_values, keys_values, grads)


def add_up(slots):
    return jnp.sum(slots.astype(jnp.float32), 0)


def per_device(tokens, timestep, mod_weight, qkv_weight, attn_scale, out_weight, grad_update):
    tok_dev, width = tokens.shape
    heads_here = attn_scale.shape[0]
    inner = qkv_weight.shape[2]
    head_dim = inner // heads_here
    span = tok_dev * lax.axis_size("col")
    embedded = embed(timestep, mod_weight.shape[0] // 2)
    gain = 1.0 + jnp.sum(embedded[:, None] * mod_weight, 0)
    tok_float = tokens.astype(jnp.float32)
    rstd = lax.rsqrt(jnp.mean(tok_float * tok_float, -1, keepdims=True) + epsilon)
    normed = tok_float * rstd
    hidden = (normed * gain).astype(jnp.bfloat16)
    (group,) = exchange([(hidden, "col", None)], 0)
    group = group.reshape(span, width)
    raw = [jnp.dot(group, qkv_weight[k], preferred_element_type=jnp.float32) for k in range(3)]
    query_unit, query_factor = zip(*[unit_rows(part) for part in by_head(raw[0], head_dim)])
    key_unit, key_factor = zip(*[unit_rows(part) for part in by_head(raw[1], head_dim)])
    queries = jnp.concatenate(query_unit, 1).astype(jnp.bfloat16)
    keys_values = jnp.concatenate(key_unit + (raw[2],), 1).astype(jnp.bfloat16)
    all_keys_values, grad_group = exchange(
        [(keys_values, "row", None), (grad_update, "col", None)], 1
    )
    all_keys_values = all_keys_values.reshape(-1, 2 * inner)
    grad_group = grad_group.reshape(span, width)
    grad_attended = dot_rows(grad_group, out_weight).astype(jnp.bfloat16)
    attended, grad_query, key_part, value_part = attention(
        attn_scale, queries, all_keys_values, grad_attended
    )
    update_part = jnp.dot(attended, out_weight, preferred_element_type=jnp.float32).astype(
        jnp.bfloat16
    )
    out_part = dot_columns(attended, grad_group).astype(jnp.bfloat16)
    key_slots, value_slots, update_slots = exchange(
        [(key_part, "row", 0), (value_part, "row", 0), (update_part, "col", 0)], 2
    )
    update = add_up(update_slots).astype(jnp.bfloat16)

    def raw_grads(grad_unit, unit, factor):
        parts = zip(by_head(grad_unit, head_dim), unit, factor)
        return jnp.concatenate([unit_grad(*part) for part in parts], 1).astype(jnp.bfloat16)

    grad_raw = [
        raw_grads(grad_query, query_unit, query_factor),
        raw_grads(add_up(key_slots), key_unit, key_factor),
        add_up(value_slots).astype(jnp.bfloat16),
    ]
    qkv_part = jnp.stack([dot_columns(group, part).astype(jnp.bfloat16) for part in grad_raw])
    hidden_part = (
        sum(dot_rows(part, qkv_weight[k]) for k, part in enumerate(grad_raw))
    ).astype(jnp.bfloat16)
    qkv_slots, hidden_slots, out_slots = exchange(
        [(qkv_part, "row", 1), (hidden_part, "col", 0), (out_part, "row", 1)], 3
    )
    grad_qkv = add_up(qkv_slots)
    grad_out = add_up(out_slots)
    grad_normed = add_up(hidden_slots) * gain
    grad_tokens = (
        rstd * (grad_normed - normed * jnp.mean(grad_normed * normed, -1, keepdims=True))
    ).astype(jnp.bfloat16)
    return (update, grad_tokens, grad_qkv, grad_out)


def flip(index, bit):
    return index + bit - 2 * bit * ((index // bit) % 2)


class Place:
    def __init__(self):
        self.row = lax.axis_index("row")
        self.col = lax.axis_index("col")
        self.partner = flip(self.col, 1)
        self.beside = flip(self.col, 2)
        self.across = flip(self.col, 4)
        self.corner = flip(self.beside, 4)
        self.inner = ((self.row + 1) // 2) % 2 == 1
        self.mate = flip(self.row, 1)
        self.facing = 3 - self.row
        low = 1 - self.row // 2
        self.ranks = [self.row, self.mate, 1 + low, 3 * low]

    def greet(self):
        barrier = pltpu.get_barrier_semaphore()
        for peer in (self.partner, self.beside, self.across, self.corner):
            pl.semaphore_signal(barrier, inc=1, device_id={"col": peer}, device_id_type=MESH)
        for peer in self.ranks[1:]:
            pl.semaphore_signal(barrier, inc=1, device_id={"row": peer}, device_id_type=MESH)

    def await_greetings(self):
        pl.semaphore_wait(pltpu.get_barrier_semaphore(), 7)


LINE, BESIDE, ACROSS, TOP, BOTTOM, MATE = 0, 1, 2, 3, 4, 5
WHOLE, LEVEL, SLICE, BLOCK, FAR = 0, 1, 2, 3, 4
LINES = (WHOLE, BLOCK, FAR)
PLANES = [(WHOLE, rank) for rank in range(4)] + [(LEVEL, 0)] + [(SLICE, r) for r in (1, 2, 3)]


def numbered(keys):
    return {key: at for at, key in enumerate(keys)}


SENDS = numbered(
    [(job, rank, 0) for job in LINES for rank in range(4)]
    + [(job, 0, 1) for job in LINES]
    + [(SLICE, at, 0) for at in range(3)]
    + [plane + (kind,) for plane in PLANES for kind in range(2, 10)]
)
ARRIVALS = numbered(
    [(SLICE, row, LINE) for row in range(4)]
    + [(job, rank, LINE) for job in LINES for rank in (1, 2, 3)]
    + [plane + (kind,) for plane in PLANES for kind in range(1, 9)]
)


class Gather:
    def __init__(self, place, job, tile, whole, send_sem, recv_sem, split=False):
        self.split = split
        self.place, self.job, self.tile, self.whole = place, job, tile, whole
        self.send_sem, self.recv_sem = send_sem, recv_sem

    def slot(self, rank, col):
        return self.whole.at[self.place.ranks[rank], col]

    def link(self, rank, kind, send, source, landing, peer):
        return pltpu.make_async_remote_copy(
            src_ref=source,
            dst_ref=landing,
            send_sem=self.send_sem.at[SENDS.get((self.job,) + send, 0)],
            recv_sem=self.recv_sem.at[ARRIVALS[self.job, rank, kind]],
            device_id=peer,
            device_id_type=MESH,
        )

    def arrived(self, rank, kind, landing):
        self.link(rank, kind, (0, 0), landing, landing, {"col": self.place.partner}).wait_recv()

    def held(self, rank):
        return self.tile if rank == 0 else self.slot(rank, self.place.col)

    def line_sends(self, rank):
        p = self.place
        mine = self.slot(rank, p.col)
        held = self.held(rank)
        if rank == 0:
            outward = self.link(1, LINE, (0, 0), held, mine, {"row": p.mate})
            inward = self.link(2, LINE, (0, 1), held, mine, {"row": p.facing})
            return [(outward, False), (inward, True)]
        if rank == 1:
            return [(self.link(3, LINE, (1, 0), held, mine, {"row": p.facing}), True)]
        return [(self.link(rank, LINE, (rank, 0), held, mine, {"row": p.mate}), True)]

    def plane_sends(self, rank):
        p = self.place
        mine, held = self.slot(rank, p.col), self.held(rank)
        return [
            self.link(rank, BESIDE, (rank, 2), held, mine, {"col": p.beside}),
            self.link(rank, ACROSS, (rank, 3), held, mine, {"col": p.across}),
            self.link(rank, MATE, (rank, 4), held, mine, {"col": p.partner}),
        ]

    def strip(self, ref, rank, side):
        if not self.split or rank == 0:
            return half(ref, side)
        size = ref.shape[0] // 4
        return ref.at[pl.ds(side * size, size)]

    def relays(self, rank):
        p = self.place
        side, over = self.slot(rank, p.beside), self.slot(rank, p.across)
        return [
            self.link(rank, TOP, (rank, 5), self.strip(side, rank, 0), self.strip(side, rank, 0), {"col": p.across}),
            self.link(rank, MATE + 1, (rank, 6), side, side, {"col": p.partner}),
            self.link(rank, BOTTOM, (rank, 7), self.strip(over, rank, 1), self.strip(over, rank, 1), {"col": p.beside}),
            self.link(rank, MATE + 2, (rank, 8), over, over, {"col": p.partner}),
        ]

    def last(self, rank):
        p = self.place
        far = self.slot(rank, p.corner)
        return self.link(rank, MATE + 3, (rank, 9), far, far, {"col": p.partner})

    def each(self, copies, act):
        for copy, inner in copies:
            if inner:
                pl.when(self.place.inner)(functools.partial(act, copy))
            else:
                act(copy)

    def pass_on(self, rank):
        self.arrived(rank, LINE, self.slot(rank, self.place.col))
        self.each(self.line_sends(rank), lambda copy: copy.start())

    def spread(self, rank):
        for copy in self.plane_sends(rank):
            copy.start()

    def relay(self, rank):
        p = self.place
        top, side, bottom, over = self.relays(rank)
        self.arrived(rank, BESIDE, self.slot(rank, p.beside))
        top.start()
        side.start()
        self.arrived(rank, ACROSS, self.slot(rank, p.across))
        bottom.start()
        over.start()

    def close(self, rank):
        p = self.place
        far = self.slot(rank, p.corner)
        self.arrived(rank, TOP, self.strip(far, rank, 0))
        self.arrived(rank, BOTTOM, self.strip(far, rank, 1))
        self.last(rank).start()

    def whole_rank(self, rank):
        p = self.place
        for kind, col in enumerate((p.col, p.beside, p.across, p.corner)):
            self.arrived(rank, MATE + kind, self.slot(rank, flip(col, 1)))

    def drain_line(self):
        for rank in range(4):
            self.each(self.line_sends(rank), lambda copy: copy.wait_send())

    def drain_plane(self, rank):
        for copy in self.plane_sends(rank) + self.relays(rank) + [self.last(rank)]:
            copy.wait_send()


class Level(Gather):
    def slot(self, rank, col):
        return self.whole.at[col]


class Line(Gather):
    def slot(self, rank, col):
        return self.whole.at[self.place.ranks[rank]]


class Corner(Gather):
    def slot(self, rank, col):
        return half(self.whole.at[self.place.ranks[rank], self.place.corner], 1)


class Slices(Gather):
    def cuts(self):
        p = self.place
        size = self.whole.shape[3]
        copies = []
        for at, peer in enumerate(p.ranks[1:]):
            mine = pl.ds(pl.multiple_of(peer * size, 128), size)
            copies.append(
                pltpu.make_async_remote_copy(
                    src_ref=self.tile.at[:, mine],
                    dst_ref=self.slot(0, p.col),
                    send_sem=self.send_sem.at[SENDS[self.job, at, 0]],
                    recv_sem=self.recv_sem.at[p.row],
                    device_id={"row": peer},
                    device_id_type=MESH,
                )
            )
        return copies

    def landed(self, rank):
        p = self.place
        slot = self.slot(rank, p.col)
        pltpu.make_async_remote_copy(
            src_ref=slot,
            dst_ref=slot,
            send_sem=self.send_sem.at[SENDS[self.job, 0, 0]],
            recv_sem=self.recv_sem.at[p.ranks[rank]],
            device_id={"col": p.partner},
            device_id_type=MESH,
        ).wait_recv()

    def held(self, rank):
        return self.slot(rank, self.place.col)


class Scatter:
    def __init__(self, place, job, part, crossed, landed, send_sem, recv_sem):
        self.place, self.job, self.part = place, job, part
        self.crossed, self.landed = crossed, landed
        self.send_sem, self.recv_sem = send_sem, recv_sem
        self.size = part.shape[0] // 8

    def targets(self):
        p = self.place
        return (p.corner, p.beside, p.across, p.col)

    def rows(self, col):
        return pl.ds(pl.multiple_of(col * self.size, 16), self.size)

    def core_send(self, at):
        p = self.place
        return pltpu.make_async_remote_copy(
            src_ref=self.part.at[self.rows(flip(self.targets()[at], 1))],
            dst_ref=self.crossed.at[self.job, at],
            send_sem=self.send_sem.at[self.job, at],
            recv_sem=self.recv_sem.at[self.job, at],
            device_id={"col": p.partner},
            device_id_type=MESH,
        )

    def chip_send(self, at):
        return pltpu.make_async_remote_copy(
            src_ref=self.part.at[self.rows(self.targets()[at])],
            dst_ref=self.landed.at[self.job, at],
            send_sem=self.send_sem.at[self.job, 4 + at],
            recv_sem=self.recv_sem.at[self.job, 4 + at],
            device_id={"col": self.targets()[at]},
            device_id_type=MESH,
        )

    def chip_sum(self, at):
        mine = self.part[self.rows(self.targets()[at]), :].astype(jnp.float32)
        return mine + self.crossed[self.job, at].astype(jnp.float32)

    def first(self):
        for at in range(4):
            self.core_send(at).start()

    def second(self):
        for at in range(3):
            self.core_send(at).wait_recv()
            self.part[self.rows(self.targets()[at]), :] = self.chip_sum(at).astype(self.part.dtype)
            self.chip_send(at).start()

    def third(self):
        self.core_send(3).wait_recv()
        total = self.chip_sum(3)
        for at in (1, 2, 0):
            self.chip_send(at).wait_recv()
            total = total + self.landed[self.job, at].astype(jnp.float32)
        for at in range(4):
            self.core_send(at).wait_send()
        for at in range(3):
            self.chip_send(at).wait_send()
        return total


LOG2E = 1.4426950408889634


def dot(left, right):
    return jnp.dot(left, right, preferred_element_type=jnp.float32)


def fused_kernel(
    scale_ref, embed_ref, tok_ref, grad_ref, mod_hbm, qkv_hbm, out_hbm,
    update_hbm, grad_tok_hbm, grad_qkv_hbm, grad_out_hbm,
    update_ref, grad_tok_ref, grad_qkv_ref, grad_out_ref, hidden_ref, gain_ref, qkv_ref, out_ref, load_sem, hid_all, grad_level, grad_cut, do_all, raw_ref, q_ref, qt_ref, k_ref, kt_ref, v_ref, vt_ref,
    w_ref, inv_ref, own_ref, att_ref, dot_ref, dkt_ref, dvt_ref, gr_ref,
    part_ref, crossed, landed, send_sem, recv_sem, send_sum, recv_sum,
):
    bf = jnp.bfloat16
    place = Place()
    rows, cols, tok_dev, width = hid_all.shape
    heads, length, hdim = q_ref.shape
    span = cols * tok_dev
    size = math.gcd(span, 256)
    per_rank = span // size
    narrow = width // rows
    dog_ref = v_ref
    mod_loads = [
        pltpu.make_async_copy(
            mod_hbm.at[pl.ds(head * hdim, hdim)], dkt_ref.at[head], load_sem.at[2 + head]
        )
        for head in range(heads)
    ]
    loads = [
        pltpu.make_async_copy(qkv_hbm, qkv_ref, load_sem.at[0]),
        pltpu.make_async_copy(out_hbm, out_ref, load_sem.at[1]),
    ]
    stores = [
        pltpu.make_async_copy(held, to, load_sem.at[2 + heads + at])
        for at, (held, to) in enumerate(
            (
                (update_ref, update_hbm),
                (grad_tok_ref, grad_tok_hbm),
                (grad_qkv_ref, grad_qkv_hbm),
                (grad_out_ref, grad_out_hbm),
            )
        )
    ]
    for load in mod_loads + loads:
        load.start()
    place.greet()
    gain = 1.0
    for head, load in enumerate(mod_loads):
        load.wait()
        waves = jnp.broadcast_to(embed_ref[head : head + 1, :], (hdim, hdim)).T[:, :1]
        here = waves * dkt_ref[head]
        gain = gain + jnp.sum(here, 0, keepdims=True)
    gain_ref[...] = jnp.broadcast_to(gain, gain_ref.shape)

    def normed_rows():
        tok_float = tok_ref[...].astype(jnp.float32)
        rstd = lax.rsqrt(jnp.mean(tok_float * tok_float, -1, keepdims=True) + epsilon)
        return tok_float * rstd, rstd

    hidden_ref[...] = (normed_rows()[0] * gain_ref[0:1, :]).astype(bf)
    place.await_greetings()
    hid = Gather(place, 0, hidden_ref, hid_all, send_sem, recv_sem, True)
    far = Corner(
        place, 4, half(hid_all.at[place.row, place.corner], 1), hid_all, send_sem, recv_sem
    )
    grd = Level(place, 1, grad_ref, grad_level, send_sem, recv_sem)
    cut = Slices(place, 2, grad_ref, grad_cut, send_sem, recv_sem)
    dol = Line(place, 3, do_all.at[place.row], do_all, send_sem, recv_sem)
    scatters = [
        Scatter(place, job, part_ref, crossed, landed, send_sum, recv_sum) for job in range(2)
    ]

    def start_all(copies):
        hid.each(copies, lambda copy: copy.start())

    def tokens_at(rank, chunk):
        return pl.multiple_of(place.ranks[rank] * span + chunk * size, size)

    def within(chunk):
        return pl.ds(pl.multiple_of(chunk * size, size), size)

    def steps(count, body):
        def step(at, carry):
            body(at)
            return carry

        lax.fori_loop(0, count, step, 0)

    def blocks(body):
        steps(heads * per_rank, lambda at: body(at // per_rank, at % per_rank))

    few = size // tok_dev

    def project(rank):
        def body(chunk):
            at = pl.ds(tokens_at(rank, chunk), size)
            here = hid_all[place.ranks[rank], pl.ds(chunk * few, few)].reshape(size, width)
            for k in range(3):
                raw = dot(here, qkv_ref[k])
                for head, part in enumerate(by_head(raw, hdim)):
                    if k < 2:
                        raw_ref[k, head, at, :] = part.astype(bf)
                        part = unit_rows(part)[0]
                    part = part.astype(bf)
                    if k == 0:
                        q_ref[head, at, :] = part
                        qt_ref[head, :, at] = part.T
                    elif k == 1:
                        k_ref[head, at, :] = part
                        kt_ref[head, :, at] = part.T
                    else:
                        v_ref[head, at, pl.ds(0, hdim)] = part
                        vt_ref[head, pl.ds(0, hdim), at] = part.T

        steps(per_rank, body)

    def cotangent():
        def body(chunk):
            here = grad_level[pl.ds(chunk * few, few)].reshape(size, width)
            value = dot_rows(here, out_ref[...]).astype(bf)
            for head, part in enumerate(by_head(value, hdim)):
                do_all[place.row, head, within(chunk), :] = part

        steps(per_rank, body)

    wide = min(512, span)

    def key_spans(key_rank):
        first = pl.multiple_of(place.ranks[key_rank] * span, span)
        for start in range(0, span, wide):
            yield pl.ds(pl.multiple_of(first + start, wide), wide)

    def weigh(head, at, here):
        coeff = scale_ref[head] * (LOG2E / hdim)
        weights = jnp.exp2(dot(q_ref[head, at, :], kt_ref[head, :, here]) * coeff).astype(bf)
        w_ref[head, at, here] = weights
        return weights

    def weigh_early(pairs):
        def body(head, chunk):
            for rank, key_rank in pairs:
                for here in key_spans(key_rank):
                    weigh(head, pl.ds(tokens_at(rank, chunk), size), here)

        blocks(body)

    def forward(rank, weighed=()):
        def body(head, chunk):
            at = pl.ds(tokens_at(rank, chunk), size)
            mixed = None
            for key_rank in range(rows):
                for here in key_spans(key_rank):
                    weights = w_ref[head, at, here] if key_rank in weighed else weigh(head, at, here)
                    more = dot(weights, v_ref[head, here, :])
                    mixed = more if mixed is None else mixed + more
            inverse = 1.0 / mixed[:, hdim:]
            attended = (mixed[:, :hdim] * inverse).astype(bf)
            if rank == 0:
                own_ref[head, within(chunk), :] = attended
            att_ref[head, :, at] = attended.T
            inv_ref[head, :, at] = inverse.T[:8]

        blocks(body)

    def prepare(rank):
        def body(head, chunk):
            at = pl.ds(tokens_at(rank, chunk), size)
            turned = do_all[place.ranks[rank], head, within(chunk), :].T.astype(jnp.float32)
            delta = jnp.sum(turned * att_ref[head, :, at].astype(jnp.float32), 0, keepdims=True)
            inverse = inv_ref[head, 0:1, at]
            turned = turned * inverse
            dot_ref[head, :, at] = turned.astype(bf)
            delta = jnp.broadcast_to(delta * inverse, (hdim, size))
            high = delta.astype(bf).astype(jnp.float32)
            line = lax.broadcasted_iota(jnp.int32, (hdim, size), 0)
            spare = jnp.where(line == 0, -high, jnp.where(line == 1, high - delta, 0.0))
            dog_ref[head, at, :] = jnp.concatenate([turned, spare], 0).astype(bf).T

        blocks(body)

    def backward(rank, fresh, stored=()):
        def body(head, chunk):
            at = pl.ds(tokens_at(rank, chunk), size)
            coeff = scale_ref[head] * (1.0 / hdim)
            whole = len(fresh) + len(stored) == rows
            grad_more = dog_ref[head, at, :]
            grad_turned = dot_ref[head, :, at]
            query_turned = qt_ref[head, :, at]
            grad_query = None
            for key_rank in stored + fresh:
                first = pl.multiple_of(place.ranks[key_rank] * span, span)
                for start in range(0, span, wide):
                    here = pl.ds(pl.multiple_of(first + start, wide), wide)
                    weights = w_ref[head, at, here]
                    if key_rank in fresh:
                        dprobs = dot(grad_more, vt_ref[head, :, here])
                        dscores = weights * dprobs.astype(bf)
                        dkt_ref[head, :, here] += dot(query_turned, dscores)
                        dvt_ref[head, :, here] += dot(grad_turned, weights)
                        if not whole:
                            w_ref[head, at, here] = dscores
                    else:
                        dscores = weights
                    if whole:
                        more = dot(dscores, k_ref[head, here, :])
                        grad_query = more if grad_query is None else grad_query + more
            if whole:
                unit, factor = unit_rows(raw_ref[0, head, at, :].astype(jnp.float32))
                gr_ref[0, head, at, :] = unit_grad(grad_query * coeff, unit, factor).astype(bf)

        blocks(body)

    def finish_keys(rank):
        def body(head, chunk):
            at = pl.ds(tokens_at(rank, chunk), size)
            coeff = scale_ref[head] * (1.0 / hdim)
            unit, factor = unit_rows(raw_ref[1, head, at, :].astype(jnp.float32))
            both = jnp.concatenate([dkt_ref[head, :, at], dvt_ref[head, :, at]], 0).astype(bf).T
            grad_key = both[:, :hdim].astype(jnp.float32) * coeff
            gr_ref[1, head, at, :] = unit_grad(grad_key, unit, factor).astype(bf)
            gr_ref[2, head, at, :] = both[:, hdim:]

        blocks(body)

    def project_out():
        def body(chunk):
            mine = jnp.concatenate([own_ref[h, within(chunk), :] for h in range(heads)], 1)
            part_ref[within(chunk), :] = dot(mine, out_ref[...]).astype(bf)

        steps(per_rank, body)

    def project_down():
        def body(chunk):
            at = pl.ds(tokens_at(0, chunk), size)
            total = None
            for k in range(3):
                mine = jnp.concatenate([gr_ref[k, head, at, :] for head in range(heads)], 1)
                more = dot_rows(mine, qkv_ref[k])
                total = more if total is None else total + more
            part_ref[within(chunk), :] = total.astype(bf)

        steps(per_rank, body)

    def weight_grads():
        part = min(256, narrow)

        def body(step):
            start = pl.multiple_of(step * part, part)
            at = pl.ds(pl.multiple_of(place.row * narrow + start, 128), part)
            turned = hid_all[:, :, :, at].reshape(length, part).T
            for k in range(3):
                here = jnp.concatenate([gr_ref[k, head] for head in range(heads)], 1)
                grad_qkv_ref[k, pl.ds(start, part), :] = dot(turned, here)

        steps(narrow // part, body)

    def out_grads():
        mine = pl.ds(pl.multiple_of(place.row * narrow, 128), narrow)
        for rank in range(rows):
            if rank == 0:
                here = grad_level[:, :, mine]
            else:
                here = grad_cut[place.ranks[rank]]
            here = here.reshape(span, narrow)
            at = pl.ds(tokens_at(rank, 0), span)
            for head in range(heads):
                more = dot(att_ref[head, :, at], here)
                to = pl.ds(head * hdim, hdim)
                if rank == 0:
                    grad_out_ref[to, :] = more
                else:
                    grad_out_ref[to, :] += more

    def tokens_grad(down):
        normed, rstd = normed_rows()
        grad_normed = down * gain_ref[0:1, :]
        pull = jnp.mean(grad_normed * normed, -1, keepdims=True)
        grad_tok_ref[...] = (rstd * (grad_normed - normed * pull)).astype(bf)

    start_all(hid.line_sends(0))
    hid.spread(0)
    hid_all[place.row, place.col] = hidden_ref[...]
    v_ref[:, :, pl.ds(hdim, hdim)] = jnp.ones((heads, length, hdim), bf)
    vt_ref[:, pl.ds(hdim, hdim), :] = jnp.ones((heads, hdim, length), bf)
    dkt_ref[...] = jnp.zeros_like(dkt_ref)
    dvt_ref[...] = jnp.zeros_like(dvt_ref)
    grad_level[place.col] = grad_ref[...]
    hid.pass_on(1)
    hid.spread(1)
    hid.relay(0)
    hid.pass_on(2)
    hid.spread(2)

    @pl.when(place.inner)
    def _():
        hid.pass_on(3)

    hid.relay(1)
    hid.close(0)
    start_all(far.line_sends(0))
    hid.whole_rank(0)
    for load in loads:
        load.wait()
    project(0)

    @pl.when(jnp.logical_not(place.inner))
    def _():
        hid.arrived(3, LINE, hid.slot(3, place.col))

    hid.spread(3)
    for copy in cut.cuts():
        copy.start()
    far.pass_on(1)
    hid.relay(2)
    hid.close(1)

    @pl.when(place.inner)
    def _():
        far.pass_on(2)

    hid.whole_rank(1)
    project(1)

    @pl.when(place.inner)
    def _():
        far.pass_on(3)

    hid.relay(3)
    grd.spread(0)
    weigh_early([(0, 0), (0, 1), (1, 0), (1, 1)])

    @pl.when(jnp.logical_not(place.inner))
    def _():
        far.arrived(2, LINE, far.slot(2, place.col))

    hid.close(2)
    hid.whole_rank(2)
    project(2)
    weigh_early([(0, 2), (1, 2), (2, 0), (2, 1), (2, 2)])

    @pl.when(jnp.logical_not(place.inner))
    def _():
        far.arrived(3, LINE, far.slot(3, place.col))

    hid.close(3)
    hid.whole_rank(3)
    project(3)
    grd.relay(0)
    forward(0, (0, 1, 2))
    grd.close(0)
    project_out()
    scatters[0].first()
    grd.whole_rank(0)
    cotangent()
    start_all(dol.line_sends(0))
    scatters[0].second()
    for rank in range(1, 4):
        cut.landed(rank)
        cut.spread(rank)
    forward(1, (0, 1, 2))
    forward(2, (0, 1, 2))
    dol.pass_on(1)

    @pl.when(place.inner)
    def _():
        dol.pass_on(2)

    forward(3)
    prepare(0)
    backward(0, (0, 1, 2, 3))

    @pl.when(place.inner)
    def _():
        dol.pass_on(3)

    cut.relay(1)
    cut.relay(2)
    prepare(1)
    backward(1, (0, 1, 2, 3))
    cut.relay(3)
    cut.close(1)
    cut.close(2)

    @pl.when(jnp.logical_not(place.inner))
    def _():
        dol.arrived(2, LINE, dol.slot(2, place.col))

    prepare(2)
    backward(2, (0,))
    cut.close(3)

    @pl.when(jnp.logical_not(place.inner))
    def _():
        dol.arrived(3, LINE, dol.slot(3, place.col))

    prepare(3)
    backward(3, (0,))
    update_ref[...] = scatters[0].third().astype(update_ref.dtype)
    stores[0].start()
    finish_keys(0)
    project_down()
    scatters[1].first()
    for rank in range(1, 4):
        cut.whole_rank(rank)
    out_grads()
    stores[3].start()
    scatters[1].second()
    backward(2, (1, 2, 3), (0,))
    backward(3, (1, 2, 3), (0,))
    for rank in range(1, 4):
        finish_keys(rank)
    weight_grads()
    stores[2].start()
    tokens_grad(scatters[1].third())
    stores[1].start()
    hid.drain_line()
    far.drain_line()
    dol.drain_line()
    grd.drain_plane(0)
    for copy in cut.cuts():
        copy.wait_send()
    for rank in range(4):
        hid.drain_plane(rank)
        if rank > 0:
            cut.drain_plane(rank)
    for store in stores:
        store.wait()


def fused(scale, embedded, tokens, grad_update, mod_weight, qkv_weight, out_weight):
    bf, f32 = jnp.bfloat16, jnp.float32
    tok_dev, width = tokens.shape
    heads = scale.shape[0]
    inner = qkv_weight.shape[2]
    hdim = inner // heads
    rows, cols = lax.axis_size("row"), lax.axis_size("col")
    span = tok_dev * cols
    length = span * rows
    narrow = width // rows
    in_vmem = pl.BlockSpec(memory_space=pltpu.VMEM)
    return pl.pallas_call(
        fused_kernel,
        out_shape=[
            jax.ShapeDtypeStruct((tok_dev, width), bf),
            jax.ShapeDtypeStruct((tok_dev, width), bf),
            jax.ShapeDtypeStruct((3, narrow, inner), f32),
            jax.ShapeDtypeStruct((inner, narrow), f32),
        ],
        in_specs=[pl.BlockSpec(memory_space=pltpu.SMEM)]
        + [in_vmem] * 3
        + [pl.BlockSpec(memory_space=pl.ANY)] * 3,
        out_specs=[pl.BlockSpec(memory_space=pl.ANY)] * 4,
        scratch_shapes=[
            pltpu.VMEM((tok_dev, width), bf),
            pltpu.VMEM((tok_dev, width), bf),
            pltpu.VMEM((3, narrow, inner), f32),
            pltpu.VMEM((inner, narrow), f32),
            pltpu.VMEM((tok_dev, width), bf),
            pltpu.VMEM((8, width), f32),
            pltpu.VMEM(qkv_weight.shape, bf),
            pltpu.VMEM(out_weight.shape, bf),
            pltpu.SemaphoreType.DMA((6 + heads,)),
            pltpu.VMEM((rows, cols, tok_dev, width), bf),
            pltpu.VMEM((cols, tok_dev, width), bf),
            pltpu.VMEM((rows, cols, tok_dev, narrow), bf),
            pltpu.VMEM((rows, heads, span, hdim), bf),
            pltpu.VMEM((2, heads, length, hdim), bf),
            pltpu.VMEM((heads, length, hdim), bf),
            pltpu.VMEM((heads, hdim, length), bf),
            pltpu.VMEM((heads, length, hdim), bf),
            pltpu.VMEM((heads, hdim, length), bf),
            pltpu.VMEM((heads, length, 2 * hdim), bf),
            pltpu.VMEM((heads, 2 * hdim, length), bf),
            pltpu.VMEM((heads, length, length), bf),
            pltpu.VMEM((heads, 8, length), f32),
            pltpu.VMEM((heads, span, hdim), bf),
            pltpu.VMEM((heads, hdim, length), bf),
            pltpu.VMEM((heads, hdim, length), bf),
            pltpu.VMEM((heads, hdim, length), f32),
            pltpu.VMEM((heads, hdim, length), f32),
            pltpu.VMEM((3, heads, length, hdim), bf),
            pltpu.VMEM((span, width), bf),
            pltpu.VMEM((2, 4, tok_dev, width), bf),
            pltpu.VMEM((2, 3, tok_dev, width), bf),
            pltpu.SemaphoreType.DMA((len(SENDS),)),
            pltpu.SemaphoreType.DMA((len(ARRIVALS),)),
            pltpu.SemaphoreType.DMA((2, 8)),
            pltpu.SemaphoreType.DMA((2, 8)),
        ],
        compiler_params=pltpu.CompilerParams(
            collective_id=4, has_side_effects=True, vmem_limit_bytes=67043328
        ),
        name="fused",
    )(scale, embedded, tokens, grad_update, mod_weight, qkv_weight, out_weight)


def hand_over_kernel(*refs):
    count = (len(refs) - 2) // 3
    given, taken, held = refs[:count], refs[count : 2 * count], refs[2 * count : 3 * count]
    in_sem, out_sem = refs[3 * count :]
    ins = [pltpu.make_async_copy(given[n], held[n], in_sem.at[n]) for n in range(count)]
    outs = [pltpu.make_async_copy(held[n], taken[n], out_sem.at[n]) for n in range(count)]
    for copy in ins:
        copy.start()
    for first, then in zip(ins, outs):
        first.wait()
        then.start()
    for copy in outs:
        copy.wait()


def hand_over(arrays):
    count = len(arrays)
    anywhere = pl.BlockSpec(memory_space=pl.ANY)
    return pl.pallas_call(
        hand_over_kernel,
        out_shape=[jax.ShapeDtypeStruct(a.shape, a.dtype) for a in arrays],
        in_specs=[anywhere] * count,
        out_specs=[anywhere] * count,
        scratch_shapes=[pltpu.VMEM(a.shape, a.dtype) for a in arrays]
        + [pltpu.SemaphoreType.DMA((count,))] * 2,
        name="hand_over",
    )(*arrays)


def gathered(tokens, timestep, mod_weight, qkv_weight, attn_scale, out_weight, grad_update):
    length = tokens.shape[0] * lax.axis_size("row") * lax.axis_size("col")
    if mod_weight.shape != (qkv_weight.shape[2], length):
        return per_device(
            tokens, timestep, mod_weight, qkv_weight, attn_scale, out_weight, grad_update
        )
    embedded = embed(timestep, mod_weight.shape[0] // 2).reshape(attn_scale.shape[0], -1)
    return tuple(
        hand_over(
            fused(attn_scale, embedded, tokens, grad_update, mod_weight, qkv_weight, out_weight)
        )
    )


def solution(mesh):
    placed = (
        P(("row", "col"), None),
        P(),
        P(),
        P(None, None, "col"),
        P("col"),
        P("col", None),
        P(("row", "col"), None),
    )
    plane = mesh.shape["row"] == 4 and mesh.shape["col"] == 8
    return jax.shard_map(
        gathered if plane else per_device,
        mesh=mesh,
        in_specs=placed,
        out_specs=(
            P(("row", "col"), None),
            P(("row", "col"), None),
            P(None, "row", "col"),
            P("col", "row"),
        ),
        check_vma=False,
    )
```
